8 devices in a mesh: dp: 2 (over z, y), tp: 4 (over x, core).
Axes of the slice: x: 2, y: 2, z: 1, core: 2. Of those that a mesh axis runs over, the one named last changes fastest.
Arguments:
- x: bfloat16 [512, 4096], P('dp'), parts along dimension 0
- ln_attn_gamma: float32 [4096], replicated
- ln_attn_beta: float32 [4096], replicated
- ln_mlp_gamma: float32 [4096], replicated
- ln_mlp_beta: float32 [4096], replicated
- w_qkv: bfloat16 [4096, 8, 6, 128], P(None, 'tp')
- w_out: bfloat16 [8, 4, 128, 4096], P('tp')
- w_up: bfloat16 [4096, 16384], P(None, 'tp')
- w_down: bfloat16 [16384, 4096], P('tp')
- k_cache: bfloat16 [512, 8, 256, 128], P('dp', 'tp'), parts along dimension 0
- v_cache: bfloat16 [512, 8, 256, 128], P('dp', 'tp'), parts along dimension 0
- positions: int32 [512], P('dp'), parts along dimension 0
Outputs:
- output 1: bfloat16 [512, 4096], P('dp'), parts along dimension 0
- output 2: bfloat16 [512, 8, 256, 128], P('dp', 'tp'), parts along dimension 0
- output 3: bfloat16 [512, 8, 256, 128], P('dp', 'tp'), parts along dimension 0
There are 2 independent parts. The reference program is written for one: setup_inputs(seed, part) draws one part's arguments, and reference() takes and returns one part's arrays. A program takes and returns all parts, laid end to end along the dimension named above; an argument that names none is the same for every part.
All inputs are finite; a program needn't handle non-finite values.
Results may differ from the reference program's by a relative error of at most 0.0101396.
Values are sent between devices in bfloat16 or wider.
A program may use at most 1 GiB of HBM per device.

```python
import math
import jax
import jax.numpy as jnp
from jax import lax

D = 4096
GROUPS = 8
QPG = 4
HEAD = 128
FF = 16384
BATCH = 256
SEQ = 256

QKV_SLOTS = QPG + 2
HALF_HEAD = HEAD // 2
SCORE_SCALE = 1.0 / math.sqrt(HEAD)
LN_EPS = 1e-5
ROPE_BASE = 10000.0
NEG_BIG = -1e30


def setup_inputs(seed: int = 0, part: int = 0) -> dict:
    shared_key, part_base = jax.random.split(jax.random.key(seed))
    shared = jax.random.split(shared_key, 8)
    local = jax.random.split(jax.random.fold_in(part_base, part), 8)
    x = jax.random.normal(local[0], (BATCH, D), jnp.float32).astype(jnp.bfloat16)
    ln_attn_gamma = 1.0 + 0.3 * jax.random.normal(shared[0], (D,), jnp.float32)
    ln_attn_beta = 0.3 * jax.random.normal(shared[1], (D,), jnp.float32)
    ln_mlp_gamma = 1.0 + 0.3 * jax.random.normal(shared[2], (D,), jnp.float32)
    ln_mlp_beta = 0.3 * jax.random.normal(shared[3], (D,), jnp.float32)
    w_qkv = (jax.random.normal(shared[4], (D, GROUPS, QKV_SLOTS, HEAD), jnp.float32) * D ** -0.5).astype(jnp.bfloat16)
    w_out = (jax.random.normal(shared[5], (GROUPS, QPG, HEAD, D), jnp.float32) * (GROUPS * QPG * HEAD) ** -0.5).astype(jnp.bfloat16)
    w_up = (jax.random.normal(shared[6], (D, FF), jnp.float32) * D ** -0.5).astype(jnp.bfloat16)
    w_down = (jax.random.normal(shared[7], (FF, D), jnp.float32) * FF ** -0.5).astype(jnp.bfloat16)
    ramp = (2.0 * jnp.arange(SEQ, dtype=jnp.float32) / SEQ - 1.0)[None, None, :, None]
    k_slope = 1.5 * jax.random.normal(local[1], (BATCH, GROUPS, 1, HEAD), jnp.float32)
    k_cache = (jax.random.normal(local[2], (BATCH, GROUPS, SEQ, HEAD), jnp.float32) + ramp * k_slope).astype(jnp.bfloat16)
    v_level = jax.random.normal(local[3], (BATCH, GROUPS, 1, HEAD), jnp.float32)
    v_slope = jax.random.normal(local[4], (BATCH, GROUPS, 1, HEAD), jnp.float32)
    v_cache = (0.5 * jax.random.normal(local[5], (BATCH, GROUPS, SEQ, HEAD), jnp.float32) + v_level + ramp * v_slope).astype(jnp.bfloat16)
    positions = jax.random.randint(local[6], (BATCH,), SEQ // 4, SEQ, dtype=jnp.int32)
    positions = positions.at[0].set(SEQ - 1).at[1].set(SEQ // 4)
    return {'x': x, 'ln_attn_gamma': ln_attn_gamma, 'ln_attn_beta': ln_attn_beta, 'ln_mlp_gamma': ln_mlp_gamma, 'ln_mlp_beta': ln_mlp_beta, 'w_qkv': w_qkv, 'w_out': w_out, 'w_up': w_up, 'w_down': w_down, 'k_cache': k_cache, 'v_cache': v_cache, 'positions': positions}


def layer_norm(act_rows, ln_gamma, ln_beta):
    rows_f32 = act_rows.astype(jnp.float32)
    row_mean = jnp.mean(rows_f32, axis=-1, keepdims=True)
    centred = rows_f32 - row_mean
    row_var = jnp.mean(centred * centred, axis=-1, keepdims=True)
    return (centred * lax.rsqrt(row_var + LN_EPS) * ln_gamma + ln_beta).astype(jnp.bfloat16)


def apply_rotary(vectors, cos_t, sin_t):
    as_f32 = vectors.astype(jnp.float32)
    lower_half = as_f32[..., :HALF_HEAD]
    upper_half = as_f32[..., HALF_HEAD:]
    return jnp.concatenate([lower_half * cos_t - upper_half * sin_t, upper_half * cos_t + lower_half * sin_t], axis=-1).astype(jnp.bfloat16)


def reference(x, ln_attn_gamma, ln_attn_beta, ln_mlp_gamma, ln_mlp_beta, w_qkv, w_out, w_up, w_down, k_cache, v_cache, positions):
    attn_in = layer_norm(x, ln_attn_gamma, ln_attn_beta)
    mlp_in = layer_norm(x, ln_mlp_gamma, ln_mlp_beta)
    qkv_rows = jnp.dot(attn_in, w_qkv.reshape(D, GROUPS * QKV_SLOTS * HEAD), preferred_element_type=jnp.float32).astype(jnp.bfloat16)
    qkv_rows = qkv_rows.reshape(BATCH, GROUPS, QKV_SLOTS, HEAD)
    inv_freq = ROPE_BASE ** (-2.0 * jnp.arange(HALF_HEAD, dtype=jnp.float32) / HEAD)
    angles = positions.astype(jnp.float32)[:, None] * inv_freq[None, :]
    cos_t = jnp.cos(angles)
    sin_t = jnp.sin(angles)
    queries = apply_rotary(qkv_rows[:, :, :QPG], cos_t[:, None, None, :], sin_t[:, None, None, :])
    new_key = apply_rotary(qkv_rows[:, :, QPG], cos_t[:, None, :], sin_t[:, None, :])
    new_value = qkv_rows[:, :, QPG + 1]
    slot_ids = jnp.arange(SEQ)
    write_mask = (slot_ids[None, :] == positions[:, None])[:, None, :, None]
    keys_all = jnp.where(write_mask, new_key[:, :, None, :], k_cache)
    values_all = jnp.where(write_mask, new_value[:, :, None, :], v_cache)
    valid_mask = slot_ids[None, :] <= positions[:, None]

    def attend_group(operands):
        q_grp, k_grp, v_grp = operands
        scores = jnp.einsum('bqh,bsh->bqs', q_grp.astype(jnp.float32), k_grp.astype(jnp.float32)) * SCORE_SCALE
        scores = jnp.where(valid_mask[:, None, :], scores, NEG_BIG)
        attn_probs = jax.nn.softmax(scores, axis=-1).astype(jnp.bfloat16)
        return jnp.einsum('bqs,bsh->bqh', attn_probs.astype(jnp.float32), v_grp.astype(jnp.float32)).astype(jnp.bfloat16)

    context = lax.map(attend_group, (jnp.moveaxis(queries, 1, 0), jnp.moveaxis(keys_all, 1, 0), jnp.moveaxis(values_all, 1, 0)))
    context = jnp.moveaxis(context, 0, 1).reshape(BATCH, GROUPS * QPG * HEAD)
    attn_out = jnp.dot(context, w_out.reshape(GROUPS * QPG * HEAD, D), preferred_element_type=jnp.float32)
    hidden = jax.nn.gelu(jnp.dot(mlp_in, w_up, preferred_element_type=jnp.float32), approximate=False).astype(jnp.bfloat16)
    mlp_out = jnp.dot(hidden, w_down, preferred_element_type=jnp.float32)
    layer_out = (x.astype(jnp.float32) + attn_out + mlp_out).astype(jnp.bfloat16)
    return (layer_out, keys_all, values_all)
```

```python
import jax
import jax.numpy as jnp
from jax import lax
from jax.experimental import pallas as pl
from jax.experimental.pallas import tpu as pltpu
from jax.sharding import PartitionSpec as P

LN_EPS = 1e-5
ROPE_BASE = 10000.0
NEG_BIG = -1e30
BF16 = jnp.bfloat16
F32 = jnp.float32
ANY = pl.BlockSpec(memory_space=pl.ANY)


QKV_CHUNK = 512
QKV_SLOTS = 6
FF_BLOCK = 512
FF_SLOTS = 6
LN_ROWS = 16


def project_kernel(x_hbm, vec_hbm, rot_hbm, wq_hbm, wu_hbm, wd_hbm,
                   q_hbm, kv_hbm, m_hbm,
                   x_s, vec_s, rot_s, attn_s, mlp_s, hid_s, wq_s, wqf_s, acc_s, ring_s, q_s, kv_s, m_s,
                   in_sem, wq_sem, ring_sem, out_sem):
    rows, width = x_s.shape
    n_chunk = width // QKV_CHUNK
    lines = wq_hbm.shape[0] // width
    n_up = wu_hbm.shape[1] // FF_BLOCK
    n_down = wd_hbm.shape[1] // FF_BLOCK
    n_ff = n_up + n_down

    copies = [
        pltpu.make_async_copy(x_hbm, x_s, in_sem.at[0]),
        pltpu.make_async_copy(vec_hbm, vec_s, in_sem.at[1]),
        pltpu.make_async_copy(rot_hbm, rot_s, in_sem.at[2]),
    ]
    for c in copies:
        c.start()

    def wq_copy(c, slot):
        return pltpu.make_async_copy(wq_hbm.at[pl.ds(c * QKV_CHUNK * lines, QKV_CHUNK * lines), :], wq_s.at[slot], wq_sem.at[slot])

    quarter = width // 4

    def ff_start(w_hbm, b, slot):
        for p in range(4):
            pltpu.make_async_copy(w_hbm.at[pl.ds(p * quarter, quarter), pl.ds(b * FF_BLOCK, FF_BLOCK)],
                                  ring_s.at[slot, pl.ds(p * quarter, quarter), :], ring_sem.at[slot]).start()

    def ff_wait(slot):
        pltpu.make_async_copy(wu_hbm.at[:, pl.ds(0, FF_BLOCK)], ring_s.at[slot], ring_sem.at[slot]).wait()

    for c in range(QKV_SLOTS):
        wq_copy(c, c).start()
    for b in range(FF_SLOTS):
        ff_start(wu_hbm, b, b)

    for c in copies:
        c.wait()

    def ln_body(i, carry):
        r = pl.ds(pl.multiple_of(i * LN_ROWS, LN_ROWS), LN_ROWS)
        xf = x_s[r, :].astype(F32)
        mean = jnp.mean(xf, axis=-1, keepdims=True)
        cen = xf - mean
        var = jnp.mean(cen * cen, axis=-1, keepdims=True)
        nrm = cen * lax.rsqrt(var + LN_EPS)
        attn_s[r, :] = (nrm * vec_s[0:1, :] + vec_s[1:2, :]).astype(BF16)
        mlp_s[r, :] = (nrm * vec_s[2:3, :] + vec_s[3:4, :]).astype(BF16)
        return carry

    lax.fori_loop(0, rows // LN_ROWS, ln_body, 0)

    for c in range(n_chunk):
        slot = c % QKV_SLOTS
        wq_copy(c, slot).wait()
        wqf_s[...] = wq_s[slot].astype(F32)
        if c + QKV_SLOTS < n_chunk:
            wq_copy(c + QKV_SLOTS, slot).start()
        lhs = attn_s[:, c * QKV_CHUNK:(c + 1) * QKV_CHUNK]
        for pair in range(lines // 2):
            w = jnp.concatenate([wqf_s[pl.ds(2 * pair + e, QKV_CHUNK, stride=lines), :].astype(BF16) for e in range(2)], axis=1)
            part = jnp.dot(lhs, w, preferred_element_type=F32)
            if c == 0:
                acc_s[:, pair * 256:(pair + 1) * 256] = part
            else:
                acc_s[:, pair * 256:(pair + 1) * 256] += part

    cos_f = rot_s[:, 0:128]
    sin_f = rot_s[:, 128:256]
    n_slot = lines // 2
    n_q = n_slot - 2
    for j in range(n_slot):
        for g in range(2):
            col = (2 * j + g) * 128
            u = acc_s[:, col:col + 128].astype(BF16).astype(F32)
            if j < n_q + 1:
                u = (u * cos_f + pltpu.roll(u, 64, 1) * sin_f).astype(BF16).astype(F32)
            if j < n_q:
                q_s[pl.ds((g * n_q + j) * rows, rows), :] = u
            else:
                kv_s[pl.ds(((j - n_q) * 2 + g) * rows, rows), :] = u
    q_out = pltpu.make_async_copy(q_s, q_hbm, out_sem.at[0])
    kv_out = pltpu.make_async_copy(kv_s, kv_hbm, out_sem.at[1])
    q_out.start()
    kv_out.start()

    def up_body(b, carry):
        slot = lax.rem(b, FF_SLOTS)
        ff_wait(slot)
        pre = jnp.dot(mlp_s[...], ring_s[slot], preferred_element_type=F32)
        act = 0.5 * pre * (1.0 + lax.erf(pre * (0.5 ** 0.5)))
        hid_s[:, pl.ds(pl.multiple_of(b * FF_BLOCK, FF_BLOCK), FF_BLOCK)] = act.astype(BF16)
        nxt = b + FF_SLOTS

        @pl.when(nxt < n_up)
        def _():
            ff_start(wu_hbm, nxt, slot)

        @pl.when(nxt >= n_up)
        def _():
            ff_start(wd_hbm, nxt - n_up, slot)
        return carry

    lax.fori_loop(0, n_up, up_body, 0)

    def m_copy(b):
        cols = pl.ds(pl.multiple_of(b * FF_BLOCK, FF_BLOCK), FF_BLOCK)
        return pltpu.make_async_copy(m_s.at[:, cols], m_hbm.at[:, cols], out_sem.at[2])

    def down_body(b, carry):
        slot = lax.rem(b + n_up, FF_SLOTS)
        ff_wait(slot)
        m_s[:, pl.ds(pl.multiple_of(b * FF_BLOCK, FF_BLOCK), FF_BLOCK)] = jnp.dot(hid_s[...], ring_s[slot], preferred_element_type=F32)
        m_copy(b).start()
        nxt = b + FF_SLOTS

        @pl.when(nxt < n_down)
        def _():
            ff_start(wd_hbm, nxt, slot)
        return carry

    lax.fori_loop(0, n_down, down_body, 0)
    pltpu.make_async_copy(m_s, m_hbm, out_sem.at[2]).wait()
    q_out.wait()
    kv_out.wait()


def project(x, vecs, rot, wq, wu, wd):
    rows, width = x.shape
    hid = wu.shape[1]
    lines = wq.shape[0] // width
    n_head = (lines // 2 - 2) * 2
    return pl.pallas_call(
        project_kernel,
        name='project',
        in_specs=[ANY] * 6,
        out_specs=[ANY] * 3,
        out_shape=[
            jax.ShapeDtypeStruct((n_head * rows, 128), F32),
            jax.ShapeDtypeStruct((4 * rows, 128), F32),
            jax.ShapeDtypeStruct((rows, width), F32),
        ],
        scratch_shapes=[
            pltpu.VMEM((rows, width), BF16),
            pltpu.VMEM(vecs.shape, F32),
            pltpu.VMEM(rot.shape, F32),
            pltpu.VMEM((rows, width), BF16),
            pltpu.VMEM((rows, width), BF16),
            pltpu.VMEM((rows, hid), BF16),
            pltpu.VMEM((QKV_SLOTS, QKV_CHUNK * lines, 128), BF16),
            pltpu.VMEM((QKV_CHUNK * lines, 128), F32),
            pltpu.VMEM((rows, lines * 128), F32),
            pltpu.VMEM((FF_SLOTS, width, FF_BLOCK), BF16),
            pltpu.VMEM((n_head * rows, 128), F32),
            pltpu.VMEM((4 * rows, 128), F32),
            pltpu.VMEM((rows, width), F32),
            pltpu.SemaphoreType.DMA((3,)),
            pltpu.SemaphoreType.DMA((QKV_SLOTS,)),
            pltpu.SemaphoreType.DMA((FF_SLOTS,)),
            pltpu.SemaphoreType.DMA((3,)),
        ],
        compiler_params=pltpu.CompilerParams(vmem_limit_bytes=63 * 1024 * 1024),
        cost_estimate=pl.CostEstimate(flops=22 * 10 ** 9, bytes_accessed=90 * 10 ** 6, transcendentals=0),
    )(x, vecs, rot, wq, wu, wd)


ROW_BLOCK = 8
KV_SLOTS = 8
KV_AHEAD = 4
OUT_BLOCK = 512


def attend_kernel(row0, n_rows, pos_ref, core_ref, q_hbm, kv_hbm, m_hbm, wo_hbm, kc_hbm, vc_hbm, *rest):
    n_alias = 2 if row0 else 0
    ko_hbm, vo_hbm, send_hbm, keep_hbm = rest[n_alias:n_alias + 4]
    q_s, kv_s, m_s, wo_s, kbuf, vbuf, ctx_s, send_s, keep_s, kin_sem, vin_sem, kout_sem, vout_sem, sem = rest[n_alias + 4:]
    n_blk = n_rows // ROW_BLOCK
    total_rows = q_hbm.shape[0] // 8

    def block(ref, i):
        return ref.at[pl.ds(row0 + i * ROW_BLOCK, ROW_BLOCK)]

    def start_in(i, slot):
        pltpu.make_async_copy(block(kc_hbm, i), kbuf.at[slot], kin_sem.at[slot]).start()
        pltpu.make_async_copy(block(vc_hbm, i), vbuf.at[slot], vin_sem.at[slot]).start()

    def wait_in(slot):
        pltpu.make_async_copy(block(kc_hbm, 0), kbuf.at[slot], kin_sem.at[slot]).wait()
        pltpu.make_async_copy(block(vc_hbm, 0), vbuf.at[slot], vin_sem.at[slot]).wait()

    def start_out(i, slot):
        pltpu.make_async_copy(kbuf.at[slot], block(ko_hbm, i), kout_sem.at[slot]).start()
        pltpu.make_async_copy(vbuf.at[slot], block(vo_hbm, i), vout_sem.at[slot]).start()

    def wait_out(slot):
        pltpu.make_async_copy(kbuf.at[slot], block(ko_hbm, 0), kout_sem.at[slot]).wait()
        pltpu.make_async_copy(vbuf.at[slot], block(vo_hbm, 0), vout_sem.at[slot]).wait()

    q_in = pltpu.make_async_copy(q_hbm, q_s, sem.at[0])
    kv_in = pltpu.make_async_copy(kv_hbm, kv_s, sem.at[1])
    q_in.start()
    kv_in.start()
    for i in range(min(KV_AHEAD, n_blk)):
        start_in(i, i)
    wo_in = pltpu.make_async_copy(wo_hbm, wo_s, sem.at[2])
    m_in = pltpu.make_async_copy(m_hbm.at[pl.ds(row0, n_rows), :], m_s, sem.at[3])
    wo_in.start()
    m_in.start()
    q_in.wait()
    kv_in.wait()

    slot_ids = lax.broadcasted_iota(jnp.int32, (8, 256), 1)
    tile_ids = lax.broadcasted_iota(jnp.int32, (16, 128), 0)
    first = lax.broadcasted_iota(jnp.int32, (8, 128), 0) < 4
    scale = 128 ** -0.5

    def body(i, carry):
        slot = lax.rem(i, KV_SLOTS)
        nxt = i + KV_AHEAD

        @pl.when(nxt < n_blk)
        def _():
            nslot = lax.rem(nxt, KV_SLOTS)

            @pl.when(nxt >= KV_SLOTS)
            def _():
                wait_out(nslot)
            start_in(nxt, nslot)

        wait_in(slot)
        pos = [pos_ref[row0 + i * ROW_BLOCK + r] for r in range(ROW_BLOCK)]
        for r in range(ROW_BLOCK):
            base = pl.multiple_of((pos[r] // 16) * 16, 16)
            hit = tile_ids == pos[r] - base
            b = row0 + i * ROW_BLOCK + r
            for g in range(2):
                for buf, which in ((kbuf, 0), (vbuf, 1)):
                    new = kv_s[pl.ds((which * 2 + g) * total_rows + b, 1), :]
                    old = buf[slot, r, g, pl.ds(base, 16), :].astype(F32)
                    buf[slot, r, g, pl.ds(base, 16), :] = jnp.where(hit, new, old).astype(BF16)
        scores = []
        for r in range(ROW_BLOCK):
            b = row0 + i * ROW_BLOCK + r
            q = q_s[pl.ds(b, 8, stride=total_rows), :]
            zero = jnp.zeros_like(q)
            q2 = jnp.concatenate([jnp.where(first, q, zero), jnp.where(first, zero, q)], axis=1).astype(BF16)
            k2 = jnp.concatenate([kbuf[slot, r, 0], kbuf[slot, r, 1]], axis=1)
            s = lax.dot_general(q2, k2, (((1,), (1,)), ((), ())), preferred_element_type=F32) * scale
            scores.append(jnp.where(slot_ids <= pos[r], s, NEG_BIG))
        s = jnp.concatenate(scores, axis=0)
        e = jnp.exp(s - jnp.max(s, axis=-1, keepdims=True))
        p = (e / jnp.sum(e, axis=-1, keepdims=True)).astype(BF16)
        for r in range(ROW_BLOCK):
            v2 = jnp.concatenate([vbuf[slot, r, 0], vbuf[slot, r, 1]], axis=1)
            c = jnp.dot(p[8 * r:8 * r + 8], v2, preferred_element_type=F32)
            ctx_s[pl.ds(i * ROW_BLOCK + r, 8, stride=n_rows), :] = jnp.where(first, c[:, :128], c[:, 128:])
        start_out(i, slot)
        return carry

    lax.fori_loop(0, n_blk, body, 0)

    ctx = jnp.concatenate([ctx_s[pl.ds(h * n_rows, n_rows), :] for h in range(8)], axis=1).astype(BF16)
    wo_in.wait()
    m_in.wait()
    core = core_ref[0]
    half = m_s.shape[1] // 2

    def out_body(n, carry):
        dst = pl.ds(pl.multiple_of(n * OUT_BLOCK, OUT_BLOCK), OUT_BLOCK)
        for mine, stage, hbm in ((False, send_s, send_hbm), (True, keep_s, keep_hbm)):
            side = core if mine else 1 - core
            src = pl.ds(pl.multiple_of(side * half + n * OUT_BLOCK, OUT_BLOCK), OUT_BLOCK)
            part = jnp.dot(ctx, wo_s[:, src], preferred_element_type=F32) + m_s[:, src]
            stage[:, dst] = part.astype(stage.dtype)
            pltpu.make_async_copy(stage.at[:, dst], hbm.at[:, dst], sem.at[4 + mine]).start()
        return carry

    lax.fori_loop(0, half // OUT_BLOCK, out_body, 0)
    pltpu.make_async_copy(send_s, send_hbm, sem.at[4]).wait()
    pltpu.make_async_copy(keep_s, keep_hbm, sem.at[5]).wait()
    for i in range(max(0, n_blk - KV_SLOTS), n_blk):
        wait_out(i % KV_SLOTS)


def attend(row0, n_rows, pos, core, q, kv, m, wo, kc, vc, prev):
    import functools
    rows, width = m.shape
    n_in = 8
    alias = {} if prev is None else {n_in: 0, n_in + 1: 1}
    extra = () if prev is None else tuple(prev)
    smem = pl.BlockSpec(memory_space=pltpu.SMEM)
    return pl.pallas_call(
        functools.partial(attend_kernel, row0, n_rows),
        name='attend',
        in_specs=[smem, smem] + [ANY] * (6 + len(extra)),
        out_specs=[ANY] * 4,
        out_shape=[
            jax.ShapeDtypeStruct(kc.shape, BF16),
            jax.ShapeDtypeStruct(vc.shape, BF16),
            jax.ShapeDtypeStruct((n_rows, width // 2), BF16),
            jax.ShapeDtypeStruct((n_rows, width // 2), F32),
        ],
        input_output_aliases=alias,
        scratch_shapes=[
            pltpu.VMEM(q.shape, F32),
            pltpu.VMEM(kv.shape, F32),
            pltpu.VMEM((n_rows, width), F32),
            pltpu.VMEM(wo.shape, BF16),
            pltpu.VMEM((KV_SLOTS, ROW_BLOCK) + kc.shape[1:], BF16),
            pltpu.VMEM((KV_SLOTS, ROW_BLOCK) + vc.shape[1:], BF16),
            pltpu.VMEM((8 * n_rows, 128), F32),
            pltpu.VMEM((n_rows, width // 2), BF16),
            pltpu.VMEM((n_rows, width // 2), F32),
            pltpu.SemaphoreType.DMA((KV_SLOTS,)),
            pltpu.SemaphoreType.DMA((KV_SLOTS,)),
            pltpu.SemaphoreType.DMA((KV_SLOTS,)),
            pltpu.SemaphoreType.DMA((KV_SLOTS,)),
            pltpu.SemaphoreType.DMA((6,)),
        ],
        compiler_params=pltpu.CompilerParams(vmem_limit_bytes=63 * 1024 * 1024),
        cost_estimate=pl.CostEstimate(flops=10 ** 10 * n_rows // 256, bytes_accessed=140 * 10 ** 6 * n_rows // 256, transcendentals=0),
    )(pos, core, q, kv, m, wo, kc, vc, *extra)


CORE_SWAP = [(0, 1), (1, 0), (2, 3), (3, 2)]
CHIP_SWAP = [(0, 2), (2, 0), (1, 3), (3, 1)]
CHUNKS = (256,)


def solution(mesh):
    row_spec = P('dp', None)
    vec_spec = P(None)
    cache_spec = P('dp', 'tp', None, None)

    def device_step(x, ln_attn_gamma, ln_attn_beta, ln_mlp_gamma, ln_mlp_beta, w_qkv, w_out, w_up, w_down, k_cache, v_cache, positions):
        rows, width = x.shape
        core = lax.rem(lax.axis_index('tp'), 2)
        core_arr = core.astype(jnp.int32).reshape(1)
        vecs = jnp.stack([ln_attn_gamma, ln_attn_beta, ln_mlp_gamma, ln_mlp_beta])
        inv_freq = ROPE_BASE ** (-2.0 * jnp.arange(64, dtype=F32) / 128)
        angles = positions.astype(F32)[:, None] * inv_freq[None, :]
        cos_t, sin_t = jnp.cos(angles), jnp.sin(angles)
        rot = jnp.concatenate([cos_t, cos_t, -sin_t, sin_t], axis=1)
        wq = jnp.transpose(w_qkv, (0, 2, 1, 3)).reshape(-1, 128)
        wo = w_out.reshape(-1, width)
        q, kv, m = project(x, vecs, rot, wq, w_up, w_down)
        caches = None
        row0 = 0
        outs = []
        half = width // 2
        for n_rows in CHUNKS:
            ko, vo, send, keep = attend(row0, n_rows, positions, core_arr, q, kv, m, wo, k_cache, v_cache, caches)
            caches = (ko, vo)
            got = lax.ppermute(send, 'tp', CORE_SWAP)
            chip_sum = (keep + got.astype(F32)).astype(BF16)
            other = lax.ppermute(chip_sum, 'tp', CHIP_SWAP)
            x_half = lax.dynamic_slice(x[row0:row0 + n_rows], (0, core * half), (n_rows, half))
            mine = (x_half.astype(F32) + (chip_sum.astype(F32) + other.astype(F32))).astype(BF16)
            partner = lax.ppermute(mine, 'tp', CORE_SWAP)
            is0 = core == 0
            outs.append(jnp.concatenate([jnp.where(is0, mine, partner), jnp.where(is0, partner, mine)], axis=1))
            row0 += n_rows
        out = outs[0] if len(outs) == 1 else jnp.concatenate(outs, axis=0)
        return out, caches[0], caches[1]

    return jax.shard_map(device_step, mesh=mesh, in_specs=(row_spec, vec_spec, vec_spec, vec_spec, vec_spec, P(None, 'tp', None, None), P('tp', None, None, None), P(None, 'tp'), P('tp', None), cache_spec, cache_spec, P('dp')), out_specs=(row_spec, cache_spec, cache_spec), check_vma=False)
```

```python
import jax
import jax.numpy as jnp
import numpy as np
from jax import lax
from jax.experimental import pallas as pl
from jax.experimental.pallas import tpu as pltpu
from jax.sharding import PartitionSpec as P

LN_EPS = 1e-5
ROPE_BASE = 10000.0
NEG_BIG = -1e30
BF16 = jnp.bfloat16
F32 = jnp.float32
ANY = pl.BlockSpec(memory_space=pl.ANY)
SMEM = pl.BlockSpec(memory_space=pltpu.SMEM)
MIB = 1024 * 1024

QKV_CHUNK = 512
LN_ROWS = 16
ROW_BLOCK = 8
SUB_BLOCKS = 2
KV_SLOTS = 12
KV_AHEAD = 8
UP_SLOTS = 3


def front_kernel(pos_ref, x_hbm, ga_hbm, ba_hbm, gm_hbm, bm_hbm, freq_hbm, wq_hbm, wu_hbm, kc_hbm, vc_hbm,
                 ko_hbm, vo_hbm, hid_hbm, ctx_hbm,
                 x_s, vec_s, freq_s, cos_s, sin_s, attn_s, mlp_s, wq_s, wqf_s, acc_s, q_s, kv_s, up_s, hid_s, ctx_s, kbuf, vbuf,
                 in_sem, wq_sem, up_sem, kin_sem, vin_sem, kout_sem, vout_sem, out_sem):
    rows, width = x_s.shape
    n_chunk = width // QKV_CHUNK
    lines = wq_hbm.shape[0] // width
    up_cols = up_s.shape[2]
    n_up = wu_hbm.shape[1] // up_cols
    n_blk = rows // ROW_BLOCK

    small = [pltpu.make_async_copy(x_hbm, x_s, in_sem.at[0])]
    for i, v in enumerate((ga_hbm, ba_hbm, gm_hbm, bm_hbm)):
        small.append(pltpu.make_async_copy(v, vec_s.at[pl.ds(i, 1), :], in_sem.at[1 + i]))
    freq_in = pltpu.make_async_copy(freq_hbm, freq_s, in_sem.at[5])
    freq_in.start()
    for c in small:
        c.start()

    def wq_copy(c):
        return pltpu.make_async_copy(wq_hbm.at[pl.ds(c * QKV_CHUNK * lines, QKV_CHUNK * lines), :], wq_s.at[c], wq_sem.at[c])

    def up_copy(b, slot):
        return pltpu.make_async_copy(wu_hbm.at[:, pl.ds(pl.multiple_of(b * up_cols, up_cols), up_cols)], up_s.at[slot], up_sem.at[slot])

    def block(ref, i):
        return ref.at[pl.ds(i * ROW_BLOCK, ROW_BLOCK)]

    def start_in(i, slot):
        pltpu.make_async_copy(block(kc_hbm, i), kbuf.at[slot], kin_sem.at[slot]).start()
        pltpu.make_async_copy(block(vc_hbm, i), vbuf.at[slot], vin_sem.at[slot]).start()

    def wait_in(slot):
        pltpu.make_async_copy(block(kc_hbm, 0), kbuf.at[slot], kin_sem.at[slot]).wait()
        pltpu.make_async_copy(block(vc_hbm, 0), vbuf.at[slot], vin_sem.at[slot]).wait()

    def start_out(i, slot):
        pltpu.make_async_copy(kbuf.at[slot], block(ko_hbm, i), kout_sem.at[slot]).start()
        pltpu.make_async_copy(vbuf.at[slot], block(vo_hbm, i), vout_sem.at[slot]).start()

    def wait_out(slot):
        pltpu.make_async_copy(kbuf.at[slot], block(ko_hbm, 0), kout_sem.at[slot]).wait()
        pltpu.make_async_copy(vbuf.at[slot], block(vo_hbm, 0), vout_sem.at[slot]).wait()

    for c in range(n_chunk):
        wq_copy(c).start()
    for b in range(UP_SLOTS):
        up_copy(b, b).start()
    for i in range(KV_AHEAD):
        start_in(i, i)

    freq_in.wait()

    def angle_body(b, carry):
        cos_s[pl.ds(b, 1), :] = pos_ref[b].astype(F32) * freq_s[0:1, :]
        return carry

    lax.fori_loop(0, rows, angle_body, 0, unroll=8)
    ang = cos_s[...]
    low = lax.broadcasted_iota(jnp.int32, ang.shape, 1) < 64
    sin_t = jnp.sin(ang)
    sin_s[...] = jnp.where(low, -sin_t, sin_t)
    cos_s[...] = jnp.cos(ang)

    for c in small:
        c.wait()

    def ln_body(i, carry):
        r = pl.ds(pl.multiple_of(i * LN_ROWS, LN_ROWS), LN_ROWS)
        xf = x_s[r, :].astype(F32)
        mean = jnp.mean(xf, axis=-1, keepdims=True)
        cen = xf - mean
        var = jnp.mean(cen * cen, axis=-1, keepdims=True)
        nrm = cen * lax.rsqrt(var + LN_EPS)
        attn_s[r, :] = (nrm * vec_s[0:1, :] + vec_s[1:2, :]).astype(BF16)
        mlp_s[r, :] = (nrm * vec_s[2:3, :] + vec_s[3:4, :]).astype(BF16)
        return carry

    lax.fori_loop(0, rows // LN_ROWS, ln_body, 0)

    for c in range(n_chunk):
        wq_copy(c).wait()
        wqf_s[...] = wq_s[c].astype(F32)
        lhs = attn_s[:, c * QKV_CHUNK:(c + 1) * QKV_CHUNK]
        for pair in range(lines // 2):
            w = jnp.concatenate([wqf_s[pl.ds(2 * pair + e, QKV_CHUNK, stride=lines), :].astype(BF16) for e in range(2)], axis=1)
            part = jnp.dot(lhs, w, preferred_element_type=F32)
            if c == 0:
                acc_s[:, pair * 256:(pair + 1) * 256] = part
            else:
                acc_s[:, pair * 256:(pair + 1) * 256] += part

    n_slot = lines // 2
    n_q = n_slot - 2
    for j in range(n_slot):
        for g in range(2):
            col = (2 * j + g) * 128
            u = acc_s[:, col:col + 128].astype(BF16).astype(F32)
            if j < n_q + 1:
                u = (u * cos_s[...] + pltpu.roll(u, 64, 1) * sin_s[...]).astype(BF16).astype(F32)
            if j < n_q:
                q_s[pl.ds((g * n_q + j) * rows, rows), :] = u
            else:
                kv_s[pl.ds(((j - n_q) * 2 + g) * rows, rows), :] = u

    slot_ids = lax.broadcasted_iota(jnp.int32, (8, 256), 1)
    tile_ids = lax.broadcasted_iota(jnp.int32, (16, 128), 0)
    first = lax.broadcasted_iota(jnp.int32, (8, 128), 0) < 4
    scale = 128 ** -0.5

    def attend_block(i, slot):
        pos = [pos_ref[i * ROW_BLOCK + r] for r in range(ROW_BLOCK)]
        for r in range(ROW_BLOCK):
            base = pl.multiple_of((pos[r] // 16) * 16, 16)
            hit = tile_ids == pos[r] - base
            b = i * ROW_BLOCK + r
            for g in range(2):
                for buf, which in ((kbuf, 0), (vbuf, 1)):
                    new = kv_s[pl.ds((which * 2 + g) * rows + b, 1), :]
                    old = buf[slot, r, g, pl.ds(base, 16), :].astype(F32)
                    buf[slot, r, g, pl.ds(base, 16), :] = jnp.where(hit, new, old).astype(BF16)
        scores = []
        for r in range(ROW_BLOCK):
            b = i * ROW_BLOCK + r
            q = q_s[pl.ds(b, 8, stride=rows), :]
            zero = jnp.zeros_like(q)
            q2 = jnp.concatenate([jnp.where(first, q, zero), jnp.where(first, zero, q)], axis=1).astype(BF16)
            k2 = jnp.concatenate([kbuf[slot, r, 0], kbuf[slot, r, 1]], axis=1)
            s = lax.dot_general(q2, k2, (((1,), (1,)), ((), ())), preferred_element_type=F32) * scale
            scores.append(jnp.where(slot_ids <= pos[r], s, NEG_BIG))
        s = jnp.concatenate(scores, axis=0)
        e = jnp.exp(s - jnp.max(s, axis=-1, keepdims=True))
        p = (e / jnp.sum(e, axis=-1, keepdims=True)).astype(BF16)
        for r in range(ROW_BLOCK):
            v2 = jnp.concatenate([vbuf[slot, r, 0], vbuf[slot, r, 1]], axis=1)
            c = jnp.dot(p[8 * r:8 * r + 8], v2, preferred_element_type=F32)
            ctx_s[pl.ds(i * ROW_BLOCK + r, 8, stride=rows), :] = jnp.where(first, c[:, :128], c[:, 128:])

    def hid_copy(i):
        cols = pl.ds(pl.multiple_of(i * up_cols, up_cols), up_cols)
        return pltpu.make_async_copy(hid_s.at[:, cols], hid_hbm.at[:, cols], out_sem.at[0])

    def body(i, carry):
        for s in range(SUB_BLOCKS):
            nxt = i * SUB_BLOCKS + s + KV_AHEAD

            @pl.when(nxt < n_blk)
            def _():
                nslot = lax.rem(nxt, KV_SLOTS)

                @pl.when(nxt >= KV_SLOTS)
                def _():
                    wait_out(nslot)
                start_in(nxt, nslot)

        @pl.when((i >= 1) & (i - 1 + UP_SLOTS < n_up))
        def _():
            up_copy(i - 1 + UP_SLOTS, lax.rem(i - 1, UP_SLOTS)).start()

        uslot = lax.rem(i, UP_SLOTS)
        up_copy(0, uslot).wait()
        pre = jnp.dot(mlp_s[...], up_s[uslot], preferred_element_type=F32)
        act = 0.5 * pre * (1.0 + lax.erf(pre * (0.5 ** 0.5)))
        hid_s[:, pl.ds(pl.multiple_of(i * up_cols, up_cols), up_cols)] = act.astype(BF16)
        for s in range(SUB_BLOCKS):
            blk = i * SUB_BLOCKS + s
            slot = lax.rem(blk, KV_SLOTS)
            wait_in(slot)
            attend_block(blk, slot)
            start_out(blk, slot)
        hid_copy(i).start()
        return carry

    lax.fori_loop(0, n_up, body, 0)
    ctx_out = pltpu.make_async_copy(ctx_s, ctx_hbm, out_sem.at[1])
    ctx_out.start()
    pltpu.make_async_copy(hid_s, hid_hbm, out_sem.at[0]).wait()
    ctx_out.wait()
    for i in range(n_blk - KV_SLOTS, n_blk):
        wait_out(i % KV_SLOTS)


def front(pos, x, ga, ba, gm, bm, freq, wq, wu, kc, vc):
    rows, width = x.shape
    hid = wu.shape[1]
    lines = wq.shape[0] // width
    n_head = (lines // 2 - 2) * 2
    up_cols = hid // (rows // (ROW_BLOCK * SUB_BLOCKS))
    return pl.pallas_call(
        front_kernel,
        name='front',
        in_specs=[SMEM] + [ANY] * 10,
        out_specs=[ANY] * 4,
        out_shape=[
            jax.ShapeDtypeStruct(kc.shape, BF16),
            jax.ShapeDtypeStruct(vc.shape, BF16),
            jax.ShapeDtypeStruct((rows, hid), BF16),
            jax.ShapeDtypeStruct((n_head * rows, 128), F32),
        ],
        scratch_shapes=[
            pltpu.VMEM((rows, width), BF16),
            pltpu.VMEM((4, width), F32),
            pltpu.VMEM((1, 128), F32),
            pltpu.VMEM((rows, 128), F32),
            pltpu.VMEM((rows, 128), F32),
            pltpu.VMEM((rows, width), BF16),
            pltpu.VMEM((rows, width), BF16),
            pltpu.VMEM((width // QKV_CHUNK, QKV_CHUNK * lines, 128), BF16),
            pltpu.VMEM((QKV_CHUNK * lines, 128), F32),
            pltpu.VMEM((rows, lines * 128), F32),
            pltpu.VMEM((n_head * rows, 128), F32),
            pltpu.VMEM((4 * rows, 128), F32),
            pltpu.VMEM((UP_SLOTS, width, up_cols), BF16),
            pltpu.VMEM((rows, hid), BF16),
            pltpu.VMEM((n_head * rows, 128), F32),
            pltpu.VMEM((KV_SLOTS, ROW_BLOCK) + kc.shape[1:], BF16),
            pltpu.VMEM((KV_SLOTS, ROW_BLOCK) + vc.shape[1:], BF16),
            pltpu.SemaphoreType.DMA((6,)),
            pltpu.SemaphoreType.DMA((width // QKV_CHUNK,)),
            pltpu.SemaphoreType.DMA((UP_SLOTS,)),
            pltpu.SemaphoreType.DMA((KV_SLOTS,)),
            pltpu.SemaphoreType.DMA((KV_SLOTS,)),
            pltpu.SemaphoreType.DMA((KV_SLOTS,)),
            pltpu.SemaphoreType.DMA((KV_SLOTS,)),
            pltpu.SemaphoreType.DMA((2,)),
        ],
        compiler_params=pltpu.CompilerParams(vmem_limit_bytes=63 * MIB),
        cost_estimate=pl.CostEstimate(flops=22 * 10 ** 9, bytes_accessed=180 * 10 ** 6, transcendentals=0),
    )(pos, x, ga, ba, gm, bm, freq, wq, wu, kc, vc)


PIECES = 8
MESH = pl.DeviceIdType.MESH


def exchange_kernel(x_hbm, hid_hbm, ctx_hbm, wd_hbm, wo_hbm, out_hbm,
                    x_s, hid_s, ctx_s, lhs_s, wd_s, wo_s, send_s, recv_s, keep_s, sum_s, other_s, out_s,
                    in_sem, wd_sem, wo_sem, c1_send, c1_recv, c2_send, c2_recv, c3_send, c3_recv, out_sem):
    rows, width = x_s.shape
    half = width // 2
    cols = half // PIECES
    heads = ctx_s.shape[0] // rows
    me = lax.axis_index('tp')
    core = lax.rem(me, 2)
    mate = me + 1 - 2 * core
    far = lax.rem(me + 2, 4)

    loads = [pltpu.make_async_copy(a, b, in_sem.at[i]) for i, (a, b) in enumerate(((hid_hbm, hid_s), (ctx_hbm, ctx_s), (x_hbm, x_s)))]
    for c in loads[:2]:
        c.start()

    def col_of(p, part):
        side = core if part else 1 - core
        return pl.multiple_of(side * half + p * cols, cols)

    def wd_copy(p, part):
        return pltpu.make_async_copy(wd_hbm.at[:, pl.ds(col_of(p, part), cols)], wd_s.at[2 * p + part], wd_sem.at[2 * p + part])

    def wo_copy(p, part):
        return pltpu.make_async_copy(wo_hbm.at[:, pl.ds(col_of(p, part), cols)], wo_s.at[2 * p + part], wo_sem.at[2 * p + part])

    for p in range(PIECES):
        for part in range(2):
            wd_copy(p, part).start()
            wo_copy(p, part).start()
        if p == 0:
            loads[2].start()

    barrier = pltpu.get_barrier_semaphore()
    for peer in (mate, far):
        pl.semaphore_signal(barrier, inc=1, device_id={'tp': peer}, device_id_type=MESH)
    pl.semaphore_wait(barrier, 2)

    def copy1(p):
        return pltpu.make_async_remote_copy(send_s.at[p], recv_s.at[p], c1_send.at[p], c1_recv.at[p], device_id={'tp': mate}, device_id_type=MESH)

    def copy2(p):
        return pltpu.make_async_remote_copy(sum_s.at[p], other_s.at[p], c2_send.at[p], c2_recv.at[p], device_id={'tp': far}, device_id_type=MESH)

    def copy3(p, side):
        view = out_s.at[side * PIECES + p]
        return pltpu.make_async_remote_copy(view, view, c3_send.at[p], c3_recv.at[p], device_id={'tp': mate}, device_id_type=MESH)

    loads[0].wait()
    loads[1].wait()
    for h in range(heads):
        lhs_s[:, h * 128:(h + 1) * 128] = ctx_s[h * rows:(h + 1) * rows, :].astype(BF16)

    def partial(p, part):
        wd_copy(p, part).wait()
        wo_copy(p, part).wait()
        return jnp.dot(lhs_s[...], wo_s[2 * p + part], preferred_element_type=F32) + jnp.dot(hid_s[...], wd_s[2 * p + part], preferred_element_type=F32)

    def chip_sum(p):
        copy1(p).wait_recv()
        sum_s[p] = (keep_s[p] + recv_s[p].astype(F32)).astype(BF16)
        copy2(p).start()

    def compute(p, carry):
        send_s[p] = partial(p, 0).astype(BF16)
        copy1(p).start()
        keep_s[p] = partial(p, 1)
        chip_sum(p)
        return carry

    lax.fori_loop(0, PIECES, compute, 0)
    loads[2].wait()

    def out_copy(p, side):
        k = side * PIECES + p
        return pltpu.make_async_copy(out_s.at[k], out_hbm.at[:, pl.ds(pl.multiple_of(k * cols, cols), cols)], out_sem.at[k])

    def finish(p, carry):
        copy2(p).wait_recv()
        xs = x_s[:, pl.ds(col_of(p, 1), cols)].astype(F32)
        out_s[core * PIECES + p] = (xs + (sum_s[p].astype(F32) + other_s[p].astype(F32))).astype(BF16)
        copy3(p, core).start()
        out_copy(p, core).start()
        return carry

    lax.fori_loop(0, PIECES, finish, 0)

    def collect(p, carry):
        copy3(p, 1 - core).wait_recv()
        out_copy(p, 1 - core).start()
        return carry

    lax.fori_loop(0, PIECES, collect, 0)

    def drain(p, carry):
        copy1(p).wait_send()
        copy2(p).wait_send()
        copy3(p, core).wait_send()
        out_copy(p, core).wait()
        out_copy(p, 1 - core).wait()
        return carry

    lax.fori_loop(0, PIECES, drain, 0)


def exchange(x, hid, ctx, wd, wo):
    rows, width = x.shape
    cols = width // 2 // PIECES
    n_ff = hid.shape[1]
    n_ctx = wo.shape[0]
    dma = pltpu.SemaphoreType.DMA
    return pl.pallas_call(
        exchange_kernel,
        name='exchange',
        in_specs=[ANY] * 5,
        out_specs=ANY,
        out_shape=jax.ShapeDtypeStruct((rows, width), BF16),
        scratch_shapes=[
            pltpu.VMEM((rows, width), BF16),
            pltpu.VMEM((rows, n_ff), BF16),
            pltpu.VMEM(ctx.shape, F32),
            pltpu.VMEM((rows, n_ctx), BF16),
            pltpu.VMEM((2 * PIECES, n_ff, cols), BF16),
            pltpu.VMEM((2 * PIECES, n_ctx, cols), BF16),
            pltpu.VMEM((PIECES, rows, cols), BF16),
            pltpu.VMEM((PIECES, rows, cols), BF16),
            pltpu.VMEM((PIECES, rows, cols), F32),
            pltpu.VMEM((PIECES, rows, cols), BF16),
            pltpu.VMEM((PIECES, rows, cols), BF16),
            pltpu.VMEM((2 * PIECES, rows, cols), BF16),
            dma((3,)), dma((2 * PIECES,)), dma((2 * PIECES,)),
            dma((PIECES,)), dma((PIECES,)), dma((PIECES,)), dma((PIECES,)), dma((PIECES,)), dma((PIECES,)),
            dma((2 * PIECES,)),
        ],
        compiler_params=pltpu.CompilerParams(vmem_limit_bytes=63 * MIB, collective_id=0, has_side_effects=True),
        cost_estimate=pl.CostEstimate(flops=11 * 10 ** 9, bytes_accessed=48 * 10 ** 6, transcendentals=0),
    )(x, hid, ctx, wd, wo)


def solution(mesh):
    row_spec = P('dp', None)
    vec_spec = P(None)
    cache_spec = P('dp', 'tp', None, None)

    def device_step(x, ln_attn_gamma, ln_attn_beta, ln_mlp_gamma, ln_mlp_beta, w_qkv, w_out, w_up, w_down, k_cache, v_cache, positions):
        width = x.shape[1]
        head = w_qkv.shape[3]
        inv_freq = ROPE_BASE ** (-2.0 * np.arange(head // 2) / head)
        freq = jnp.asarray(np.concatenate([inv_freq, inv_freq])[None, :], F32)
        vecs = [v.reshape(1, width) for v in (ln_attn_gamma, ln_attn_beta, ln_mlp_gamma, ln_mlp_beta)]
        wq = jnp.transpose(w_qkv, (0, 2, 1, 3)).reshape(-1, head)
        ko, vo, hid, ctx = front(positions, x, *vecs, freq, wq, w_up, k_cache, v_cache)
        out = exchange(x, hid, ctx, w_down, w_out.reshape(-1, width))
        return out, ko, vo

    return jax.shard_map(device_step, mesh=mesh, in_specs=(row_spec, vec_spec, vec_spec, vec_spec, vec_spec, P(None, 'tp', None, None), P('tp', None, None, None), P(None, 'tp'), P('tp', None), cache_spec, cache_spec, P('dp')), out_specs=(row_spec, cache_spec, cache_spec), check_vma=False)
```

```python
import jax
import jax.numpy as jnp
import numpy as np
from jax import lax
from jax.experimental import pallas as pl
from jax.experimental.pallas import tpu as pltpu
from jax.sharding import PartitionSpec as P

LN_EPS = 1e-5
ROPE_BASE = 10000.0
NEG_BIG = -1e30
BF16 = jnp.bfloat16
F32 = jnp.float32
ANY = pl.BlockSpec(memory_space=pl.ANY)
SMEM = pl.BlockSpec(memory_space=pltpu.SMEM)
MIB = 1024 * 1024

QKV_CHUNK = 512
LN_ROWS = 16
ROW_BLOCK = 8
SUB_BLOCKS = 2
KV_SLOTS = 12
KV_AHEAD = 8
UP_SLOTS = 3


def front_kernel(pos_ref, x_hbm, ga_hbm, ba_hbm, gm_hbm, bm_hbm, freq_hbm, wq_hbm, wu_hbm, kc_hbm, vc_hbm,
                 ko_hbm, vo_hbm, hid_hbm, ctx_hbm,
                 x_s, vec_s, freq_s, cos_s, sin_s, attn_s, mlp_s, wq_s, wqf_s, acc_s, q_s, kv_s, up_s, hid_s, ctx_s, kbuf, vbuf,
                 in_sem, wq_sem, up_sem, kin_sem, vin_sem, kout_sem, vout_sem, out_sem):
    rows, width = x_s.shape
    n_chunk = width // QKV_CHUNK
    lines = wq_hbm.shape[0] // width
    up_cols = up_s.shape[2]
    n_up = wu_hbm.shape[1] // up_cols
    n_blk = rows // ROW_BLOCK

    small = [pltpu.make_async_copy(x_hbm, x_s, in_sem.at[0])]
    for i, v in enumerate((ga_hbm, ba_hbm, gm_hbm, bm_hbm)):
        small.append(pltpu.make_async_copy(v, vec_s.at[pl.ds(i, 1), :], in_sem.at[1 + i]))
    freq_in = pltpu.make_async_copy(freq_hbm, freq_s, in_sem.at[5])
    freq_in.start()
    for c in small:
        c.start()

    def wq_copy(c):
        return pltpu.make_async_copy(wq_hbm.at[pl.ds(c * QKV_CHUNK * lines, QKV_CHUNK * lines), :], wq_s.at[c], wq_sem.at[c])

    def up_copy(b, slot):
        return pltpu.make_async_copy(wu_hbm.at[:, pl.ds(pl.multiple_of(b * up_cols, up_cols), up_cols)], up_s.at[slot], up_sem.at[slot])

    def block(ref, i):
        return ref.at[pl.ds(i * ROW_BLOCK, ROW_BLOCK)]

    def start_in(i, slot):
        pltpu.make_async_copy(block(kc_hbm, i), kbuf.at[slot], kin_sem.at[slot]).start()
        pltpu.make_async_copy(block(vc_hbm, i), vbuf.at[slot], vin_sem.at[slot]).start()

    def wait_in(slot):
        pltpu.make_async_copy(block(kc_hbm, 0), kbuf.at[slot], kin_sem.at[slot]).wait()
        pltpu.make_async_copy(block(vc_hbm, 0), vbuf.at[slot], vin_sem.at[slot]).wait()

    def start_out(i, slot):
        pltpu.make_async_copy(kbuf.at[slot], block(ko_hbm, i), kout_sem.at[slot]).start()
        pltpu.make_async_copy(vbuf.at[slot], block(vo_hbm, i), vout_sem.at[slot]).start()

    def wait_out(slot):
        pltpu.make_async_copy(kbuf.at[slot], block(ko_hbm, 0), kout_sem.at[slot]).wait()
        pltpu.make_async_copy(vbuf.at[slot], block(vo_hbm, 0), vout_sem.at[slot]).wait()

    wq_copy(0).start()
    wq_copy(1).start()

    freq_in.wait()

    def angle_body(b, carry):
        cos_s[pl.ds(b, 1), :] = pos_ref[b].astype(F32) * freq_s[0:1, :]
        return carry

    lax.fori_loop(0, rows, angle_body, 0, unroll=8)
    ang = cos_s[...]
    low = lax.broadcasted_iota(jnp.int32, ang.shape, 1) < 64
    sin_t = jnp.sin(ang)
    sin_s[...] = jnp.where(low, -sin_t, sin_t)
    cos_s[...] = jnp.cos(ang)

    for c in small:
        c.wait()
    wq_copy(2).start()
    wq_copy(3).start()

    def ln_body(i, carry):
        r = pl.ds(pl.multiple_of(i * LN_ROWS, LN_ROWS), LN_ROWS)
        xf = x_s[r, :].astype(F32)
        mean = jnp.mean(xf, axis=-1, keepdims=True)
        cen = xf - mean
        var = jnp.mean(cen * cen, axis=-1, keepdims=True)
        nrm = cen * lax.rsqrt(var + LN_EPS)
        attn_s[r, :] = (nrm * vec_s[0:1, :] + vec_s[1:2, :]).astype(BF16)
        mlp_s[r, :] = (nrm * vec_s[2:3, :] + vec_s[3:4, :]).astype(BF16)
        return carry

    half_ln = rows // LN_ROWS // 2
    lax.fori_loop(0, half_ln, ln_body, 0)
    for c in range(4, n_chunk):
        wq_copy(c).start()
    lax.fori_loop(half_ln, 2 * half_ln, ln_body, 0)

    for c in range(n_chunk):
        wq_copy(c).wait()
        start_in(c, c)
        if c >= n_chunk - UP_SLOTS:
            up_copy(c - n_chunk + UP_SLOTS, c - n_chunk + UP_SLOTS).start()
        wqf_s[...] = wq_s[c].astype(F32)
        lhs = attn_s[:, c * QKV_CHUNK:(c + 1) * QKV_CHUNK]
        for pair in range(lines // 2):
            w = jnp.concatenate([wqf_s[pl.ds(2 * pair + e, QKV_CHUNK, stride=lines), :].astype(BF16) for e in range(2)], axis=1)
            part = jnp.dot(lhs, w, preferred_element_type=F32)
            if c == 0:
                acc_s[:, pair * 256:(pair + 1) * 256] = part
            else:
                acc_s[:, pair * 256:(pair + 1) * 256] += part

    n_slot = lines // 2
    n_q = n_slot - 2
    for j in range(n_slot):
        for g in range(2):
            col = (2 * j + g) * 128
            u = acc_s[:, col:col + 128].astype(BF16).astype(F32)
            if j < n_q + 1:
                u = (u * cos_s[...] + pltpu.roll(u, 64, 1) * sin_s[...]).astype(BF16).astype(F32)
            if j < n_q:
                q_s[pl.ds((g * n_q + j) * rows, rows), :] = u
            else:
                kv_s[pl.ds(((j - n_q) * 2 + g) * rows, rows), :] = u

    slot_ids = lax.broadcasted_iota(jnp.int32, (8, 256), 1)
    tile_ids = lax.broadcasted_iota(jnp.int32, (16, 128), 0)
    first = lax.broadcasted_iota(jnp.int32, (8, 128), 0) < 4
    scale = 128 ** -0.5

    def attend_block(i, slot):
        pos = [pos_ref[i * ROW_BLOCK + r] for r in range(ROW_BLOCK)]
        for r in range(ROW_BLOCK):
            base = pl.multiple_of((pos[r] // 16) * 16, 16)
            hit = tile_ids == pos[r] - base
            b = i * ROW_BLOCK + r
            for g in range(2):
                for buf, which in ((kbuf, 0), (vbuf, 1)):
                    new = kv_s[pl.ds((which * 2 + g) * rows + b, 1), :]
                    old = buf[slot, r, g, pl.ds(base, 16), :].astype(F32)
                    buf[slot, r, g, pl.ds(base, 16), :] = jnp.where(hit, new, old).astype(BF16)
        scores = []
        for r in range(ROW_BLOCK):
            b = i * ROW_BLOCK + r
            q = q_s[pl.ds(b, 8, stride=rows), :]
            zero = jnp.zeros_like(q)
            q2 = jnp.concatenate([jnp.where(first, q, zero), jnp.where(first, zero, q)], axis=1).astype(BF16)
            k2 = jnp.concatenate([kbuf[slot, r, 0], kbuf[slot, r, 1]], axis=1)
            s = lax.dot_general(q2, k2, (((1,), (1,)), ((), ())), preferred_element_type=F32) * scale
            scores.append(jnp.where(slot_ids <= pos[r], s, NEG_BIG))
        s = jnp.concatenate(scores, axis=0)
        e = jnp.exp(s - jnp.max(s, axis=-1, keepdims=True))
        p = (e / jnp.sum(e, axis=-1, keepdims=True)).astype(BF16)
        for r in range(ROW_BLOCK):
            v2 = jnp.concatenate([vbuf[slot, r, 0], vbuf[slot, r, 1]], axis=1)
            c = jnp.dot(p[8 * r:8 * r + 8], v2, preferred_element_type=F32)
            ctx_s[pl.ds(i * ROW_BLOCK + r, 8, stride=rows), :] = jnp.where(first, c[:, :128], c[:, 128:])

    def hid_copy(i):
        cols = pl.ds(pl.multiple_of(i * up_cols, up_cols), up_cols)
        return pltpu.make_async_copy(hid_s.at[:, cols], hid_hbm.at[:, cols], out_sem.at[0])

    def body(i, carry):
        for s in range(SUB_BLOCKS):
            nxt = i * SUB_BLOCKS + s + KV_AHEAD

            @pl.when(nxt < n_blk)
            def _():
                nslot = lax.rem(nxt, KV_SLOTS)

                @pl.when(nxt >= KV_SLOTS)
                def _():
                    wait_out(nslot)
                start_in(nxt, nslot)

        @pl.when((i >= 1) & (i - 1 + UP_SLOTS < n_up))
        def _():
            up_copy(i - 1 + UP_SLOTS, lax.rem(i - 1, UP_SLOTS)).start()

        uslot = lax.rem(i, UP_SLOTS)
        up_copy(0, uslot).wait()
        pre = jnp.dot(mlp_s[...], up_s[uslot], preferred_element_type=F32)
        act = 0.5 * pre * (1.0 + lax.erf(pre * (0.5 ** 0.5)))
        hid_s[:, pl.ds(pl.multiple_of(i * up_cols, up_cols), up_cols)] = act.astype(BF16)
        for s in range(SUB_BLOCKS):
            blk = i * SUB_BLOCKS + s
            slot = lax.rem(blk, KV_SLOTS)
            wait_in(slot)
            attend_block(blk, slot)
            start_out(blk, slot)
        hid_copy(i).start()
        return carry

    lax.fori_loop(0, n_up, body, 0)
    ctx_out = pltpu.make_async_copy(ctx_s, ctx_hbm, out_sem.at[1])
    ctx_out.start()
    pltpu.make_async_copy(hid_s, hid_hbm, out_sem.at[0]).wait()
    ctx_out.wait()
    for i in range(n_blk - KV_SLOTS, n_blk):
        wait_out(i % KV_SLOTS)


def front(pos, x, ga, ba, gm, bm, freq, wq, wu, kc, vc):
    rows, width = x.shape
    hid = wu.shape[1]
    lines = wq.shape[0] // width
    n_head = (lines // 2 - 2) * 2
    up_cols = hid // (rows // (ROW_BLOCK * SUB_BLOCKS))
    return pl.pallas_call(
        front_kernel,
        name='front',
        in_specs=[SMEM] + [ANY] * 10,
        out_specs=[ANY] * 4,
        out_shape=[
            jax.ShapeDtypeStruct(kc.shape, BF16),
            jax.ShapeDtypeStruct(vc.shape, BF16),
            jax.ShapeDtypeStruct((rows, hid), BF16),
            jax.ShapeDtypeStruct((n_head * rows, 128), F32),
        ],
        scratch_shapes=[
            pltpu.VMEM((rows, width), BF16),
            pltpu.VMEM((4, width), F32),
            pltpu.VMEM((1, 128), F32),
            pltpu.VMEM((rows, 128), F32),
            pltpu.VMEM((rows, 128), F32),
            pltpu.VMEM((rows, width), BF16),
            pltpu.VMEM((rows, width), BF16),
            pltpu.VMEM((width // QKV_CHUNK, QKV_CHUNK * lines, 128), BF16),
            pltpu.VMEM((QKV_CHUNK * lines, 128), F32),
            pltpu.VMEM((rows, lines * 128), F32),
            pltpu.VMEM((n_head * rows, 128), F32),
            pltpu.VMEM((4 * rows, 128), F32),
            pltpu.VMEM((UP_SLOTS, width, up_cols), BF16),
            pltpu.VMEM((rows, hid), BF16),
            pltpu.VMEM((n_head * rows, 128), F32),
            pltpu.VMEM((KV_SLOTS, ROW_BLOCK) + kc.shape[1:], BF16),
            pltpu.VMEM((KV_SLOTS, ROW_BLOCK) + vc.shape[1:], BF16),
            pltpu.SemaphoreType.DMA((6,)),
            pltpu.SemaphoreType.DMA((width // QKV_CHUNK,)),
            pltpu.SemaphoreType.DMA((UP_SLOTS,)),
            pltpu.SemaphoreType.DMA((KV_SLOTS,)),
            pltpu.SemaphoreType.DMA((KV_SLOTS,)),
            pltpu.SemaphoreType.DMA((KV_SLOTS,)),
            pltpu.SemaphoreType.DMA((KV_SLOTS,)),
            pltpu.SemaphoreType.DMA((2,)),
        ],
        compiler_params=pltpu.CompilerParams(vmem_limit_bytes=63 * MIB),
        cost_estimate=pl.CostEstimate(flops=22 * 10 ** 9, bytes_accessed=180 * 10 ** 6, transcendentals=0),
    )(pos, x, ga, ba, gm, bm, freq, wq, wu, kc, vc)


PIECES = 8
W_SLOTS = 4
MESH = pl.DeviceIdType.MESH


def exchange_kernel(x_hbm, hid_hbm, ctx_hbm, wd_hbm, wo_hbm, out_hbm,
                    x_s, hid_s, ctx_s, lhs_s, wd_s, wo_s, send_s, recv_s, keep_s, sum_s, other_s, out_s,
                    in_sem, wd_sem, wo_sem, c1_send, c1_recv, c2_send, c2_recv, c3_send, c3_recv, out_sem):
    rows, width = x_s.shape
    half = width // 2
    cols = half // PIECES
    heads = ctx_s.shape[0] // rows
    me = lax.axis_index('tp')
    core = lax.rem(me, 2)
    mate = me + 1 - 2 * core
    far = lax.rem(me + 2, 4)

    loads = [pltpu.make_async_copy(a, b, in_sem.at[i]) for i, (a, b) in enumerate(((hid_hbm, hid_s), (ctx_hbm, ctx_s), (x_hbm, x_s)))]
    for c in loads[:2]:
        c.start()

    def col_of(p, part):
        side = core if part else 1 - core
        return pl.multiple_of(side * half + p * cols, cols)

    def slot_of(p, part):
        return (2 * p + part) % W_SLOTS

    def wd_copy(p, part):
        return pltpu.make_async_copy(wd_hbm.at[:, pl.ds(col_of(p, part), cols)], wd_s.at[slot_of(p, part)], wd_sem.at[slot_of(p, part)])

    def wo_copy(p, part):
        return pltpu.make_async_copy(wo_hbm.at[:, pl.ds(col_of(p, part), cols)], wo_s.at[slot_of(p, part)], wo_sem.at[slot_of(p, part)])

    def w_start(p, part):
        wd_copy(p, part).start()
        wo_copy(p, part).start()

    w_start(0, 0)
    w_start(0, 1)

    barrier = pltpu.get_barrier_semaphore()
    for peer in (mate, far):
        pl.semaphore_signal(barrier, inc=1, device_id={'tp': peer}, device_id_type=MESH)
    pl.semaphore_wait(barrier, 2)

    def copy1(p):
        return pltpu.make_async_remote_copy(send_s.at[p], recv_s.at[p], c1_send.at[p], c1_recv.at[p], device_id={'tp': mate}, device_id_type=MESH)

    def copy2(p):
        return pltpu.make_async_remote_copy(sum_s.at[p], other_s.at[p], c2_send.at[p], c2_recv.at[p], device_id={'tp': far}, device_id_type=MESH)

    def copy3(p, side):
        view = out_s.at[side * PIECES + p]
        return pltpu.make_async_remote_copy(view, view, c3_send.at[p], c3_recv.at[p], device_id={'tp': mate}, device_id_type=MESH)

    w_start(1, 0)
    loads[2].start()
    loads[0].wait()
    loads[1].wait()
    for h in range(heads):
        lhs_s[:, h * 128:(h + 1) * 128] = ctx_s[h * rows:(h + 1) * rows, :].astype(BF16)

    def partial(p, part):
        wd_copy(p, part).wait()
        wo_copy(p, part).wait()
        nxt = p + 1 + part

        @pl.when(nxt < PIECES)
        def _():
            w_start(nxt, 1 - part)
        slot = slot_of(p, part)
        return jnp.dot(lhs_s[...], wo_s[slot], preferred_element_type=F32) + jnp.dot(hid_s[...], wd_s[slot], preferred_element_type=F32)

    def chip_sum(p):
        copy1(p).wait_recv()
        sum_s[p] = (keep_s[p] + recv_s[p].astype(F32)).astype(BF16)
        copy2(p).start()

    def compute(p, carry):
        send_s[p] = partial(p, 0).astype(BF16)
        copy1(p).start()
        keep_s[p] = partial(p, 1)
        chip_sum(p)
        return carry

    lax.fori_loop(0, PIECES, compute, 0)
    loads[2].wait()

    def out_copy(p, side):
        k = side * PIECES + p
        return pltpu.make_async_copy(out_s.at[k], out_hbm.at[:, pl.ds(pl.multiple_of(k * cols, cols), cols)], out_sem.at[k])

    def finish(p, carry):
        copy2(p).wait_recv()
        xs = x_s[:, pl.ds(col_of(p, 1), cols)].astype(F32)
        out_s[core * PIECES + p] = (xs + (sum_s[p].astype(F32) + other_s[p].astype(F32))).astype(BF16)
        copy3(p, core).start()
        out_copy(p, core).start()
        return carry

    lax.fori_loop(0, PIECES, finish, 0)

    def collect(p, carry):
        copy3(p, 1 - core).wait_recv()
        out_copy(p, 1 - core).start()
        return carry

    lax.fori_loop(0, PIECES, collect, 0)

    def drain(p, carry):
        copy1(p).wait_send()
        copy2(p).wait_send()
        copy3(p, core).wait_send()
        out_copy(p, core).wait()
        out_copy(p, 1 - core).wait()
        return carry

    lax.fori_loop(0, PIECES, drain, 0)


def exchange(x, hid, ctx, wd, wo):
    rows, width = x.shape
    cols = width // 2 // PIECES
    n_ff = hid.shape[1]
    n_ctx = wo.shape[0]
    dma = pltpu.SemaphoreType.DMA
    return pl.pallas_call(
        exchange_kernel,
        name='exchange',
        in_specs=[ANY] * 5,
        out_specs=ANY,
        out_shape=jax.ShapeDtypeStruct((rows, width), BF16),
        scratch_shapes=[
            pltpu.VMEM((rows, width), BF16),
            pltpu.VMEM((rows, n_ff), BF16),
            pltpu.VMEM(ctx.shape, F32),
            pltpu.VMEM((rows, n_ctx), BF16),
            pltpu.VMEM((W_SLOTS, n_ff, cols), BF16),
            pltpu.VMEM((W_SLOTS, n_ctx, cols), BF16),
            pltpu.VMEM((PIECES, rows, cols), BF16),
            pltpu.VMEM((PIECES, rows, cols), BF16),
            pltpu.VMEM((PIECES, rows, cols), F32),
            pltpu.VMEM((PIECES, rows, cols), BF16),
            pltpu.VMEM((PIECES, rows, cols), BF16),
            pltpu.VMEM((2 * PIECES, rows, cols), BF16),
            dma((3,)), dma((W_SLOTS,)), dma((W_SLOTS,)),
            dma((PIECES,)), dma((PIECES,)), dma((PIECES,)), dma((PIECES,)), dma((PIECES,)), dma((PIECES,)),
            dma((2 * PIECES,)),
        ],
        compiler_params=pltpu.CompilerParams(vmem_limit_bytes=63 * MIB, collective_id=0, has_side_effects=True),
        cost_estimate=pl.CostEstimate(flops=11 * 10 ** 9, bytes_accessed=48 * 10 ** 6, transcendentals=0),
    )(x, hid, ctx, wd, wo)


def solution(mesh):
    row_spec = P('dp', None)
    vec_spec = P(None)
    cache_spec = P('dp', 'tp', None, None)

    def device_step(x, ln_attn_gamma, ln_attn_beta, ln_mlp_gamma, ln_mlp_beta, w_qkv, w_out, w_up, w_down, k_cache, v_cache, positions):
        width = x.shape[1]
        head = w_qkv.shape[3]
        inv_freq = ROPE_BASE ** (-2.0 * np.arange(head // 2) / head)
        freq = jnp.asarray(np.concatenate([inv_freq, inv_freq])[None, :], F32)
        vecs = [v.reshape(1, width) for v in (ln_attn_gamma, ln_attn_beta, ln_mlp_gamma, ln_mlp_beta)]
        wq = jnp.transpose(w_qkv, (0, 2, 1, 3)).reshape(-1, head)
        ko, vo, hid, ctx = front(positions, x, *vecs, freq, wq, w_up, k_cache, v_cache)
        out = exchange(x, hid, ctx, w_down, w_out.reshape(-1, width))
        return out, ko, vo

    return jax.shard_map(device_step, mesh=mesh, in_specs=(row_spec, vec_spec, vec_spec, vec_spec, vec_spec, P(None, 'tp', None, None), P('tp', None, None, None), P(None, 'tp'), P('tp', None), cache_spec, cache_spec, P('dp')), out_specs=(row_spec, cache_spec, cache_spec), check_vma=False)
```

```python
import jax
import jax.numpy as jnp
import numpy as np
from jax import lax
from jax.experimental import pallas as pl
from jax.experimental.pallas import tpu as pltpu
from jax.sharding import PartitionSpec as P

LN_EPS = 1e-5
ROPE_BASE = 10000.0
NEG_BIG = -1e30
BF16 = jnp.bfloat16
F32 = jnp.float32
ANY = pl.BlockSpec(memory_space=pl.ANY)
HBM = pl.BlockSpec(memory_space=pltpu.HBM)
SMEM = pl.BlockSpec(memory_space=pltpu.SMEM)
MIB = 1024 * 1024

QKV_CHUNK = 512
LN_ROWS = 16
ROW_BLOCK = 8
SUB_BLOCKS = 2
KV_SLOTS = 10
KV_AHEAD = 6
UP_SLOTS = 4
W_PARTS = 4


def front_kernel(pos_ref, x_hbm, ga_hbm, ba_hbm, gm_hbm, bm_hbm, freq_hbm, wq_hbm, wu_hbm, kc_hbm, vc_hbm,
                 ko_hbm, vo_hbm, hid_hbm, ctx_hbm,
                 x_s, vec_s, freq_s, cos_s, sin_s, attn_s, mlp_s, wq_s, wqf_s, acc_s, q_s, kv_s, up_s, hid_s, ctx_s, kbuf, vbuf,
                 in_sem, wq_sem, up_sem, kin_sem, vin_sem, kout_sem, vout_sem, out_sem):
    rows, width = x_s.shape
    n_chunk = width // QKV_CHUNK
    lines = wq_hbm.shape[0] // width
    up_cols = up_s.shape[2]
    n_up = wu_hbm.shape[1] // up_cols
    n_blk = rows // ROW_BLOCK

    small = [pltpu.make_async_copy(x_hbm, x_s, in_sem.at[0])]
    for i, v in enumerate((ga_hbm, ba_hbm, gm_hbm, bm_hbm)):
        small.append(pltpu.make_async_copy(v, vec_s.at[pl.ds(i, 1), :], in_sem.at[1 + i]))
    freq_in = pltpu.make_async_copy(freq_hbm, freq_s, in_sem.at[5])
    freq_in.start()
    for c in small:
        c.start()

    def wq_copy(c):
        return pltpu.make_async_copy(wq_hbm.at[pl.ds(c * QKV_CHUNK * lines, QKV_CHUNK * lines), :], wq_s.at[c], wq_sem.at[c])

    def up_start(b, slot):
        cols = pl.ds(pl.multiple_of(b * up_cols, up_cols), up_cols)
        for k in range(W_PARTS):
            part = pl.ds(k * (width // W_PARTS), width // W_PARTS)
            pltpu.make_async_copy(wu_hbm.at[part, cols], up_s.at[slot, part, :], up_sem.at[slot]).start()

    def up_wait(slot):
        pltpu.make_async_copy(wu_hbm.at[:, pl.ds(0, up_cols)], up_s.at[slot], up_sem.at[slot]).wait()

    def block(ref, i):
        return ref.at[pl.ds(i * ROW_BLOCK, ROW_BLOCK)]

    def start_in(i, slot):
        pltpu.make_async_copy(block(kc_hbm, i), kbuf.at[slot], kin_sem.at[slot]).start(priority=1)
        pltpu.make_async_copy(block(vc_hbm, i), vbuf.at[slot], vin_sem.at[slot]).start(priority=1)

    def wait_in(slot):
        pltpu.make_async_copy(block(kc_hbm, 0), kbuf.at[slot], kin_sem.at[slot]).wait()
        pltpu.make_async_copy(block(vc_hbm, 0), vbuf.at[slot], vin_sem.at[slot]).wait()

    def start_out(i, slot):
        pltpu.make_async_copy(kbuf.at[slot], block(ko_hbm, i), kout_sem.at[slot]).start()
        pltpu.make_async_copy(vbuf.at[slot], block(vo_hbm, i), vout_sem.at[slot]).start()

    def wait_out(slot):
        pltpu.make_async_copy(kbuf.at[slot], block(ko_hbm, 0), kout_sem.at[slot]).wait()
        pltpu.make_async_copy(vbuf.at[slot], block(vo_hbm, 0), vout_sem.at[slot]).wait()

    wq_copy(0).start()
    wq_copy(1).start()

    freq_in.wait()

    def angle_body(b, carry):
        cos_s[pl.ds(b, 1), :] = pos_ref[b].astype(F32) * freq_s[0:1, :]
        return carry

    lax.fori_loop(0, rows, angle_body, 0, unroll=8)
    ang = cos_s[...]
    low = lax.broadcasted_iota(jnp.int32, ang.shape, 1) < 64
    sin_t = jnp.sin(ang)
    sin_s[...] = jnp.where(low, -sin_t, sin_t)
    cos_s[...] = jnp.cos(ang)

    for c in small:
        c.wait()
    wq_copy(2).start()
    wq_copy(3).start()

    def ln_body(i, carry):
        r = pl.ds(pl.multiple_of(i * LN_ROWS, LN_ROWS), LN_ROWS)
        xf = x_s[r, :].astype(F32)
        mean = jnp.mean(xf, axis=-1, keepdims=True)
        cen = xf - mean
        var = jnp.mean(cen * cen, axis=-1, keepdims=True)
        nrm = cen * lax.rsqrt(var + LN_EPS)
        attn_s[r, :] = (nrm * vec_s[0:1, :] + vec_s[1:2, :]).astype(BF16)
        mlp_s[r, :] = (nrm * vec_s[2:3, :] + vec_s[3:4, :]).astype(BF16)
        return carry

    half_ln = rows // LN_ROWS // 2
    lax.fori_loop(0, half_ln, ln_body, 0)
    for c in range(4, n_chunk):
        wq_copy(c).start()
    lax.fori_loop(half_ln, 2 * half_ln, ln_body, 0)

    for c in range(n_chunk):
        wq_copy(c).wait()
        if c < KV_AHEAD:
            start_in(c, c)
        if c >= n_chunk - UP_SLOTS:
            up_start(c - n_chunk + UP_SLOTS, c - n_chunk + UP_SLOTS)
        wqf_s[...] = wq_s[c].astype(F32)
        lhs = attn_s[:, c * QKV_CHUNK:(c + 1) * QKV_CHUNK]
        for pair in range(lines // 2):
            w = jnp.concatenate([wqf_s[pl.ds(2 * pair + e, QKV_CHUNK, stride=lines), :].astype(BF16) for e in range(2)], axis=1)
            part = jnp.dot(lhs, w, preferred_element_type=F32)
            if c == 0:
                acc_s[:, pair * 256:(pair + 1) * 256] = part
            else:
                acc_s[:, pair * 256:(pair + 1) * 256] += part

    n_slot = lines // 2
    n_q = n_slot - 2
    for j in range(n_slot):
        for g in range(2):
            col = (2 * j + g) * 128
            u = acc_s[:, col:col + 128].astype(BF16).astype(F32)
            if j < n_q + 1:
                u = (u * cos_s[...] + pltpu.roll(u, 64, 1) * sin_s[...]).astype(BF16).astype(F32)
            if j < n_q:
                q_s[pl.ds((g * n_q + j) * rows, rows), :] = u
            else:
                kv_s[pl.ds(((j - n_q) * 2 + g) * rows, rows), :] = u

    slot_ids = lax.broadcasted_iota(jnp.int32, (8, 256), 1)
    tile_ids = lax.broadcasted_iota(jnp.int32, (16, 128), 0)
    first = lax.broadcasted_iota(jnp.int32, (8, 128), 0) < 4
    scale = 128 ** -0.5

    def attend_block(i, slot):
        pos = [pos_ref[i * ROW_BLOCK + r] for r in range(ROW_BLOCK)]
        for r in range(ROW_BLOCK):
            base = pl.multiple_of((pos[r] // 16) * 16, 16)
            hit = tile_ids == pos[r] - base
            b = i * ROW_BLOCK + r
            for g in range(2):
                for buf, which in ((kbuf, 0), (vbuf, 1)):
                    new = kv_s[pl.ds((which * 2 + g) * rows + b, 1), :]
                    old = buf[slot, r, g, pl.ds(base, 16), :].astype(F32)
                    buf[slot, r, g, pl.ds(base, 16), :] = jnp.where(hit, new, old).astype(BF16)
        scores = []
        for r in range(ROW_BLOCK):
            b = i * ROW_BLOCK + r
            q = q_s[pl.ds(b, 8, stride=rows), :]
            zero = jnp.zeros_like(q)
            q2 = jnp.concatenate([jnp.where(first, q, zero), jnp.where(first, zero, q)], axis=1).astype(BF16)
            k2 = jnp.concatenate([kbuf[slot, r, 0], kbuf[slot, r, 1]], axis=1)
            s = lax.dot_general(q2, k2, (((1,), (1,)), ((), ())), preferred_element_type=F32) * scale
            scores.append(jnp.where(slot_ids <= pos[r], s, NEG_BIG))
        s = jnp.concatenate(scores, axis=0)
        e = jnp.exp(s - jnp.max(s, axis=-1, keepdims=True))
        p = (e / jnp.sum(e, axis=-1, keepdims=True)).astype(BF16)
        for r in range(ROW_BLOCK):
            v2 = jnp.concatenate([vbuf[slot, r, 0], vbuf[slot, r, 1]], axis=1)
            c = jnp.dot(p[8 * r:8 * r + 8], v2, preferred_element_type=F32)
            ctx_s[pl.ds(i * ROW_BLOCK + r, 8, stride=rows), :] = jnp.where(first, c[:, :128], c[:, 128:])

    def hid_copy(i):
        cols = pl.ds(pl.multiple_of(i * up_cols, up_cols), up_cols)
        return pltpu.make_async_copy(hid_s.at[:, cols], hid_hbm.at[:, cols], out_sem.at[0])

    def body(i, carry):
        for s in range(SUB_BLOCKS):
            nxt = i * SUB_BLOCKS + s + KV_AHEAD

            @pl.when(nxt < n_blk)
            def _():
                nslot = lax.rem(nxt, KV_SLOTS)

                @pl.when(nxt >= KV_SLOTS)
                def _():
                    wait_out(nslot)
                start_in(nxt, nslot)

        @pl.when((i >= 1) & (i - 1 + UP_SLOTS < n_up))
        def _():
            up_start(i - 1 + UP_SLOTS, lax.rem(i - 1, UP_SLOTS))

        uslot = lax.rem(i, UP_SLOTS)
        up_wait(uslot)
        pre = jnp.dot(mlp_s[...], up_s[uslot], preferred_element_type=F32)
        act = 0.5 * pre * (1.0 + lax.erf(pre * (0.5 ** 0.5)))
        hid_s[:, pl.ds(pl.multiple_of(i * up_cols, up_cols), up_cols)] = act.astype(BF16)
        for s in range(SUB_BLOCKS):
            blk = i * SUB_BLOCKS + s
            slot = lax.rem(blk, KV_SLOTS)
            wait_in(slot)
            attend_block(blk, slot)
            start_out(blk, slot)
        hid_copy(i).start()
        return carry

    lax.fori_loop(0, n_up, body, 0)
    ctx_out = pltpu.make_async_copy(ctx_s, ctx_hbm, out_sem.at[1])
    ctx_out.start()
    pltpu.make_async_copy(hid_s, hid_hbm, out_sem.at[0]).wait()
    ctx_out.wait()
    for i in range(n_blk - KV_SLOTS, n_blk):
        wait_out(i % KV_SLOTS)


def front(pos, x, ga, ba, gm, bm, freq, wq, wu, kc, vc):
    rows, width = x.shape
    hid = wu.shape[1]
    lines = wq.shape[0] // width
    n_head = (lines // 2 - 2) * 2
    up_cols = hid // (rows // (ROW_BLOCK * SUB_BLOCKS))
    return pl.pallas_call(
        front_kernel,
        name='front',
        in_specs=[SMEM] + [HBM] * 10,
        out_specs=[HBM] * 4,
        out_shape=[
            jax.ShapeDtypeStruct(kc.shape, BF16),
            jax.ShapeDtypeStruct(vc.shape, BF16),
            jax.ShapeDtypeStruct((rows, hid), BF16),
            jax.ShapeDtypeStruct((n_head * rows, 128), F32),
        ],
        scratch_shapes=[
            pltpu.VMEM((rows, width), BF16),
            pltpu.VMEM((4, width), F32),
            pltpu.VMEM((1, 128), F32),
            pltpu.VMEM((rows, 128), F32),
            pltpu.VMEM((rows, 128), F32),
            pltpu.VMEM((rows, width), BF16),
            pltpu.VMEM((rows, width), BF16),
            pltpu.VMEM((width // QKV_CHUNK, QKV_CHUNK * lines, 128), BF16),
            pltpu.VMEM((QKV_CHUNK * lines, 128), F32),
            pltpu.VMEM((rows, lines * 128), F32),
            pltpu.VMEM((n_head * rows, 128), F32),
            pltpu.VMEM((4 * rows, 128), F32),
            pltpu.VMEM((UP_SLOTS, width, up_cols), BF16),
            pltpu.VMEM((rows, hid), BF16),
            pltpu.VMEM((n_head * rows, 128), F32),
            pltpu.VMEM((KV_SLOTS, ROW_BLOCK) + kc.shape[1:], BF16),
            pltpu.VMEM((KV_SLOTS, ROW_BLOCK) + vc.shape[1:], BF16),
            pltpu.SemaphoreType.DMA((6,)),
            pltpu.SemaphoreType.DMA((width // QKV_CHUNK,)),
            pltpu.SemaphoreType.DMA((UP_SLOTS,)),
            pltpu.SemaphoreType.DMA((KV_SLOTS,)),
            pltpu.SemaphoreType.DMA((KV_SLOTS,)),
            pltpu.SemaphoreType.DMA((KV_SLOTS,)),
            pltpu.SemaphoreType.DMA((KV_SLOTS,)),
            pltpu.SemaphoreType.DMA((2,)),
        ],
        compiler_params=pltpu.CompilerParams(vmem_limit_bytes=63 * MIB),
        cost_estimate=pl.CostEstimate(flops=22 * 10 ** 9, bytes_accessed=180 * 10 ** 6, transcendentals=0),
    )(pos, x, ga, ba, gm, bm, freq, wq, wu, kc, vc)


PIECES = 8
W_SLOTS = 4
MESH = pl.DeviceIdType.MESH


def exchange_kernel(x_hbm, hid_hbm, ctx_hbm, wd_hbm, wo_hbm, out_ref,
                    x_s, hid_s, ctx_s, lhs_s, wd_s, wo_s, send_s, recv_s, keep_s, sum_s, other_s,
                    in_sem, wd_sem, wo_sem, c1_send, c1_recv, c2_send, c2_recv, c3_send, c3_recv):
    rows, width = x_s.shape
    half = width // 2
    cols = half // PIECES
    heads = ctx_s.shape[0] // rows
    me = lax.axis_index('tp')
    core = lax.rem(me, 2)
    mate = me + 1 - 2 * core
    far = lax.rem(me + 2, 4)

    loads = [pltpu.make_async_copy(a, b, in_sem.at[i]) for i, (a, b) in enumerate(((hid_hbm, hid_s), (ctx_hbm, ctx_s), (x_hbm, x_s)))]
    loads[1].start()
    for k in range(W_PARTS):
        part = pl.ds(k * (rows // W_PARTS), rows // W_PARTS)
        pltpu.make_async_copy(hid_hbm.at[part, :], hid_s.at[part, :], in_sem.at[0]).start()

    def col_of(p, part):
        side = core if part else 1 - core
        return pl.multiple_of(side * half + p * cols, cols)

    def slot_of(p, part):
        return (2 * p + part) % W_SLOTS

    def wd_copy(p, part, k=None):
        depth = wd_hbm.shape[0] // W_PARTS
        rng = slice(None) if k is None else pl.ds(k * depth, depth)
        return pltpu.make_async_copy(wd_hbm.at[rng, pl.ds(col_of(p, part), cols)], wd_s.at[slot_of(p, part), rng, :], wd_sem.at[slot_of(p, part)])

    def wo_copy(p, part):
        return pltpu.make_async_copy(wo_hbm.at[:, pl.ds(col_of(p, part), cols)], wo_s.at[slot_of(p, part)], wo_sem.at[slot_of(p, part)])

    def w_start(p, part):
        wo_copy(p, part).start()
        for k in range(W_PARTS):
            wd_copy(p, part, k).start()

    w_start(0, 0)

    barrier = pltpu.get_barrier_semaphore()
    for peer in (mate, far):
        pl.semaphore_signal(barrier, inc=1, device_id={'tp': peer}, device_id_type=MESH)
    pl.semaphore_wait(barrier, 2)

    def copy1(p):
        return pltpu.make_async_remote_copy(send_s.at[p], recv_s.at[p], c1_send.at[p], c1_recv.at[p], device_id={'tp': mate}, device_id_type=MESH)

    def copy2(p):
        return pltpu.make_async_remote_copy(sum_s.at[p], other_s.at[p], c2_send.at[p], c2_recv.at[p], device_id={'tp': far}, device_id_type=MESH)

    def copy3(p, side):
        view = out_ref.at[:, pl.ds(pl.multiple_of(side * half + p * cols, cols), cols)]
        return pltpu.make_async_remote_copy(view, view, c3_send.at[p], c3_recv.at[p], device_id={'tp': mate}, device_id_type=MESH)

    loads[1].wait()
    w_start(0, 1)
    for h in range(heads):
        lhs_s[:, h * 128:(h + 1) * 128] = ctx_s[h * rows:(h + 1) * rows, :].astype(BF16)
    loads[0].wait()
    w_start(1, 0)
    loads[2].start()

    def partial(p, part):
        wd_copy(p, part).wait()
        wo_copy(p, part).wait()
        nxt = p + 1 + part

        @pl.when(nxt < PIECES)
        def _():
            w_start(nxt, 1 - part)
        slot = slot_of(p, part)
        return jnp.dot(lhs_s[...], wo_s[slot], preferred_element_type=F32) + jnp.dot(hid_s[...], wd_s[slot], preferred_element_type=F32)

    def chip_sum(p):
        copy1(p).wait_recv()
        sum_s[p] = (keep_s[p] + recv_s[p].astype(F32)).astype(BF16)
        copy2(p).start()

    def compute(p, carry):
        send_s[p] = partial(p, 0).astype(BF16)
        copy1(p).start()
        keep_s[p] = partial(p, 1)
        chip_sum(p)
        return carry

    lax.fori_loop(0, PIECES, compute, 0)
    loads[2].wait()

    def finish(p, carry):
        copy2(p).wait_recv()
        xs = x_s[:, pl.ds(col_of(p, 1), cols)].astype(F32)
        out_ref[:, pl.ds(col_of(p, 1), cols)] = (xs + (sum_s[p].astype(F32) + other_s[p].astype(F32))).astype(BF16)
        copy3(p, core).start()
        return carry

    lax.fori_loop(0, PIECES, finish, 0)

    def drain(p, carry):
        copy1(p).wait_send()
        copy2(p).wait_send()
        copy3(p, core).wait_send()
        copy3(p, 1 - core).wait_recv()
        return carry

    lax.fori_loop(0, PIECES, drain, 0)


def exchange(x, hid, ctx, wd, wo):
    rows, width = x.shape
    cols = width // 2 // PIECES
    n_ff = hid.shape[1]
    n_ctx = wo.shape[0]
    dma = pltpu.SemaphoreType.DMA
    return pl.pallas_call(
        exchange_kernel,
        name='exchange',
        in_specs=[HBM] * 5,
        out_specs=pl.BlockSpec(memory_space=pltpu.VMEM),
        out_shape=jax.ShapeDtypeStruct((rows, width), BF16),
        scratch_shapes=[
            pltpu.VMEM((rows, width), BF16),
            pltpu.VMEM((rows, n_ff), BF16),
            pltpu.VMEM(ctx.shape, F32),
            pltpu.VMEM((rows, n_ctx), BF16),
            pltpu.VMEM((W_SLOTS, n_ff, cols), BF16),
            pltpu.VMEM((W_SLOTS, n_ctx, cols), BF16),
            pltpu.VMEM((PIECES, rows, cols), BF16),
            pltpu.VMEM((PIECES, rows, cols), BF16),
            pltpu.VMEM((PIECES, rows, cols), F32),
            pltpu.VMEM((PIECES, rows, cols), BF16),
            pltpu.VMEM((PIECES, rows, cols), BF16),
            dma((3,)), dma((W_SLOTS,)), dma((W_SLOTS,)),
            dma((PIECES,)), dma((PIECES,)), dma((PIECES,)), dma((PIECES,)), dma((PIECES,)), dma((PIECES,)),
        ],
        compiler_params=pltpu.CompilerParams(vmem_limit_bytes=32 * MIB, collective_id=0, has_side_effects=True),
        cost_estimate=pl.CostEstimate(flops=11 * 10 ** 9, bytes_accessed=48 * 10 ** 6, transcendentals=0),
    )(x, hid, ctx, wd, wo)


def solution(mesh):
    row_spec = P('dp', None)
    vec_spec = P(None)
    cache_spec = P('dp', 'tp', None, None)

    def device_step(x, ln_attn_gamma, ln_attn_beta, ln_mlp_gamma, ln_mlp_beta, w_qkv, w_out, w_up, w_down, k_cache, v_cache, positions):
        width = x.shape[1]
        head = w_qkv.shape[3]
        inv_freq = ROPE_BASE ** (-2.0 * np.arange(head // 2) / head)
        freq = jnp.asarray(np.concatenate([inv_freq, inv_freq])[None, :], F32)
        vecs = [v.reshape(1, width) for v in (ln_attn_gamma, ln_attn_beta, ln_mlp_gamma, ln_mlp_beta)]
        wq = jnp.transpose(w_qkv, (0, 2, 1, 3)).reshape(-1, head)
        ko, vo, hid, ctx = front(positions, x, *vecs, freq, wq, w_up, k_cache, v_cache)
        held = [pltpu.with_memory_space_constraint(a, pltpu.HBM) for a in (x, hid, ctx, w_down, w_out.reshape(-1, width))]
        out = exchange(*held)
        return out, ko, vo

    return jax.shard_map(device_step, mesh=mesh, in_specs=(row_spec, vec_spec, vec_spec, vec_spec, vec_spec, P(None, 'tp', None, None), P('tp', None, None, None), P(None, 'tp'), P('tp', None), cache_spec, cache_spec, P('dp')), out_specs=(row_spec, cache_spec, cache_spec), check_vma=False)
```

```python
import jax
import jax.numpy as jnp
import numpy as np
from jax import lax
from jax.experimental import pallas as pl
from jax.experimental.pallas import tpu as pltpu
from jax.sharding import PartitionSpec as P

LN_EPS = 1e-5
ROPE_BASE = 10000.0
NEG_BIG = -1e30
BF16 = jnp.bfloat16
F32 = jnp.float32
ANY = pl.BlockSpec(memory_space=pl.ANY)
HBM = pl.BlockSpec(memory_space=pltpu.HBM)
SMEM = pl.BlockSpec(memory_space=pltpu.SMEM)
MIB = 1024 * 1024

QKV_CHUNK = 512
LN_ROWS = 16
ROW_BLOCK = 8
SUB_BLOCKS = 2
KV_SLOTS = 10
KV_AHEAD = 6
UP_SLOTS = 4
W_PARTS = 4


def front_kernel(pos_ref, x_hbm, ga_hbm, ba_hbm, gm_hbm, bm_hbm, freq_hbm, wq_hbm, wu_hbm, kc_hbm, vc_hbm,
                 ko_hbm, vo_hbm, hid_hbm, ctx_hbm,
                 x_s, vec_s, freq_s, cos_s, sin_s, attn_s, mlp_s, wq_s, wqf_s, acc_s, q_s, kv_s, up_s, hid_s, ctx_s, kbuf, vbuf,
                 in_sem, wq_sem, up_sem, kin_sem, vin_sem, kout_sem, vout_sem, out_sem):
    rows, width = x_s.shape
    n_chunk = width // QKV_CHUNK
    lines = wq_hbm.shape[0] // width
    up_cols = up_s.shape[2]
    n_up = wu_hbm.shape[1] // up_cols
    n_blk = rows // ROW_BLOCK

    small = [pltpu.make_async_copy(x_hbm, x_s, in_sem.at[0])]
    for i, v in enumerate((ga_hbm, ba_hbm, gm_hbm, bm_hbm)):
        small.append(pltpu.make_async_copy(v, vec_s.at[pl.ds(i, 1), :], in_sem.at[1 + i]))
    freq_in = pltpu.make_async_copy(freq_hbm, freq_s, in_sem.at[5])
    freq_in.start()
    for c in small:
        c.start()

    def wq_copy(c):
        return pltpu.make_async_copy(wq_hbm.at[pl.ds(c * QKV_CHUNK * lines, QKV_CHUNK * lines), :], wq_s.at[c], wq_sem.at[c])

    def up_start(b, slot):
        cols = pl.ds(pl.multiple_of(b * up_cols, up_cols), up_cols)
        for k in range(W_PARTS):
            part = pl.ds(k * (width // W_PARTS), width // W_PARTS)
            pltpu.make_async_copy(wu_hbm.at[part, cols], up_s.at[slot, part, :], up_sem.at[slot]).start()

    def up_wait(slot):
        pltpu.make_async_copy(wu_hbm.at[:, pl.ds(0, up_cols)], up_s.at[slot], up_sem.at[slot]).wait()

    def block(ref, i):
        return ref.at[pl.ds(i * ROW_BLOCK, ROW_BLOCK)]

    def start_in(i, slot):
        pltpu.make_async_copy(block(kc_hbm, i), kbuf.at[slot], kin_sem.at[slot]).start(priority=1)
        pltpu.make_async_copy(block(vc_hbm, i), vbuf.at[slot], vin_sem.at[slot]).start(priority=1)

    def wait_in(slot):
        pltpu.make_async_copy(block(kc_hbm, 0), kbuf.at[slot], kin_sem.at[slot]).wait()
        pltpu.make_async_copy(block(vc_hbm, 0), vbuf.at[slot], vin_sem.at[slot]).wait()

    def start_out(i, slot):
        pltpu.make_async_copy(kbuf.at[slot], block(ko_hbm, i), kout_sem.at[slot]).start()
        pltpu.make_async_copy(vbuf.at[slot], block(vo_hbm, i), vout_sem.at[slot]).start()

    def wait_out(slot):
        pltpu.make_async_copy(kbuf.at[slot], block(ko_hbm, 0), kout_sem.at[slot]).wait()
        pltpu.make_async_copy(vbuf.at[slot], block(vo_hbm, 0), vout_sem.at[slot]).wait()

    wq_copy(0).start()
    wq_copy(1).start()

    freq_in.wait()

    def angle_body(b, carry):
        cos_s[pl.ds(b, 1), :] = pos_ref[b].astype(F32) * freq_s[0:1, :]
        return carry

    lax.fori_loop(0, rows, angle_body, 0, unroll=8)
    ang = cos_s[...]
    low = lax.broadcasted_iota(jnp.int32, ang.shape, 1) < 64
    sin_t = jnp.sin(ang)
    sin_s[...] = jnp.where(low, -sin_t, sin_t)
    cos_s[...] = jnp.cos(ang)

    for c in small:
        c.wait()
    wq_copy(2).start()
    wq_copy(3).start()

    def ln_body(i, carry):
        r = pl.ds(pl.multiple_of(i * LN_ROWS, LN_ROWS), LN_ROWS)
        xf = x_s[r, :].astype(F32)
        mean = jnp.mean(xf, axis=-1, keepdims=True)
        cen = xf - mean
        var = jnp.mean(cen * cen, axis=-1, keepdims=True)
        nrm = cen * lax.rsqrt(var + LN_EPS)
        attn_s[r, :] = (nrm * vec_s[0:1, :] + vec_s[1:2, :]).astype(BF16)
        mlp_s[r, :] = (nrm * vec_s[2:3, :] + vec_s[3:4, :]).astype(BF16)
        return carry

    half_ln = rows // LN_ROWS // 2
    lax.fori_loop(0, half_ln, ln_body, 0)
    for c in range(4, n_chunk):
        wq_copy(c).start()
    lax.fori_loop(half_ln, 2 * half_ln, ln_body, 0)

    for c in range(n_chunk):
        wq_copy(c).wait()
        if c < KV_AHEAD:
            start_in(c, c)
        if c >= n_chunk - UP_SLOTS:
            up_start(c - n_chunk + UP_SLOTS, c - n_chunk + UP_SLOTS)
        wqf_s[...] = wq_s[c].astype(F32)
        lhs = attn_s[:, c * QKV_CHUNK:(c + 1) * QKV_CHUNK]
        for pair in range(lines // 2):
            w = jnp.concatenate([wqf_s[pl.ds(2 * pair + e, QKV_CHUNK, stride=lines), :].astype(BF16) for e in range(2)], axis=1)
            part = jnp.dot(lhs, w, preferred_element_type=F32)
            if c == 0:
                acc_s[:, pair * 256:(pair + 1) * 256] = part
            else:
                acc_s[:, pair * 256:(pair + 1) * 256] += part

    n_slot = lines // 2
    n_q = n_slot - 2
    for j in range(n_slot):
        for g in range(2):
            col = (2 * j + g) * 128
            u = acc_s[:, col:col + 128].astype(BF16).astype(F32)
            if j < n_q + 1:
                u = (u * cos_s[...] + pltpu.roll(u, 64, 1) * sin_s[...]).astype(BF16).astype(F32)
            if j < n_q:
                q_s[pl.ds((g * n_q + j) * rows, rows), :] = u
            else:
                kv_s[pl.ds(((j - n_q) * 2 + g) * rows, rows), :] = u

    slot_ids = lax.broadcasted_iota(jnp.int32, (8, 256), 1)
    tile_ids = lax.broadcasted_iota(jnp.int32, (16, 128), 0)
    first = lax.broadcasted_iota(jnp.int32, (8, 128), 0) < 4
    scale = 128 ** -0.5

    def attend_block(i, slot):
        pos = [pos_ref[i * ROW_BLOCK + r] for r in range(ROW_BLOCK)]
        for r in range(ROW_BLOCK):
            base = pl.multiple_of((pos[r] // 16) * 16, 16)
            hit = tile_ids == pos[r] - base
            b = i * ROW_BLOCK + r
            for g in range(2):
                for buf, which in ((kbuf, 0), (vbuf, 1)):
                    new = kv_s[pl.ds((which * 2 + g) * rows + b, 1), :]
                    old = buf[slot, r, g, pl.ds(base, 16), :].astype(F32)
                    buf[slot, r, g, pl.ds(base, 16), :] = jnp.where(hit, new, old).astype(BF16)
        scores = []
        for r in range(ROW_BLOCK):
            b = i * ROW_BLOCK + r
            q = q_s[pl.ds(b, 8, stride=rows), :]
            zero = jnp.zeros_like(q)
            q2 = jnp.concatenate([jnp.where(first, q, zero), jnp.where(first, zero, q)], axis=1).astype(BF16)
            k2 = jnp.concatenate([kbuf[slot, r, 0], kbuf[slot, r, 1]], axis=1)
            s = lax.dot_general(q2, k2, (((1,), (1,)), ((), ())), preferred_element_type=F32) * scale
            scores.append(jnp.where(slot_ids <= pos[r], s, NEG_BIG))
        s = jnp.concatenate(scores, axis=0)
        e = jnp.exp(s - jnp.max(s, axis=-1, keepdims=True))
        p = (e / jnp.sum(e, axis=-1, keepdims=True)).astype(BF16)
        for r in range(ROW_BLOCK):
            v2 = jnp.concatenate([vbuf[slot, r, 0], vbuf[slot, r, 1]], axis=1)
            c = jnp.dot(p[8 * r:8 * r + 8], v2, preferred_element_type=F32)
            ctx_s[pl.ds(i * ROW_BLOCK + r, 8, stride=rows), :] = jnp.where(first, c[:, :128], c[:, 128:])

    def hid_copy(i):
        cols = pl.ds(pl.multiple_of(i * up_cols, up_cols), up_cols)
        return pltpu.make_async_copy(hid_s.at[:, cols], hid_hbm.at[:, cols], out_sem.at[0])

    def body(i, carry):
        for s in range(SUB_BLOCKS):
            nxt = i * SUB_BLOCKS + s + KV_AHEAD

            @pl.when(nxt < n_blk)
            def _():
                nslot = lax.rem(nxt, KV_SLOTS)

                @pl.when(nxt >= KV_SLOTS)
                def _():
                    wait_out(nslot)
                start_in(nxt, nslot)

        @pl.when((i >= 1) & (i - 1 + UP_SLOTS < n_up))
        def _():
            up_start(i - 1 + UP_SLOTS, lax.rem(i - 1, UP_SLOTS))

        uslot = lax.rem(i, UP_SLOTS)
        up_wait(uslot)
        for s in range(SUB_BLOCKS):
            wait_in(lax.rem(i * SUB_BLOCKS + s, KV_SLOTS))
        deep = width // 2
        pre = (jnp.dot(mlp_s[:, :deep], up_s[uslot, :deep, :], preferred_element_type=F32)
               + jnp.dot(mlp_s[:, deep:], up_s[uslot, deep:, :], preferred_element_type=F32))
        act = 0.5 * pre * (1.0 + lax.erf(pre * (0.5 ** 0.5)))
        hid_s[:, pl.ds(pl.multiple_of(i * up_cols, up_cols), up_cols)] = act.astype(BF16)
        for s in range(SUB_BLOCKS):
            blk = i * SUB_BLOCKS + s
            attend_block(blk, lax.rem(blk, KV_SLOTS))
        for s in range(SUB_BLOCKS):
            blk = i * SUB_BLOCKS + s
            start_out(blk, lax.rem(blk, KV_SLOTS))
        hid_copy(i).start()
        return carry

    lax.fori_loop(0, n_up, body, 0)
    ctx_out = pltpu.make_async_copy(ctx_s, ctx_hbm, out_sem.at[1])
    ctx_out.start()
    pltpu.make_async_copy(hid_s, hid_hbm, out_sem.at[0]).wait()
    ctx_out.wait()
    for i in range(n_blk - KV_SLOTS, n_blk):
        wait_out(i % KV_SLOTS)


def front(pos, x, ga, ba, gm, bm, freq, wq, wu, kc, vc):
    rows, width = x.shape
    hid = wu.shape[1]
    lines = wq.shape[0] // width
    n_head = (lines // 2 - 2) * 2
    up_cols = hid // (rows // (ROW_BLOCK * SUB_BLOCKS))
    return pl.pallas_call(
        front_kernel,
        name='front',
        in_specs=[SMEM] + [HBM] * 10,
        out_specs=[HBM] * 4,
        out_shape=[
            jax.ShapeDtypeStruct(kc.shape, BF16),
            jax.ShapeDtypeStruct(vc.shape, BF16),
            jax.ShapeDtypeStruct((rows, hid), BF16),
            jax.ShapeDtypeStruct((n_head * rows, 128), F32),
        ],
        scratch_shapes=[
            pltpu.VMEM((rows, width), BF16),
            pltpu.VMEM((4, width), F32),
            pltpu.VMEM((1, 128), F32),
            pltpu.VMEM((rows, 128), F32),
            pltpu.VMEM((rows, 128), F32),
            pltpu.VMEM((rows, width), BF16),
            pltpu.VMEM((rows, width), BF16),
            pltpu.VMEM((width // QKV_CHUNK, QKV_CHUNK * lines, 128), BF16),
            pltpu.VMEM((QKV_CHUNK * lines, 128), F32),
            pltpu.VMEM((rows, lines * 128), F32),
            pltpu.VMEM((n_head * rows, 128), F32),
            pltpu.VMEM((4 * rows, 128), F32),
            pltpu.VMEM((UP_SLOTS, width, up_cols), BF16),
            pltpu.VMEM((rows, hid), BF16),
            pltpu.VMEM((n_head * rows, 128), F32),
            pltpu.VMEM((KV_SLOTS, ROW_BLOCK) + kc.shape[1:], BF16),
            pltpu.VMEM((KV_SLOTS, ROW_BLOCK) + vc.shape[1:], BF16),
            pltpu.SemaphoreType.DMA((6,)),
            pltpu.SemaphoreType.DMA((width // QKV_CHUNK,)),
            pltpu.SemaphoreType.DMA((UP_SLOTS,)),
            pltpu.SemaphoreType.DMA((KV_SLOTS,)),
            pltpu.SemaphoreType.DMA((KV_SLOTS,)),
            pltpu.SemaphoreType.DMA((KV_SLOTS,)),
            pltpu.SemaphoreType.DMA((KV_SLOTS,)),
            pltpu.SemaphoreType.DMA((2,)),
        ],
        compiler_params=pltpu.CompilerParams(vmem_limit_bytes=63 * MIB),
        cost_estimate=pl.CostEstimate(flops=22 * 10 ** 9, bytes_accessed=180 * 10 ** 6, transcendentals=0),
    )(pos, x, ga, ba, gm, bm, freq, wq, wu, kc, vc)


PIECES = 16
W_SLOTS = 4
MESH = pl.DeviceIdType.MESH


def exchange_kernel(x_hbm, hid_hbm, ctx_hbm, wd_hbm, wo_hbm, out_ref,
                    x_s, ctx_s, lhs_s, w_s, send_s, recv_s, keep_s, sum_s, other_s,
                    in_sem, w_sem, c1_send, c1_recv, c2_send, c2_recv, c3_send, c3_recv):
    rows, width = x_s.shape
    half = width // 2
    cols = half // PIECES
    heads = ctx_s.shape[0] // rows
    n_ff, n_ctx = wd_hbm.shape[0], wo_hbm.shape[0]
    me = lax.axis_index('tp')
    core = lax.rem(me, 2)
    mate = me + 1 - 2 * core
    far = lax.rem(me + 2, 4)

    ctx_in = pltpu.make_async_copy(ctx_hbm, ctx_s, in_sem.at[1])
    ctx_in.start()
    for k in range(W_PARTS):
        part = pl.ds(k * (rows // W_PARTS), rows // W_PARTS)
        pltpu.make_async_copy(hid_hbm.at[part, :], lhs_s.at[part, pl.ds(0, n_ff)], in_sem.at[0]).start()

    def col_of(p, part):
        side = core if part else 1 - core
        return pl.multiple_of(side * half + p * cols, cols)

    def w_start(p):
        slot = lax.rem(p, W_SLOTS)
        for part in range(2):
            src, dst = pl.ds(col_of(p, part), cols), pl.ds(part * cols, cols)
            pltpu.make_async_copy(wo_hbm.at[:, src], w_s.at[slot, pl.ds(n_ff, n_ctx), dst], w_sem.at[slot]).start()
            for k in range(2):
                deep = pl.ds(k * (n_ff // 2), n_ff // 2)
                pltpu.make_async_copy(wd_hbm.at[deep, src], w_s.at[slot, deep, dst], w_sem.at[slot]).start()

    def w_wait(p):
        slot = lax.rem(p, W_SLOTS)
        for part in range(2):
            dst = pl.ds(part * cols, cols)
            pltpu.make_async_copy(wo_hbm.at[:, pl.ds(0, cols)], w_s.at[slot, pl.ds(n_ff, n_ctx), dst], w_sem.at[slot]).wait()
            pltpu.make_async_copy(wd_hbm.at[:, pl.ds(0, cols)], w_s.at[slot, pl.ds(0, n_ff), dst], w_sem.at[slot]).wait()

    w_start(0)

    barrier = pltpu.get_barrier_semaphore()
    for peer in (mate, far):
        pl.semaphore_signal(barrier, inc=1, device_id={'tp': peer}, device_id_type=MESH)
    pl.semaphore_wait(barrier, 2)

    def copy1(p):
        return pltpu.make_async_remote_copy(send_s.at[p], recv_s.at[p], c1_send.at[p], c1_recv.at[p], device_id={'tp': mate}, device_id_type=MESH)

    def copy2(p):
        return pltpu.make_async_remote_copy(sum_s.at[p], other_s.at[p], c2_send.at[p], c2_recv.at[p], device_id={'tp': far}, device_id_type=MESH)

    def copy3(p, side):
        view = out_ref.at[:, pl.ds(pl.multiple_of(side * half + p * cols, cols), cols)]
        return pltpu.make_async_remote_copy(view, view, c3_send.at[p], c3_recv.at[p], device_id={'tp': mate}, device_id_type=MESH)

    ctx_in.wait()
    w_start(1)
    for h in range(heads):
        lhs_s[:, n_ff + h * 128:n_ff + (h + 1) * 128] = ctx_s[h * rows:(h + 1) * rows, :].astype(BF16)
    pltpu.make_async_copy(hid_hbm, lhs_s.at[:, pl.ds(0, n_ff)], in_sem.at[0]).wait()
    x_in = pltpu.make_async_copy(x_hbm, x_s, in_sem.at[2])
    x_in.start()
    w_start(2)

    def chip_sum(p):
        copy1(p).wait_recv()
        sum_s[p] = (keep_s[p] + recv_s[p].astype(F32)).astype(BF16)
        copy2(p).start()

    def compute(p, carry):
        w_wait(p)

        @pl.when(p + 3 < PIECES)
        def _():
            w_start(p + 3)
        slot = lax.rem(p, W_SLOTS)
        deep = (n_ff + n_ctx) // 2
        s = (jnp.dot(lhs_s[:, :deep], w_s[slot, :deep, :], preferred_element_type=F32)
             + jnp.dot(lhs_s[:, deep:], w_s[slot, deep:, :], preferred_element_type=F32))
        send_s[p] = s[:, :cols].astype(BF16)
        keep_s[p] = s[:, cols:]
        copy1(p).start()

        @pl.when(p > 0)
        def _():
            chip_sum(p - 1)
        return carry

    lax.fori_loop(0, PIECES, compute, 0)
    chip_sum(PIECES - 1)
    x_in.wait()

    def finish(p, carry):
        copy2(p).wait_recv()
        xs = x_s[:, pl.ds(col_of(p, 1), cols)].astype(F32)
        out_ref[:, pl.ds(col_of(p, 1), cols)] = (xs + (sum_s[p].astype(F32) + other_s[p].astype(F32))).astype(BF16)
        copy3(p, core).start()
        return carry

    lax.fori_loop(0, PIECES, finish, 0)

    def drain(p, carry):
        copy1(p).wait_send()
        copy2(p).wait_send()
        copy3(p, core).wait_send()
        copy3(p, 1 - core).wait_recv()
        return carry

    lax.fori_loop(0, PIECES, drain, 0)


def exchange(x, hid, ctx, wd, wo):
    rows, width = x.shape
    cols = width // 2 // PIECES
    n_ff = hid.shape[1]
    n_ctx = wo.shape[0]
    dma = pltpu.SemaphoreType.DMA
    return pl.pallas_call(
        exchange_kernel,
        name='exchange',
        in_specs=[HBM] * 5,
        out_specs=pl.BlockSpec(memory_space=pltpu.VMEM),
        out_shape=jax.ShapeDtypeStruct((rows, width), BF16),
        scratch_shapes=[
            pltpu.VMEM((rows, width), BF16),
            pltpu.VMEM(ctx.shape, F32),
            pltpu.VMEM((rows, n_ff + n_ctx), BF16),
            pltpu.VMEM((W_SLOTS, n_ff + n_ctx, 2 * cols), BF16),
            pltpu.VMEM((PIECES, rows, cols), BF16),
            pltpu.VMEM((PIECES, rows, cols), BF16),
            pltpu.VMEM((PIECES, rows, cols), F32),
            pltpu.VMEM((PIECES, rows, cols), BF16),
            pltpu.VMEM((PIECES, rows, cols), BF16),
            dma((3,)), dma((W_SLOTS,)),
            dma((PIECES,)), dma((PIECES,)), dma((PIECES,)), dma((PIECES,)), dma((PIECES,)), dma((PIECES,)),
        ],
        compiler_params=pltpu.CompilerParams(vmem_limit_bytes=32 * MIB, collective_id=0, has_side_effects=True),
        cost_estimate=pl.CostEstimate(flops=11 * 10 ** 9, bytes_accessed=48 * 10 ** 6, transcendentals=0),
    )(x, hid, ctx, wd, wo)


def solution(mesh):
    row_spec = P('dp', None)
    vec_spec = P(None)
    cache_spec = P('dp', 'tp', None, None)

    def device_step(x, ln_attn_gamma, ln_attn_beta, ln_mlp_gamma, ln_mlp_beta, w_qkv, w_out, w_up, w_down, k_cache, v_cache, positions):
        width = x.shape[1]
        head = w_qkv.shape[3]
        inv_freq = ROPE_BASE ** (-2.0 * np.arange(head // 2) / head)
        freq = jnp.asarray(np.concatenate([inv_freq, inv_freq])[None, :], F32)
        vecs = [v.reshape(1, width) for v in (ln_attn_gamma, ln_attn_beta, ln_mlp_gamma, ln_mlp_beta)]
        wq = jnp.transpose(w_qkv, (0, 2, 1, 3)).reshape(-1, head)
        ko, vo, hid, ctx = front(positions, x, *vecs, freq, wq, w_up, k_cache, v_cache)
        held = [pltpu.with_memory_space_constraint(a, pltpu.HBM) for a in (x, hid, ctx, w_down, w_out.reshape(-1, width))]
        out = exchange(*held)
        return out, ko, vo

    return jax.shard_map(device_step, mesh=mesh, in_specs=(row_spec, vec_spec, vec_spec, vec_spec, vec_spec, P(None, 'tp', None, None), P('tp', None, None, None), P(None, 'tp'), P('tp', None), cache_spec, cache_spec, P('dp')), out_specs=(row_spec, cache_spec, cache_spec), check_vma=False)
```

```python
import jax
import jax.numpy as jnp
import numpy as np
from jax import lax
from jax.experimental import pallas as pl
from jax.experimental.pallas import tpu as pltpu
from jax.sharding import PartitionSpec as P

LN_EPS = 1e-5
ROPE_BASE = 10000.0
NEG_BIG = -1e30
BF16 = jnp.bfloat16
F32 = jnp.float32
ANY = pl.BlockSpec(memory_space=pl.ANY)
HBM = pl.BlockSpec(memory_space=pltpu.HBM)
VMEM = pl.BlockSpec(memory_space=pltpu.VMEM)
SMEM = pl.BlockSpec(memory_space=pltpu.SMEM)
MIB = 1024 * 1024

QKV_CHUNK = 512
LN_ROWS = 16
ROW_BLOCK = 8
SUB_BLOCKS = 2
KV_SLOTS = 12
KV_AHEAD = 8
UP_SLOTS = 4
W_PARTS = 4


def front_kernel(pos_ref, x_hbm, ga_hbm, ba_hbm, gm_hbm, bm_hbm, freq_hbm, wq_hbm, wu_hbm, wd_hbm, wo_hbm, kc_hbm, vc_hbm,
                 ko_hbm, vo_hbm, lhs_ref, w0_ref,
                 x_s, vec_s, freq_s, cos_s, sin_s, attn_s, wqf_s, acc_s, q_s, kv_s, up_s, ctx_s, kbuf, vbuf,
                 in_sem, wq_sem, up_sem, kin_sem, vin_sem, kout_sem, vout_sem, w0_sem):
    mlp_s = x_s
    rows, width = x_s.shape
    seq = kc_hbm.shape[0] // (2 * rows)
    lines_blk = ROW_BLOCK * 2 * seq
    n_ff = lhs_ref.shape[1] - wo_hbm.shape[0]
    n_chunk = width // QKV_CHUNK
    lines = wq_hbm.shape[0] // width
    up_cols = up_s.shape[2]
    n_up = wu_hbm.shape[1] // up_cols
    n_blk = rows // ROW_BLOCK

    small = [pltpu.make_async_copy(x_hbm, x_s, in_sem.at[0])]
    for i, v in enumerate((ga_hbm, ba_hbm, gm_hbm, bm_hbm)):
        small.append(pltpu.make_async_copy(v, vec_s.at[pl.ds(i, 1), :], in_sem.at[1 + i]))
    freq_in = pltpu.make_async_copy(freq_hbm, freq_s, in_sem.at[5])
    freq_in.start()
    for c in small:
        c.start()

    wq_lines = QKV_CHUNK * lines
    wq_base = (KV_SLOTS - n_chunk * wq_lines // (2 * lines_blk)) * lines_blk
    wq_order = [c for pair in zip(range(n_chunk // 2), range(n_chunk // 2, n_chunk)) for c in pair]

    def wq_view(c):
        buf = kbuf if c < n_chunk // 2 else vbuf
        return buf.at[pl.ds(wq_base + (c % (n_chunk // 2)) * wq_lines, wq_lines), :]

    def wq_copy(c):
        return pltpu.make_async_copy(wq_hbm.at[pl.ds(c * wq_lines, wq_lines), :], wq_view(c), wq_sem.at[c])

    def up_start(b, slot):
        cols = pl.ds(pl.multiple_of(b * up_cols, up_cols), up_cols)
        for k in range(W_PARTS):
            part = pl.ds(k * (width // W_PARTS), width // W_PARTS)
            pltpu.make_async_copy(wu_hbm.at[part, cols], up_s.at[slot, part, :], up_sem.at[slot]).start()

    def up_wait(slot):
        pltpu.make_async_copy(wu_hbm.at[:, pl.ds(0, up_cols)], up_s.at[slot], up_sem.at[slot]).wait()

    def block(ref, i):
        return ref.at[pl.ds(pl.multiple_of(i * lines_blk, lines_blk), lines_blk), :]

    def start_in(i, slot):
        pltpu.make_async_copy(block(kc_hbm, i), block(kbuf, slot), kin_sem.at[slot]).start(priority=1)
        pltpu.make_async_copy(block(vc_hbm, i), block(vbuf, slot), vin_sem.at[slot]).start(priority=1)

    def wait_in(slot):
        pltpu.make_async_copy(block(kc_hbm, 0), block(kbuf, slot), kin_sem.at[slot]).wait()
        pltpu.make_async_copy(block(vc_hbm, 0), block(vbuf, slot), vin_sem.at[slot]).wait()

    def start_out(i, slot):
        pltpu.make_async_copy(block(kbuf, slot), block(ko_hbm, i), kout_sem.at[slot]).start()
        pltpu.make_async_copy(block(vbuf, slot), block(vo_hbm, i), vout_sem.at[slot]).start()

    def wait_out(slot):
        pltpu.make_async_copy(block(kbuf, slot), block(ko_hbm, 0), kout_sem.at[slot]).wait()
        pltpu.make_async_copy(block(vbuf, slot), block(vo_hbm, 0), vout_sem.at[slot]).wait()

    for c in wq_order[:2]:
        wq_copy(c).start()

    freq_in.wait()

    def angle_body(b, carry):
        cos_s[pl.ds(b, 1), :] = pos_ref[b].astype(F32) * freq_s[0:1, :]
        return carry

    lax.fori_loop(0, rows, angle_body, 0, unroll=8)
    ang = cos_s[...]
    low = lax.broadcasted_iota(jnp.int32, ang.shape, 1) < 64
    sin_t = jnp.sin(ang)
    sin_s[...] = jnp.where(low, -sin_t, sin_t)
    cos_s[...] = jnp.cos(ang)

    for c in small:
        c.wait()
    for c in wq_order[2:4]:
        wq_copy(c).start()

    def ln_body(i, carry):
        r = pl.ds(pl.multiple_of(i * LN_ROWS, LN_ROWS), LN_ROWS)
        xf = x_s[r, :].astype(F32)
        mean = jnp.mean(xf, axis=-1, keepdims=True)
        cen = xf - mean
        var = jnp.mean(cen * cen, axis=-1, keepdims=True)
        nrm = cen * lax.rsqrt(var + LN_EPS)
        attn_s[r, :] = (nrm * vec_s[0:1, :] + vec_s[1:2, :]).astype(BF16)
        mlp_s[r, :] = (nrm * vec_s[2:3, :] + vec_s[3:4, :]).astype(BF16)
        return carry

    half_ln = rows // LN_ROWS // 2
    lax.fori_loop(0, half_ln, ln_body, 0)
    for c in wq_order[4:]:
        wq_copy(c).start()
    lax.fori_loop(half_ln, 2 * half_ln, ln_body, 0)

    for step, c in enumerate(wq_order):
        wq_copy(c).wait()
        if step < KV_AHEAD:
            start_in(step, step)
        if step >= n_chunk - UP_SLOTS:
            up_start(step - n_chunk + UP_SLOTS, step - n_chunk + UP_SLOTS)
        wqf_s[...] = wq_view(c)[...].astype(F32)
        lhs = attn_s[:, c * QKV_CHUNK:(c + 1) * QKV_CHUNK]
        for pair in range(lines // 2):
            w = jnp.concatenate([wqf_s[pl.ds(2 * pair + e, QKV_CHUNK, stride=lines), :].astype(BF16) for e in range(2)], axis=1)
            part = jnp.dot(lhs, w, preferred_element_type=F32)
            if step == 0:
                acc_s[:, pair * 256:(pair + 1) * 256] = part
            else:
                acc_s[:, pair * 256:(pair + 1) * 256] += part

    n_slot = lines // 2
    n_q = n_slot - 2
    for j in range(n_slot):
        for g in range(2):
            col = (2 * j + g) * 128
            u = acc_s[:, col:col + 128].astype(BF16).astype(F32)
            if j < n_q + 1:
                u = (u * cos_s[...] + pltpu.roll(u, 64, 1) * sin_s[...]).astype(BF16).astype(F32)
            if j < n_q:
                q_s[pl.ds((g * n_q + j) * rows, rows), :] = u
            else:
                kv_s[pl.ds(((j - n_q) * 2 + g) * rows, rows), :] = u

    slot_ids = lax.broadcasted_iota(jnp.int32, (8, 256), 1)
    tile_ids = lax.broadcasted_iota(jnp.int32, (16, 128), 0)
    first = lax.broadcasted_iota(jnp.int32, (8, 128), 0) < 4
    scale = 128 ** -0.5

    def pair_of(buf, slot, r):
        at = [pl.ds(pl.multiple_of(slot * lines_blk + (2 * r + g) * seq, seq), seq) for g in range(2)]
        return jnp.concatenate([buf[a, :] for a in at], axis=1)

    def attend_block(i, slot):
        pos = [pos_ref[i * ROW_BLOCK + r] for r in range(ROW_BLOCK)]
        for r in range(ROW_BLOCK):
            base = pl.multiple_of((pos[r] // 16) * 16, 16)
            hit = tile_ids == pos[r] - base
            b = i * ROW_BLOCK + r
            for g in range(2):
                tile = pl.ds(pl.multiple_of(slot * lines_blk + (2 * r + g) * seq + base, 16), 16)
                for buf, which in ((kbuf, 0), (vbuf, 1)):
                    new = kv_s[pl.ds((which * 2 + g) * rows + b, 1), :]
                    buf[tile, :] = jnp.where(hit, new, buf[tile, :].astype(F32)).astype(BF16)
        scores = []
        for r in range(ROW_BLOCK):
            b = i * ROW_BLOCK + r
            q = q_s[pl.ds(b, 8, stride=rows), :]
            zero = jnp.zeros_like(q)
            q2 = jnp.concatenate([jnp.where(first, q, zero), jnp.where(first, zero, q)], axis=1).astype(BF16)
            k2 = pair_of(kbuf, slot, r)
            s = lax.dot_general(q2, k2, (((1,), (1,)), ((), ())), preferred_element_type=F32) * scale
            scores.append(jnp.where(slot_ids <= pos[r], s, NEG_BIG))
        s = jnp.concatenate(scores, axis=0)
        e = jnp.exp(s - jnp.max(s, axis=-1, keepdims=True))
        p = (e / jnp.sum(e, axis=-1, keepdims=True)).astype(BF16)
        for r in range(ROW_BLOCK):
            v2 = pair_of(vbuf, slot, r)
            c = jnp.dot(p[8 * r:8 * r + 8], v2, preferred_element_type=F32)
            ctx_s[pl.ds(i * ROW_BLOCK + r, 8, stride=rows), :] = jnp.where(first, c[:, :128], c[:, 128:])

    core = lax.rem(lax.axis_index('tp'), 2)
    cols = w0_ref.shape[1] // 2
    w0_in = []
    for part in range(2):
        src = pl.ds(pl.multiple_of((core if part else 1 - core) * (wd_hbm.shape[1] // 2), cols), cols)
        dst = pl.ds(part * cols, cols)
        w0_in.append(pltpu.make_async_copy(wd_hbm.at[:, src], w0_ref.at[pl.ds(0, n_ff), dst], w0_sem.at[0]))
        w0_in.append(pltpu.make_async_copy(wo_hbm.at[:, src], w0_ref.at[pl.ds(n_ff, wo_hbm.shape[0]), dst], w0_sem.at[0]))

    def body(i, carry):
        for s in range(SUB_BLOCKS):
            nxt = i * SUB_BLOCKS + s + KV_AHEAD

            @pl.when(nxt < n_blk)
            def _():
                nslot = lax.rem(nxt, KV_SLOTS)

                @pl.when(nxt >= KV_SLOTS)
                def _():
                    wait_out(nslot)
                start_in(nxt, nslot)

        @pl.when((i >= 1) & (i - 1 + UP_SLOTS < n_up))
        def _():
            up_start(i - 1 + UP_SLOTS, lax.rem(i - 1, UP_SLOTS))

        uslot = lax.rem(i, UP_SLOTS)
        up_wait(uslot)
        for s in range(SUB_BLOCKS):
            wait_in(lax.rem(i * SUB_BLOCKS + s, KV_SLOTS))
        deep = width // 2
        pre = (jnp.dot(mlp_s[:, :deep], up_s[uslot, :deep, :], preferred_element_type=F32)
               + jnp.dot(mlp_s[:, deep:], up_s[uslot, deep:, :], preferred_element_type=F32))
        act = 0.5 * pre * (1.0 + lax.erf(pre * (0.5 ** 0.5)))
        lhs_ref[:, pl.ds(pl.multiple_of(i * up_cols, up_cols), up_cols)] = act.astype(BF16)
        for s in range(SUB_BLOCKS):
            blk = i * SUB_BLOCKS + s
            attend_block(blk, lax.rem(blk, KV_SLOTS))
        for s in range(SUB_BLOCKS):
            blk = i * SUB_BLOCKS + s
            start_out(blk, lax.rem(blk, KV_SLOTS))

        @pl.when(i == n_up - 4)
        def _():
            for c in w0_in:
                c.start(priority=1)
        return carry

    lax.fori_loop(0, n_up, body, 0)
    for h in range(ctx_s.shape[0] // rows):
        lhs_ref[:, n_ff + h * 128:n_ff + (h + 1) * 128] = ctx_s[h * rows:(h + 1) * rows, :].astype(BF16)
    for c in w0_in:
        c.wait()
    for i in range(n_blk - KV_SLOTS, n_blk):
        wait_out(i % KV_SLOTS)


def front(pos, x, ga, ba, gm, bm, freq, wq, wu, wd, wo, kc, vc):
    rows, width = x.shape
    hid = wu.shape[1]
    lines = wq.shape[0] // width
    n_head = (lines // 2 - 2) * 2
    up_cols = hid // (rows // (ROW_BLOCK * SUB_BLOCKS))
    lines_blk = kc.shape[0] // rows * ROW_BLOCK
    return pl.pallas_call(
        front_kernel,
        name='front',
        in_specs=[SMEM] + [HBM] * 12,
        out_specs=[HBM, HBM, VMEM, VMEM],
        out_shape=[
            jax.ShapeDtypeStruct(kc.shape, BF16),
            jax.ShapeDtypeStruct(vc.shape, BF16),
            jax.ShapeDtypeStruct((rows, hid + wo.shape[0]), BF16),
            jax.ShapeDtypeStruct((hid + wo.shape[0], width // PIECES), BF16),
        ],
        scratch_shapes=[
            pltpu.VMEM((rows, width), BF16),
            pltpu.VMEM((4, width), F32),
            pltpu.VMEM((1, 128), F32),
            pltpu.VMEM((rows, 128), F32),
            pltpu.VMEM((rows, 128), F32),
            pltpu.VMEM((rows, width), BF16),
            pltpu.VMEM((QKV_CHUNK * lines, 128), F32),
            pltpu.VMEM((rows, lines * 128), F32),
            pltpu.VMEM((n_head * rows, 128), F32),
            pltpu.VMEM((4 * rows, 128), F32),
            pltpu.VMEM((UP_SLOTS, width, up_cols), BF16),
            pltpu.VMEM((n_head * rows, 128), F32),
            pltpu.VMEM((KV_SLOTS * lines_blk, 128), BF16),
            pltpu.VMEM((KV_SLOTS * lines_blk, 128), BF16),
            pltpu.SemaphoreType.DMA((6,)),
            pltpu.SemaphoreType.DMA((width // QKV_CHUNK,)),
            pltpu.SemaphoreType.DMA((UP_SLOTS,)),
            pltpu.SemaphoreType.DMA((KV_SLOTS,)),
            pltpu.SemaphoreType.DMA((KV_SLOTS,)),
            pltpu.SemaphoreType.DMA((KV_SLOTS,)),
            pltpu.SemaphoreType.DMA((KV_SLOTS,)),
            pltpu.SemaphoreType.DMA((1,)),
        ],
        compiler_params=pltpu.CompilerParams(vmem_limit_bytes=44 * MIB),
        cost_estimate=pl.CostEstimate(flops=22 * 10 ** 9, bytes_accessed=180 * 10 ** 6, transcendentals=0),
    )(pos, x, ga, ba, gm, bm, freq, wq, wu, wd, wo, kc, vc)


PIECES = 16
W_SLOTS = 4
MESH = pl.DeviceIdType.MESH


def exchange_kernel(x_hbm, lhs_s, w0_ref, wd_hbm, wo_hbm, out_ref,
                    x_s, w_s, send_s, recv_s, keep_s, sum_s, other_s,
                    in_sem, w_sem, c1_send, c1_recv, c2_send, c2_recv, c3_send, c3_recv):
    rows, width = x_s.shape
    half = width // 2
    cols = half // PIECES
    n_ff, n_ctx = wd_hbm.shape[0], wo_hbm.shape[0]
    me = lax.axis_index('tp')
    core = lax.rem(me, 2)
    mate = me + 1 - 2 * core
    far = lax.rem(me + 2, 4)

    def col_of(p, part):
        side = core if part else 1 - core
        return pl.multiple_of(side * half + p * cols, cols)

    def w_start(p):
        slot = lax.rem(p, W_SLOTS)
        for part in range(2):
            src, dst = pl.ds(col_of(p, part), cols), pl.ds(part * cols, cols)
            pltpu.make_async_copy(wo_hbm.at[:, src], w_s.at[slot, pl.ds(n_ff, n_ctx), dst], w_sem.at[slot]).start()
            for k in range(2):
                deep = pl.ds(k * (n_ff // 2), n_ff // 2)
                pltpu.make_async_copy(wd_hbm.at[deep, src], w_s.at[slot, deep, dst], w_sem.at[slot]).start()

    def w_wait(p):
        slot = lax.rem(p, W_SLOTS)
        for part in range(2):
            dst = pl.ds(part * cols, cols)
            pltpu.make_async_copy(wo_hbm.at[:, pl.ds(0, cols)], w_s.at[slot, pl.ds(n_ff, n_ctx), dst], w_sem.at[slot]).wait()
            pltpu.make_async_copy(wd_hbm.at[:, pl.ds(0, cols)], w_s.at[slot, pl.ds(0, n_ff), dst], w_sem.at[slot]).wait()

    for p in range(1, W_SLOTS):
        w_start(p)
    x_in = pltpu.make_async_copy(x_hbm, x_s, in_sem.at[0])
    x_in.start()

    barrier = pltpu.get_barrier_semaphore()
    for peer in (mate, far):
        pl.semaphore_signal(barrier, inc=1, device_id={'tp': peer}, device_id_type=MESH)
    pl.semaphore_wait(barrier, 2)

    def copy1(p):
        return pltpu.make_async_remote_copy(send_s.at[p], recv_s.at[p], c1_send.at[p], c1_recv.at[p], device_id={'tp': mate}, device_id_type=MESH)

    def copy2(p):
        return pltpu.make_async_remote_copy(sum_s.at[p], other_s.at[p], c2_send.at[p], c2_recv.at[p], device_id={'tp': far}, device_id_type=MESH)

    def copy3(p, side):
        view = out_ref.at[:, pl.ds(pl.multiple_of(side * half + p * cols, cols), cols)]
        return pltpu.make_async_remote_copy(view, view, c3_send.at[p], c3_recv.at[p], device_id={'tp': mate}, device_id_type=MESH)

    def chip_sum(p):
        copy1(p).wait_recv()
        sum_s[p] = (keep_s[p] + recv_s[p].astype(F32)).astype(BF16)
        copy2(p).start()

    def partial(p, w):
        deep = (n_ff + n_ctx) // 2
        s = (jnp.dot(lhs_s[:, :deep], w[:deep, :], preferred_element_type=F32)
             + jnp.dot(lhs_s[:, deep:], w[deep:, :], preferred_element_type=F32))
        send_s[p] = s[:, :cols].astype(BF16)
        keep_s[p] = s[:, cols:]
        copy1(p).start()

    partial(0, w0_ref)
    chip_sum(0)

    def compute(p, carry):
        w_wait(p)

        @pl.when(p + 3 < PIECES)
        def _():
            w_start(p + 3)
        partial(p, w_s.at[lax.rem(p, W_SLOTS)])

        @pl.when(p > 1)
        def _():
            chip_sum(p - 1)
        return carry

    lax.fori_loop(1, PIECES, compute, 0)
    chip_sum(PIECES - 1)
    x_in.wait()

    def finish(p, carry):
        copy2(p).wait_recv()
        xs = x_s[:, pl.ds(col_of(p, 1), cols)].astype(F32)
        out_ref[:, pl.ds(col_of(p, 1), cols)] = (xs + (sum_s[p].astype(F32) + other_s[p].astype(F32))).astype(BF16)
        copy3(p, core).start()
        return carry

    lax.fori_loop(0, PIECES, finish, 0)

    def drain(p, carry):
        copy1(p).wait_send()
        copy2(p).wait_send()
        copy3(p, core).wait_send()
        copy3(p, 1 - core).wait_recv()
        return carry

    lax.fori_loop(0, PIECES, drain, 0)


def exchange(x, lhs, w0, wd, wo):
    rows, width = x.shape
    cols = width // 2 // PIECES
    n_ff = wd.shape[0]
    n_ctx = wo.shape[0]
    dma = pltpu.SemaphoreType.DMA
    return pl.pallas_call(
        exchange_kernel,
        name='exchange',
        in_specs=[HBM, VMEM, VMEM, HBM, HBM],
        out_specs=VMEM,
        out_shape=jax.ShapeDtypeStruct((rows, width), BF16),
        scratch_shapes=[
            pltpu.VMEM((rows, width), BF16),
            pltpu.VMEM((W_SLOTS, n_ff + n_ctx, 2 * cols), BF16),
            pltpu.VMEM((PIECES, rows, cols), BF16),
            pltpu.VMEM((PIECES, rows, cols), BF16),
            pltpu.VMEM((PIECES, rows, cols), F32),
            pltpu.VMEM((PIECES, rows, cols), BF16),
            pltpu.VMEM((PIECES, rows, cols), BF16),
            dma((1,)), dma((W_SLOTS,)),
            dma((PIECES,)), dma((PIECES,)), dma((PIECES,)), dma((PIECES,)), dma((PIECES,)), dma((PIECES,)),
        ],
        compiler_params=pltpu.CompilerParams(vmem_limit_bytes=32 * MIB, collective_id=0, has_side_effects=True),
        cost_estimate=pl.CostEstimate(flops=11 * 10 ** 9, bytes_accessed=48 * 10 ** 6, transcendentals=0),
    )(x, lhs, w0, wd, wo)


def solution(mesh):
    row_spec = P('dp', None)
    vec_spec = P(None)
    cache_spec = P('dp', 'tp', None, None)

    def device_step(x, ln_attn_gamma, ln_attn_beta, ln_mlp_gamma, ln_mlp_beta, w_qkv, w_out, w_up, w_down, k_cache, v_cache, positions):
        width = x.shape[1]
        head = w_qkv.shape[3]
        inv_freq = ROPE_BASE ** (-2.0 * np.arange(head // 2) / head)
        freq = jnp.asarray(np.concatenate([inv_freq, inv_freq])[None, :], F32)
        vecs = [v.reshape(1, width) for v in (ln_attn_gamma, ln_attn_beta, ln_mlp_gamma, ln_mlp_beta)]
        wq = jnp.transpose(w_qkv, (0, 2, 1, 3)).reshape(-1, head)
        wo = w_out.reshape(-1, width)
        in_hbm = [pltpu.with_memory_space_constraint(a, pltpu.HBM) for a in (positions, x, *vecs, freq, wq, w_up, w_down, wo, k_cache.reshape(-1, head), v_cache.reshape(-1, head))]
        x_h, wd_h, wo_h = in_hbm[1], in_hbm[-4], in_hbm[-3]
        ko, vo, lhs, w0 = front(*in_hbm)
        out = exchange(x_h, lhs, w0, wd_h, wo_h)
        return out, ko.reshape(k_cache.shape), vo.reshape(v_cache.shape)

    return jax.shard_map(device_step, mesh=mesh, in_specs=(row_spec, vec_spec, vec_spec, vec_spec, vec_spec, P(None, 'tp', None, None), P('tp', None, None, None), P(None, 'tp'), P('tp', None), cache_spec, cache_spec, P('dp')), out_specs=(row_spec, cache_spec, cache_spec), check_vma=False)
```

```python
import jax
import jax.numpy as jnp
import numpy as np
from jax import lax
from jax.experimental import pallas as pl
from jax.experimental.pallas import tpu as pltpu
from jax.sharding import PartitionSpec as P

LN_EPS = 1e-5
ROPE_BASE = 10000.0
NEG_BIG = -1e30
BF16 = jnp.bfloat16
F32 = jnp.float32
ANY = pl.BlockSpec(memory_space=pl.ANY)
HBM = pl.BlockSpec(memory_space=pltpu.HBM)
VMEM = pl.BlockSpec(memory_space=pltpu.VMEM)
SMEM = pl.BlockSpec(memory_space=pltpu.SMEM)
MIB = 1024 * 1024

QKV_CHUNK = 512
LN_ROWS = 16
ROW_BLOCK = 8
SUB_BLOCKS = 2
KV_SLOTS = 12
KV_AHEAD = 8
UP_SLOTS = 4
W_PARTS = 4


def front_kernel(pos_ref, x_hbm, ga_hbm, ba_hbm, gm_hbm, bm_hbm, freq_hbm, wq_hbm, wu_hbm, wd_hbm, wo_hbm, kc_hbm, vc_hbm,
                 ko_hbm, vo_hbm, lhs_ref, w0_ref,
                 x_s, vec_s, freq_s, cos_s, sin_s, attn_s, wqf_s, acc_s, q_s, kv_s, up_s, ctx_s, kbuf, vbuf,
                 in_sem, wq_sem, up_sem, kin_sem, vin_sem, kout_sem, vout_sem, w0_sem):
    mlp_s = x_s
    rows, width = x_s.shape
    seq = kc_hbm.shape[0] // (2 * rows)
    lines_blk = ROW_BLOCK * 2 * seq
    n_ff = lhs_ref.shape[1] - wo_hbm.shape[0]
    n_chunk = width // QKV_CHUNK
    lines = wq_hbm.shape[0] // width
    up_cols = up_s.shape[2]
    n_up = wu_hbm.shape[1] // up_cols
    n_blk = rows // ROW_BLOCK

    x_parts = [pl.ds(k * (rows // W_PARTS), rows // W_PARTS) for k in range(W_PARTS)]
    small = [pltpu.make_async_copy(x_hbm.at[part, :], x_s.at[part, :], in_sem.at[0]) for part in x_parts]
    for i, v in enumerate((ga_hbm, ba_hbm, gm_hbm, bm_hbm)):
        small.append(pltpu.make_async_copy(v, vec_s.at[pl.ds(i, 1), :], in_sem.at[1 + i]))
    freq_in = pltpu.make_async_copy(freq_hbm, freq_s, in_sem.at[5])
    freq_in.start()
    for c in small:
        c.start()

    wq_lines = QKV_CHUNK * lines
    wq_base = (KV_SLOTS - n_chunk * wq_lines // (2 * lines_blk)) * lines_blk
    wq_order = [c for pair in zip(range(n_chunk // 2), range(n_chunk // 2, n_chunk)) for c in pair]

    def wq_view(c):
        buf = kbuf if c < n_chunk // 2 else vbuf
        return buf.at[pl.ds(wq_base + (c % (n_chunk // 2)) * wq_lines, wq_lines), :]

    def wq_copy(c):
        return pltpu.make_async_copy(wq_hbm.at[pl.ds(c * wq_lines, wq_lines), :], wq_view(c), wq_sem.at[c])

    def up_start(b, slot):
        cols = pl.ds(pl.multiple_of(b * up_cols, up_cols), up_cols)
        for k in range(W_PARTS):
            part = pl.ds(k * (width // W_PARTS), width // W_PARTS)
            pltpu.make_async_copy(wu_hbm.at[part, cols], up_s.at[slot, part, :], up_sem.at[slot]).start()

    def up_wait(slot):
        pltpu.make_async_copy(wu_hbm.at[:, pl.ds(0, up_cols)], up_s.at[slot], up_sem.at[slot]).wait()

    def block(ref, i):
        return ref.at[pl.ds(pl.multiple_of(i * lines_blk, lines_blk), lines_blk), :]

    def start_in(i, slot):
        pltpu.make_async_copy(block(kc_hbm, i), block(kbuf, slot), kin_sem.at[slot]).start(priority=1)
        pltpu.make_async_copy(block(vc_hbm, i), block(vbuf, slot), vin_sem.at[slot]).start(priority=1)

    def wait_in(slot):
        pltpu.make_async_copy(block(kc_hbm, 0), block(kbuf, slot), kin_sem.at[slot]).wait()
        pltpu.make_async_copy(block(vc_hbm, 0), block(vbuf, slot), vin_sem.at[slot]).wait()

    def start_out(i, slot):
        pltpu.make_async_copy(block(kbuf, slot), block(ko_hbm, i), kout_sem.at[slot]).start()
        pltpu.make_async_copy(block(vbuf, slot), block(vo_hbm, i), vout_sem.at[slot]).start()

    def wait_out(slot):
        pltpu.make_async_copy(block(kbuf, slot), block(ko_hbm, 0), kout_sem.at[slot]).wait()
        pltpu.make_async_copy(block(vbuf, slot), block(vo_hbm, 0), vout_sem.at[slot]).wait()

    for c in wq_order[:2]:
        wq_copy(c).start()
    for i in range(2):
        start_in(i, i)

    freq_in.wait()

    def angle_body(b, carry):
        cos_s[pl.ds(b, 1), :] = pos_ref[b].astype(F32) * freq_s[0:1, :]
        return carry

    lax.fori_loop(0, rows, angle_body, 0, unroll=8)
    ang = cos_s[...]
    low = lax.broadcasted_iota(jnp.int32, ang.shape, 1) < 64
    sin_t = jnp.sin(ang)
    sin_s[...] = jnp.where(low, -sin_t, sin_t)
    cos_s[...] = jnp.cos(ang)

    for c in small:
        c.wait()
    for c in wq_order[2:4]:
        wq_copy(c).start()
    for i in range(2, 4):
        start_in(i, i)

    def ln_body(i, carry):
        r = pl.ds(pl.multiple_of(i * LN_ROWS, LN_ROWS), LN_ROWS)
        xf = x_s[r, :].astype(F32)
        mean = jnp.mean(xf, axis=-1, keepdims=True)
        cen = xf - mean
        var = jnp.mean(cen * cen, axis=-1, keepdims=True)
        nrm = cen * lax.rsqrt(var + LN_EPS)
        attn_s[r, :] = (nrm * vec_s[0:1, :] + vec_s[1:2, :]).astype(BF16)
        mlp_s[r, :] = (nrm * vec_s[2:3, :] + vec_s[3:4, :]).astype(BF16)
        return carry

    half_ln = rows // LN_ROWS // 2
    lax.fori_loop(0, half_ln, ln_body, 0)
    for c in wq_order[4:]:
        wq_copy(c).start()
    for i in range(4, 6):
        start_in(i, i)
    lax.fori_loop(half_ln, 2 * half_ln, ln_body, 0)

    for step, c in enumerate(wq_order):
        wq_copy(c).wait()
        if 6 <= step < KV_AHEAD:
            start_in(step, step)
        if step >= n_chunk - UP_SLOTS:
            up_start(step - n_chunk + UP_SLOTS, step - n_chunk + UP_SLOTS)
        wqf_s[...] = wq_view(c)[...].astype(F32)
        lhs = attn_s[:, c * QKV_CHUNK:(c + 1) * QKV_CHUNK]
        for pair in range(lines // 2):
            w = jnp.concatenate([wqf_s[pl.ds(2 * pair + e, QKV_CHUNK, stride=lines), :].astype(BF16) for e in range(2)], axis=1)
            part = jnp.dot(lhs, w, preferred_element_type=F32)
            if step == 0:
                acc_s[:, pair * 256:(pair + 1) * 256] = part
            else:
                acc_s[:, pair * 256:(pair + 1) * 256] += part

    n_slot = lines // 2
    n_q = n_slot - 2
    for j in range(n_slot):
        for g in range(2):
            col = (2 * j + g) * 128
            u = acc_s[:, col:col + 128].astype(BF16).astype(F32)
            if j < n_q + 1:
                u = (u * cos_s[...] + pltpu.roll(u, 64, 1) * sin_s[...]).astype(BF16).astype(F32)
            if j < n_q:
                q_s[pl.ds((g * n_q + j) * rows, rows), :] = u
            else:
                kv_s[pl.ds(((j - n_q) * 2 + g) * rows, rows), :] = u

    slot_ids = lax.broadcasted_iota(jnp.int32, (8, 256), 1)
    tile_ids = lax.broadcasted_iota(jnp.int32, (16, 128), 0)
    first = lax.broadcasted_iota(jnp.int32, (8, 128), 0) < 4
    scale = 128 ** -0.5

    def pair_of(buf, slot, r):
        at = [pl.ds(pl.multiple_of(slot * lines_blk + (2 * r + g) * seq, seq), seq) for g in range(2)]
        return jnp.concatenate([buf[a, :] for a in at], axis=1)

    def attend_block(i, slot):
        pos = [pos_ref[i * ROW_BLOCK + r] for r in range(ROW_BLOCK)]
        for r in range(ROW_BLOCK):
            base = pl.multiple_of((pos[r] // 16) * 16, 16)
            hit = tile_ids == pos[r] - base
            b = i * ROW_BLOCK + r
            for g in range(2):
                tile = pl.ds(pl.multiple_of(slot * lines_blk + (2 * r + g) * seq + base, 16), 16)
                for buf, which in ((kbuf, 0), (vbuf, 1)):
                    new = kv_s[pl.ds((which * 2 + g) * rows + b, 1), :]
                    buf[tile, :] = jnp.where(hit, new, buf[tile, :].astype(F32)).astype(BF16)
        scores = []
        for r in range(ROW_BLOCK):
            b = i * ROW_BLOCK + r
            q = q_s[pl.ds(b, 8, stride=rows), :]
            zero = jnp.zeros_like(q)
            q2 = jnp.concatenate([jnp.where(first, q, zero), jnp.where(first, zero, q)], axis=1).astype(BF16)
            k2 = pair_of(kbuf, slot, r)
            s = lax.dot_general(q2, k2, (((1,), (1,)), ((), ())), preferred_element_type=F32) * scale
            scores.append(jnp.where(slot_ids <= pos[r], s, NEG_BIG))
        s = jnp.concatenate(scores, axis=0)
        e = jnp.exp(s - jnp.max(s, axis=-1, keepdims=True))
        p = (e / jnp.sum(e, axis=-1, keepdims=True)).astype(BF16)
        for r in range(ROW_BLOCK):
            v2 = pair_of(vbuf, slot, r)
            c = jnp.dot(p[8 * r:8 * r + 8], v2, preferred_element_type=F32)
            ctx_s[pl.ds(i * ROW_BLOCK + r, 8, stride=rows), :] = jnp.where(first, c[:, :128], c[:, 128:])

    core = lax.rem(lax.axis_index('tp'), 2)
    cols = w0_ref.shape[1] // 2
    w0_in = []
    for part in range(2):
        src = pl.ds(pl.multiple_of((core if part else 1 - core) * (wd_hbm.shape[1] // 2), cols), cols)
        dst = pl.ds(part * cols, cols)
        w0_in.append(pltpu.make_async_copy(wd_hbm.at[:, src], w0_ref.at[pl.ds(0, n_ff), dst], w0_sem.at[0]))
        w0_in.append(pltpu.make_async_copy(wo_hbm.at[:, src], w0_ref.at[pl.ds(n_ff, wo_hbm.shape[0]), dst], w0_sem.at[0]))

    def body(i, carry):
        for s in range(SUB_BLOCKS):
            nxt = i * SUB_BLOCKS + s + KV_AHEAD

            @pl.when(nxt < n_blk)
            def _():
                nslot = lax.rem(nxt, KV_SLOTS)

                @pl.when(nxt >= KV_SLOTS)
                def _():
                    wait_out(nslot)
                start_in(nxt, nslot)

        @pl.when((i >= 1) & (i - 1 + UP_SLOTS < n_up))
        def _():
            up_start(i - 1 + UP_SLOTS, lax.rem(i - 1, UP_SLOTS))

        uslot = lax.rem(i, UP_SLOTS)
        up_wait(uslot)
        for s in range(SUB_BLOCKS):
            wait_in(lax.rem(i * SUB_BLOCKS + s, KV_SLOTS))
        deep = width // 2
        pre = (jnp.dot(mlp_s[:, :deep], up_s[uslot, :deep, :], preferred_element_type=F32)
               + jnp.dot(mlp_s[:, deep:], up_s[uslot, deep:, :], preferred_element_type=F32))
        act = 0.5 * pre * (1.0 + lax.erf(pre * (0.5 ** 0.5)))
        lhs_ref[:, pl.ds(pl.multiple_of(i * up_cols, up_cols), up_cols)] = act.astype(BF16)
        for s in range(SUB_BLOCKS):
            blk = i * SUB_BLOCKS + s
            attend_block(blk, lax.rem(blk, KV_SLOTS))
        for s in range(SUB_BLOCKS):
            blk = i * SUB_BLOCKS + s
            start_out(blk, lax.rem(blk, KV_SLOTS))

        @pl.when(i == n_up - 4)
        def _():
            for c in w0_in:
                c.start(priority=1)
        return carry

    lax.fori_loop(0, n_up, body, 0)
    for h in range(ctx_s.shape[0] // rows):
        lhs_ref[:, n_ff + h * 128:n_ff + (h + 1) * 128] = ctx_s[h * rows:(h + 1) * rows, :].astype(BF16)
    for c in w0_in:
        c.wait()
    for i in range(n_blk - KV_SLOTS, n_blk):
        wait_out(i % KV_SLOTS)


def front(pos, x, ga, ba, gm, bm, freq, wq, wu, wd, wo, kc, vc):
    rows, width = x.shape
    hid = wu.shape[1]
    lines = wq.shape[0] // width
    n_head = (lines // 2 - 2) * 2
    up_cols = hid // (rows // (ROW_BLOCK * SUB_BLOCKS))
    lines_blk = kc.shape[0] // rows * ROW_BLOCK
    return pl.pallas_call(
        front_kernel,
        name='front',
        in_specs=[SMEM] + [HBM] * 12,
        out_specs=[HBM, HBM, VMEM, VMEM],
        out_shape=[
            jax.ShapeDtypeStruct(kc.shape, BF16),
            jax.ShapeDtypeStruct(vc.shape, BF16),
            jax.ShapeDtypeStruct((rows, hid + wo.shape[0]), BF16),
            jax.ShapeDtypeStruct((hid + wo.shape[0], width // PIECES), BF16),
        ],
        scratch_shapes=[
            pltpu.VMEM((rows, width), BF16),
            pltpu.VMEM((4, width), F32),
            pltpu.VMEM((1, 128), F32),
            pltpu.VMEM((rows, 128), F32),
            pltpu.VMEM((rows, 128), F32),
            pltpu.VMEM((rows, width), BF16),
            pltpu.VMEM((QKV_CHUNK * lines, 128), F32),
            pltpu.VMEM((rows, lines * 128), F32),
            pltpu.VMEM((n_head * rows, 128), F32),
            pltpu.VMEM((4 * rows, 128), F32),
            pltpu.VMEM((UP_SLOTS, width, up_cols), BF16),
            pltpu.VMEM((n_head * rows, 128), F32),
            pltpu.VMEM((KV_SLOTS * lines_blk, 128), BF16),
            pltpu.VMEM((KV_SLOTS * lines_blk, 128), BF16),
            pltpu.SemaphoreType.DMA((6,)),
            pltpu.SemaphoreType.DMA((width // QKV_CHUNK,)),
            pltpu.SemaphoreType.DMA((UP_SLOTS,)),
            pltpu.SemaphoreType.DMA((KV_SLOTS,)),
            pltpu.SemaphoreType.DMA((KV_SLOTS,)),
            pltpu.SemaphoreType.DMA((KV_SLOTS,)),
            pltpu.SemaphoreType.DMA((KV_SLOTS,)),
            pltpu.SemaphoreType.DMA((1,)),
        ],
        compiler_params=pltpu.CompilerParams(vmem_limit_bytes=44 * MIB),
        cost_estimate=pl.CostEstimate(flops=22 * 10 ** 9, bytes_accessed=180 * 10 ** 6, transcendentals=0),
    )(pos, x, ga, ba, gm, bm, freq, wq, wu, wd, wo, kc, vc)


PIECES = 16
W_SLOTS = 4
MESH = pl.DeviceIdType.MESH


def exchange_kernel(x_hbm, lhs_s, w0_ref, wd_hbm, wo_hbm, out_ref,
                    x_s, w_s, send_s, recv_s, keep_s, sum_s, other_s,
                    in_sem, w_sem, c1_send, c1_recv, c2_send, c2_recv, c3_send, c3_recv):
    rows, width = x_s.shape
    half = width // 2
    cols = half // PIECES
    n_ff, n_ctx = wd_hbm.shape[0], wo_hbm.shape[0]
    me = lax.axis_index('tp')
    core = lax.rem(me, 2)
    mate = me + 1 - 2 * core
    far = lax.rem(me + 2, 4)

    def col_of(p, part):
        side = core if part else 1 - core
        return pl.multiple_of(side * half + p * cols, cols)

    def w_start(p):
        slot = lax.rem(p, W_SLOTS)
        for part in range(2):
            src, dst = pl.ds(col_of(p, part), cols), pl.ds(part * cols, cols)
            pltpu.make_async_copy(wo_hbm.at[:, src], w_s.at[slot, pl.ds(n_ff, n_ctx), dst], w_sem.at[slot]).start()
            for k in range(2):
                deep = pl.ds(k * (n_ff // 2), n_ff // 2)
                pltpu.make_async_copy(wd_hbm.at[deep, src], w_s.at[slot, deep, dst], w_sem.at[slot]).start()

    def w_wait(p):
        slot = lax.rem(p, W_SLOTS)
        for part in range(2):
            dst = pl.ds(part * cols, cols)
            pltpu.make_async_copy(wo_hbm.at[:, pl.ds(0, cols)], w_s.at[slot, pl.ds(n_ff, n_ctx), dst], w_sem.at[slot]).wait()
            pltpu.make_async_copy(wd_hbm.at[:, pl.ds(0, cols)], w_s.at[slot, pl.ds(0, n_ff), dst], w_sem.at[slot]).wait()

    w_start(1)
    x_in = pltpu.make_async_copy(x_hbm, x_s, in_sem.at[0])

    barrier = pltpu.get_barrier_semaphore()
    for peer in (mate, far):
        pl.semaphore_signal(barrier, inc=1, device_id={'tp': peer}, device_id_type=MESH)
    pl.semaphore_wait(barrier, 2)

    def copy1(p):
        return pltpu.make_async_remote_copy(send_s.at[p], recv_s.at[p], c1_send.at[p], c1_recv.at[p], device_id={'tp': mate}, device_id_type=MESH)

    def copy2(p):
        return pltpu.make_async_remote_copy(sum_s.at[p], other_s.at[p], c2_send.at[p], c2_recv.at[p], device_id={'tp': far}, device_id_type=MESH)

    def copy3(p, side):
        view = out_ref.at[:, pl.ds(pl.multiple_of(side * half + p * cols, cols), cols)]
        return pltpu.make_async_remote_copy(view, view, c3_send.at[p], c3_recv.at[p], device_id={'tp': mate}, device_id_type=MESH)

    def chip_sum(p):
        copy1(p).wait_recv()
        sum_s[p] = (keep_s[p] + recv_s[p].astype(F32)).astype(BF16)
        copy2(p).start()

    def partial(p, w):
        deep = (n_ff + n_ctx) // 2
        s = (jnp.dot(lhs_s[:, :deep], w[:deep, :], preferred_element_type=F32)
             + jnp.dot(lhs_s[:, deep:], w[deep:, :], preferred_element_type=F32))
        send_s[p] = s[:, :cols].astype(BF16)
        keep_s[p] = s[:, cols:]
        copy1(p).start()

    partial(0, w0_ref)
    w_start(2)
    chip_sum(0)
    w_start(3)
    x_in.start()

    def compute(p, carry):
        w_wait(p)

        @pl.when(p + 3 < PIECES)
        def _():
            w_start(p + 3)
        partial(p, w_s.at[lax.rem(p, W_SLOTS)])

        @pl.when(p > 1)
        def _():
            chip_sum(p - 1)
        return carry

    lax.fori_loop(1, PIECES, compute, 0)
    chip_sum(PIECES - 1)
    x_in.wait()

    def finish(p, carry):
        copy1(p).wait_send()
        copy2(p).wait_send()
        copy2(p).wait_recv()
        xs = x_s[:, pl.ds(col_of(p, 1), cols)].astype(F32)
        out_ref[:, pl.ds(col_of(p, 1), cols)] = (xs + (sum_s[p].astype(F32) + other_s[p].astype(F32))).astype(BF16)
        copy3(p, core).start()
        return carry

    lax.fori_loop(0, PIECES, finish, 0)

    def drain(p, carry):
        copy3(p, core).wait_send()
        copy3(p, 1 - core).wait_recv()
        return carry

    lax.fori_loop(0, PIECES, drain, 0)


def exchange(x, lhs, w0, wd, wo):
    rows, width = x.shape
    cols = width // 2 // PIECES
    n_ff = wd.shape[0]
    n_ctx = wo.shape[0]
    dma = pltpu.SemaphoreType.DMA
    return pl.pallas_call(
        exchange_kernel,
        name='exchange',
        in_specs=[HBM, VMEM, VMEM, HBM, HBM],
        out_specs=VMEM,
        out_shape=jax.ShapeDtypeStruct((rows, width), BF16),
        scratch_shapes=[
            pltpu.VMEM((rows, width), BF16),
            pltpu.VMEM((W_SLOTS, n_ff + n_ctx, 2 * cols), BF16),
            pltpu.VMEM((PIECES, rows, cols), BF16),
            pltpu.VMEM((PIECES, rows, cols), BF16),
            pltpu.VMEM((PIECES, rows, cols), F32),
            pltpu.VMEM((PIECES, rows, cols), BF16),
            pltpu.VMEM((PIECES, rows, cols), BF16),
            dma((1,)), dma((W_SLOTS,)),
            dma((PIECES,)), dma((PIECES,)), dma((PIECES,)), dma((PIECES,)), dma((PIECES,)), dma((PIECES,)),
        ],
        compiler_params=pltpu.CompilerParams(vmem_limit_bytes=32 * MIB, collective_id=0, has_side_effects=True),
        cost_estimate=pl.CostEstimate(flops=11 * 10 ** 9, bytes_accessed=48 * 10 ** 6, transcendentals=0),
    )(x, lhs, w0, wd, wo)


def solution(mesh):
    row_spec = P('dp', None)
    vec_spec = P(None)
    cache_spec = P('dp', 'tp', None, None)

    def device_step(x, ln_attn_gamma, ln_attn_beta, ln_mlp_gamma, ln_mlp_beta, w_qkv, w_out, w_up, w_down, k_cache, v_cache, positions):
        width = x.shape[1]
        head = w_qkv.shape[3]
        inv_freq = ROPE_BASE ** (-2.0 * np.arange(head // 2) / head)
        freq = jnp.asarray(np.concatenate([inv_freq, inv_freq])[None, :], F32)
        vecs = [v.reshape(1, width) for v in (ln_attn_gamma, ln_attn_beta, ln_mlp_gamma, ln_mlp_beta)]
        wq = jnp.transpose(w_qkv, (0, 2, 1, 3)).reshape(-1, head)
        wo = w_out.reshape(-1, width)
        in_hbm = [pltpu.with_memory_space_constraint(a, pltpu.HBM) for a in (positions, x, *vecs, freq, wq, w_up, w_down, wo, k_cache.reshape(-1, head), v_cache.reshape(-1, head))]
        x_h, wd_h, wo_h = in_hbm[1], in_hbm[-4], in_hbm[-3]
        ko, vo, lhs, w0 = front(*in_hbm)
        out = exchange(x_h, lhs, w0, wd_h, wo_h)
        return out, ko.reshape(k_cache.shape), vo.reshape(v_cache.shape)

    return jax.shard_map(device_step, mesh=mesh, in_specs=(row_spec, vec_spec, vec_spec, vec_spec, vec_spec, P(None, 'tp', None, None), P('tp', None, None, None), P(None, 'tp'), P('tp', None), cache_spec, cache_spec, P('dp')), out_specs=(row_spec, cache_spec, cache_spec), check_vma=False)
```

```python
import jax
import jax.numpy as jnp
import numpy as np
from jax import lax
from jax.experimental import pallas as pl
from jax.experimental.pallas import tpu as pltpu
from jax.sharding import PartitionSpec as P

LN_EPS = 1e-5
ROPE_BASE = 10000.0
NEG_BIG = -1e30
BF16 = jnp.bfloat16
F32 = jnp.float32
ANY = pl.BlockSpec(memory_space=pl.ANY)
HBM = pl.BlockSpec(memory_space=pltpu.HBM)
VMEM = pl.BlockSpec(memory_space=pltpu.VMEM)
SMEM = pl.BlockSpec(memory_space=pltpu.SMEM)
MIB = 1024 * 1024

QKV_CHUNK = 512
LN_ROWS = 16
ROW_BLOCK = 16
SUB_BLOCKS = 1
KV_SLOTS = 6
KV_AHEAD = 4
UP_SLOTS = 4
W_PARTS = 4


def front_kernel(pos_ref, x_hbm, ga_hbm, ba_hbm, gm_hbm, bm_hbm, freq_hbm, wq_hbm, wu_hbm, wd_hbm, wo_hbm, kc_hbm, vc_hbm,
                 ko_hbm, vo_hbm, lhs_ref, w0_ref,
                 x_s, vec_s, freq_s, cos_s, sin_s, attn_s, wqf_s, acc_s, q_s, kv_s, up_s, ctx_s, kbuf, vbuf,
                 in_sem, wq_sem, up_sem, kin_sem, vin_sem, kout_sem, vout_sem, w0_sem):
    mlp_s = x_s
    rows, width = x_s.shape
    seq = kc_hbm.shape[0] // (2 * rows)
    lines_blk = ROW_BLOCK * 2 * seq
    n_ff = lhs_ref.shape[1] - wo_hbm.shape[0]
    n_chunk = width // QKV_CHUNK
    lines = wq_hbm.shape[0] // width
    up_cols = up_s.shape[2]
    n_up = wu_hbm.shape[1] // up_cols
    n_blk = rows // ROW_BLOCK

    x_parts = [pl.ds(k * (rows // W_PARTS), rows // W_PARTS) for k in range(W_PARTS)]
    small = [pltpu.make_async_copy(x_hbm.at[part, :], x_s.at[part, :], in_sem.at[0]) for part in x_parts]
    for i, v in enumerate((ga_hbm, ba_hbm, gm_hbm, bm_hbm)):
        small.append(pltpu.make_async_copy(v, vec_s.at[pl.ds(i, 1), :], in_sem.at[1 + i]))
    freq_in = pltpu.make_async_copy(freq_hbm, freq_s, in_sem.at[5])
    freq_in.start()
    for c in small:
        c.start()

    wq_lines = QKV_CHUNK * lines
    wq_base = (KV_SLOTS - n_chunk * wq_lines // (2 * lines_blk)) * lines_blk
    wq_order = [c for pair in zip(range(n_chunk // 2), range(n_chunk // 2, n_chunk)) for c in pair]

    def wq_view(c):
        buf = kbuf if c < n_chunk // 2 else vbuf
        return buf.at[pl.ds(wq_base + (c % (n_chunk // 2)) * wq_lines, wq_lines), :]

    def wq_copy(c):
        return pltpu.make_async_copy(wq_hbm.at[pl.ds(c * wq_lines, wq_lines), :], wq_view(c), wq_sem.at[c])

    def up_start(b, slot):
        cols = pl.ds(pl.multiple_of(b * up_cols, up_cols), up_cols)
        for k in range(W_PARTS):
            part = pl.ds(k * (width // W_PARTS), width // W_PARTS)
            pltpu.make_async_copy(wu_hbm.at[part, cols], up_s.at[slot, part, :], up_sem.at[slot]).start()

    def up_wait(slot):
        pltpu.make_async_copy(wu_hbm.at[:, pl.ds(0, up_cols)], up_s.at[slot], up_sem.at[slot]).wait()

    def block(ref, i):
        return ref.at[pl.ds(pl.multiple_of(i * lines_blk, lines_blk), lines_blk), :]

    def start_in(i, slot):
        pltpu.make_async_copy(block(kc_hbm, i), block(kbuf, slot), kin_sem.at[slot]).start(priority=1)
        pltpu.make_async_copy(block(vc_hbm, i), block(vbuf, slot), vin_sem.at[slot]).start(priority=1)

    def wait_in(slot):
        pltpu.make_async_copy(block(kc_hbm, 0), block(kbuf, slot), kin_sem.at[slot]).wait()
        pltpu.make_async_copy(block(vc_hbm, 0), block(vbuf, slot), vin_sem.at[slot]).wait()

    def start_out(i, slot):
        pltpu.make_async_copy(block(kbuf, slot), block(ko_hbm, i), kout_sem.at[slot]).start()
        pltpu.make_async_copy(block(vbuf, slot), block(vo_hbm, i), vout_sem.at[slot]).start()

    def wait_out(slot):
        pltpu.make_async_copy(block(kbuf, slot), block(ko_hbm, 0), kout_sem.at[slot]).wait()
        pltpu.make_async_copy(block(vbuf, slot), block(vo_hbm, 0), vout_sem.at[slot]).wait()

    for c in wq_order[:2]:
        wq_copy(c).start()
    start_in(0, 0)

    freq_in.wait()

    def angle_body(b, carry):
        cos_s[pl.ds(b, 1), :] = pos_ref[b].astype(F32) * freq_s[0:1, :]
        return carry

    lax.fori_loop(0, rows, angle_body, 0, unroll=8)
    ang = cos_s[...]
    low = lax.broadcasted_iota(jnp.int32, ang.shape, 1) < 64
    sin_t = jnp.sin(ang)
    sin_s[...] = jnp.where(low, -sin_t, sin_t)
    cos_s[...] = jnp.cos(ang)

    for c in small:
        c.wait()
    for c in wq_order[2:4]:
        wq_copy(c).start()
    start_in(1, 1)

    def ln_body(i, carry):
        r = pl.ds(pl.multiple_of(i * LN_ROWS, LN_ROWS), LN_ROWS)
        xf = x_s[r, :].astype(F32)
        mean = jnp.mean(xf, axis=-1, keepdims=True)
        cen = xf - mean
        var = jnp.mean(cen * cen, axis=-1, keepdims=True)
        nrm = cen * lax.rsqrt(var + LN_EPS)
        attn_s[r, :] = (nrm * vec_s[0:1, :] + vec_s[1:2, :]).astype(BF16)
        mlp_s[r, :] = (nrm * vec_s[2:3, :] + vec_s[3:4, :]).astype(BF16)
        return carry

    half_ln = rows // LN_ROWS // 2
    lax.fori_loop(0, half_ln, ln_body, 0)
    for c in wq_order[4:]:
        wq_copy(c).start()
    free = wq_base // lines_blk
    for i in range(2, free):
        start_in(i, i)
    lax.fori_loop(half_ln, 2 * half_ln, ln_body, 0)

    for step, c in enumerate(wq_order):
        wq_copy(c).wait()
        if step == n_chunk - 2:
            for i in range(free, KV_AHEAD):
                start_in(i, i)
        if step >= n_chunk - UP_SLOTS:
            up_start(step - n_chunk + UP_SLOTS, step - n_chunk + UP_SLOTS)
        wqf_s[...] = wq_view(c)[...].astype(F32)
        lhs = attn_s[:, c * QKV_CHUNK:(c + 1) * QKV_CHUNK]
        for pair in range(lines // 2):
            w = jnp.concatenate([wqf_s[pl.ds(2 * pair + e, QKV_CHUNK, stride=lines), :].astype(BF16) for e in range(2)], axis=1)
            part = jnp.dot(lhs, w, preferred_element_type=F32)
            if step == 0:
                acc_s[:, pair * 256:(pair + 1) * 256] = part
            else:
                acc_s[:, pair * 256:(pair + 1) * 256] += part

    n_slot = lines // 2
    n_q = n_slot - 2
    for j in range(n_slot):
        for g in range(2):
            col = (2 * j + g) * 128
            u = acc_s[:, col:col + 128].astype(BF16).astype(F32)
            if j < n_q + 1:
                u = (u * cos_s[...] + pltpu.roll(u, 64, 1) * sin_s[...]).astype(BF16).astype(F32)
            if j < n_q:
                q_s[pl.ds((g * n_q + j) * rows, rows), :] = u
            else:
                kv_s[pl.ds(((j - n_q) * 2 + g) * rows, rows), :] = u

    slot_ids = lax.broadcasted_iota(jnp.int32, (8, 256), 1)
    tile_ids = lax.broadcasted_iota(jnp.int32, (16, 128), 0)
    first = lax.broadcasted_iota(jnp.int32, (8, 128), 0) < 4
    scale = 128 ** -0.5

    def pair_of(buf, slot, r):
        at = [pl.ds(pl.multiple_of(slot * lines_blk + (2 * r + g) * seq, seq), seq) for g in range(2)]
        return jnp.concatenate([buf[a, :] for a in at], axis=1)

    def attend_block(i, slot):
        pos = [pos_ref[i * ROW_BLOCK + r] for r in range(ROW_BLOCK)]
        for r in range(ROW_BLOCK):
            base = pl.multiple_of((pos[r] // 16) * 16, 16)
            hit = tile_ids == pos[r] - base
            b = i * ROW_BLOCK + r
            for g in range(2):
                tile = pl.ds(pl.multiple_of(slot * lines_blk + (2 * r + g) * seq + base, 16), 16)
                for buf, which in ((kbuf, 0), (vbuf, 1)):
                    new = kv_s[pl.ds((which * 2 + g) * rows + b, 1), :]
                    buf[tile, :] = jnp.where(hit, new, buf[tile, :].astype(F32)).astype(BF16)
        scores = []
        for r in range(ROW_BLOCK):
            b = i * ROW_BLOCK + r
            q = q_s[pl.ds(b, 8, stride=rows), :]
            zero = jnp.zeros_like(q)
            q2 = jnp.concatenate([jnp.where(first, q, zero), jnp.where(first, zero, q)], axis=1).astype(BF16)
            k2 = pair_of(kbuf, slot, r)
            s = lax.dot_general(q2, k2, (((1,), (1,)), ((), ())), preferred_element_type=F32) * scale
            scores.append(jnp.where(slot_ids <= pos[r], s, NEG_BIG))
        s = jnp.concatenate(scores, axis=0)
        e = jnp.exp(s - jnp.max(s, axis=-1, keepdims=True))
        p = (e / jnp.sum(e, axis=-1, keepdims=True)).astype(BF16)
        for r in range(ROW_BLOCK):
            v2 = pair_of(vbuf, slot, r)
            c = jnp.dot(p[8 * r:8 * r + 8], v2, preferred_element_type=F32)
            ctx_s[pl.ds(i * ROW_BLOCK + r, 8, stride=rows), :] = jnp.where(first, c[:, :128], c[:, 128:])

    core = lax.rem(lax.axis_index('tp'), 2)
    cols = w0_ref.shape[1] // 2
    w0_in = []
    for part in range(2):
        src = pl.ds(pl.multiple_of((core if part else 1 - core) * (wd_hbm.shape[1] // 2), cols), cols)
        dst = pl.ds(part * cols, cols)
        w0_in.append(pltpu.make_async_copy(wd_hbm.at[:, src], w0_ref.at[pl.ds(0, n_ff), dst], w0_sem.at[0]))
        w0_in.append(pltpu.make_async_copy(wo_hbm.at[:, src], w0_ref.at[pl.ds(n_ff, wo_hbm.shape[0]), dst], w0_sem.at[0]))

    def body(i, carry):
        for s in range(SUB_BLOCKS):
            nxt = i * SUB_BLOCKS + s + KV_AHEAD

            @pl.when(nxt < n_blk)
            def _():
                nslot = lax.rem(nxt, KV_SLOTS)

                @pl.when(nxt >= KV_SLOTS)
                def _():
                    wait_out(nslot)
                start_in(nxt, nslot)

        @pl.when((i >= 1) & (i - 1 + UP_SLOTS < n_up))
        def _():
            up_start(i - 1 + UP_SLOTS, lax.rem(i - 1, UP_SLOTS))

        uslot = lax.rem(i, UP_SLOTS)
        up_wait(uslot)
        for s in range(SUB_BLOCKS):
            wait_in(lax.rem(i * SUB_BLOCKS + s, KV_SLOTS))
        deep = width // 2
        pre = (jnp.dot(mlp_s[:, :deep], up_s[uslot, :deep, :], preferred_element_type=F32)
               + jnp.dot(mlp_s[:, deep:], up_s[uslot, deep:, :], preferred_element_type=F32))
        act = 0.5 * pre * (1.0 + lax.erf(pre * (0.5 ** 0.5)))
        lhs_ref[:, pl.ds(pl.multiple_of(i * up_cols, up_cols), up_cols)] = act.astype(BF16)
        for s in range(SUB_BLOCKS):
            blk = i * SUB_BLOCKS + s
            attend_block(blk, lax.rem(blk, KV_SLOTS))
        for s in range(SUB_BLOCKS):
            blk = i * SUB_BLOCKS + s
            start_out(blk, lax.rem(blk, KV_SLOTS))

        @pl.when(i == n_up - 4)
        def _():
            for c in w0_in:
                c.start(priority=1)
        return carry

    lax.fori_loop(0, n_up, body, 0)
    for h in range(ctx_s.shape[0] // rows):
        lhs_ref[:, n_ff + h * 128:n_ff + (h + 1) * 128] = ctx_s[h * rows:(h + 1) * rows, :].astype(BF16)
    for c in w0_in:
        c.wait()
    for i in range(n_blk - KV_SLOTS, n_blk):
        wait_out(i % KV_SLOTS)


def front(pos, x, ga, ba, gm, bm, freq, wq, wu, wd, wo, kc, vc):
    rows, width = x.shape
    hid = wu.shape[1]
    lines = wq.shape[0] // width
    n_head = (lines // 2 - 2) * 2
    up_cols = hid // (rows // (ROW_BLOCK * SUB_BLOCKS))
    lines_blk = kc.shape[0] // rows * ROW_BLOCK
    return pl.pallas_call(
        front_kernel,
        name='front',
        in_specs=[SMEM] + [HBM] * 12,
        out_specs=[HBM, HBM, VMEM, VMEM],
        out_shape=[
            jax.ShapeDtypeStruct(kc.shape, BF16),
            jax.ShapeDtypeStruct(vc.shape, BF16),
            jax.ShapeDtypeStruct((rows, hid + wo.shape[0]), BF16),
            jax.ShapeDtypeStruct((hid + wo.shape[0], width // PIECES), BF16),
        ],
        scratch_shapes=[
            pltpu.VMEM((rows, width), BF16),
            pltpu.VMEM((4, width), F32),
            pltpu.VMEM((1, 128), F32),
            pltpu.VMEM((rows, 128), F32),
            pltpu.VMEM((rows, 128), F32),
            pltpu.VMEM((rows, width), BF16),
            pltpu.VMEM((QKV_CHUNK * lines, 128), F32),
            pltpu.VMEM((rows, lines * 128), F32),
            pltpu.VMEM((n_head * rows, 128), F32),
            pltpu.VMEM((4 * rows, 128), F32),
            pltpu.VMEM((UP_SLOTS, width, up_cols), BF16),
            pltpu.VMEM((n_head * rows, 128), F32),
            pltpu.VMEM((KV_SLOTS * lines_blk, 128), BF16),
            pltpu.VMEM((KV_SLOTS * lines_blk, 128), BF16),
            pltpu.SemaphoreType.DMA((6,)),
            pltpu.SemaphoreType.DMA((width // QKV_CHUNK,)),
            pltpu.SemaphoreType.DMA((UP_SLOTS,)),
            pltpu.SemaphoreType.DMA((KV_SLOTS,)),
            pltpu.SemaphoreType.DMA((KV_SLOTS,)),
            pltpu.SemaphoreType.DMA((KV_SLOTS,)),
            pltpu.SemaphoreType.DMA((KV_SLOTS,)),
            pltpu.SemaphoreType.DMA((1,)),
        ],
        compiler_params=pltpu.CompilerParams(vmem_limit_bytes=44 * MIB),
        cost_estimate=pl.CostEstimate(flops=22 * 10 ** 9, bytes_accessed=180 * 10 ** 6, transcendentals=0),
    )(pos, x, ga, ba, gm, bm, freq, wq, wu, wd, wo, kc, vc)


PIECES = 16
GROUPS = ((0, 1), (1, 2), (3, 5), (8, 5), (13, 2), (15, 1))
W_SLOTS = 4
MESH = pl.DeviceIdType.MESH


def exchange_kernel(x_hbm, lhs_s, w0_ref, wd_hbm, wo_hbm, out_ref,
                    x_s, w_s, send_s, recv_s, keep_s, sum_s, other_s,
                    in_sem, w_sem, c1_send, c1_recv, c2_send, c2_recv, c3_send, c3_recv):
    rows, width = x_s.shape
    half = width // 2
    cols = half // PIECES
    n_ff, n_ctx = wd_hbm.shape[0], wo_hbm.shape[0]
    me = lax.axis_index('tp')
    core = lax.rem(me, 2)
    mate = me + 1 - 2 * core
    far = lax.rem(me + 2, 4)

    def col_of(p, part):
        side = core if part else 1 - core
        return pl.multiple_of(side * half + p * cols, cols)

    def w_start(p):
        slot = lax.rem(p, W_SLOTS)
        for part in range(2):
            src, dst = pl.ds(col_of(p, part), cols), pl.ds(part * cols, cols)
            pltpu.make_async_copy(wo_hbm.at[:, src], w_s.at[slot, pl.ds(n_ff, n_ctx), dst], w_sem.at[slot]).start()
            for k in range(2):
                deep = pl.ds(k * (n_ff // 2), n_ff // 2)
                pltpu.make_async_copy(wd_hbm.at[deep, src], w_s.at[slot, deep, dst], w_sem.at[slot]).start()

    def w_wait(p):
        slot = lax.rem(p, W_SLOTS)
        for part in range(2):
            dst = pl.ds(part * cols, cols)
            pltpu.make_async_copy(wo_hbm.at[:, pl.ds(0, cols)], w_s.at[slot, pl.ds(n_ff, n_ctx), dst], w_sem.at[slot]).wait()
            pltpu.make_async_copy(wd_hbm.at[:, pl.ds(0, cols)], w_s.at[slot, pl.ds(0, n_ff), dst], w_sem.at[slot]).wait()

    w_start(1)
    x_in = pltpu.make_async_copy(x_hbm, x_s, in_sem.at[0])

    barrier = pltpu.get_barrier_semaphore()
    for peer in (mate, far):
        pl.semaphore_signal(barrier, inc=1, device_id={'tp': peer}, device_id_type=MESH)
    pl.semaphore_wait(barrier, 2)

    def copy1(p):
        return pltpu.make_async_remote_copy(send_s.at[p], recv_s.at[p], c1_send.at[p], c1_recv.at[p], device_id={'tp': mate}, device_id_type=MESH)

    def copy2(i):
        pieces = pl.ds(*GROUPS[i])
        return pltpu.make_async_remote_copy(sum_s.at[pieces], other_s.at[pieces], c2_send.at[i], c2_recv.at[i], device_id={'tp': far}, device_id_type=MESH)

    def copy3(p, side):
        view = out_ref.at[:, pl.ds(pl.multiple_of(side * half + p * cols, cols), cols)]
        return pltpu.make_async_remote_copy(view, view, c3_send.at[p], c3_recv.at[p], device_id={'tp': mate}, device_id_type=MESH)

    def chip_sum(p):
        copy1(p).wait_recv()
        sum_s[p] = (keep_s[p] + recv_s[p].astype(F32)).astype(BF16)
        for i, (a, n) in enumerate(GROUPS):
            @pl.when(p == a + n - 1)
            def _():
                copy2(i).start()

    def partial(p, w):
        deep = (n_ff + n_ctx) // 2
        s = (jnp.dot(lhs_s[:, :deep], w[:deep, :], preferred_element_type=F32)
             + jnp.dot(lhs_s[:, deep:], w[deep:, :], preferred_element_type=F32))
        send_s[p] = s[:, :cols].astype(BF16)
        keep_s[p] = s[:, cols:]
        copy1(p).start()

    partial(0, w0_ref)
    w_start(2)
    chip_sum(0)
    w_start(3)
    x_in.start()

    def compute(p, carry):
        w_wait(p)

        @pl.when(p + 3 < PIECES)
        def _():
            w_start(p + 3)
        partial(p, w_s.at[lax.rem(p, W_SLOTS)])

        @pl.when(p > 1)
        def _():
            chip_sum(p - 1)
        return carry

    lax.fori_loop(1, PIECES, compute, 0)
    chip_sum(PIECES - 1)
    x_in.wait()

    def finish(p, carry):
        copy1(p).wait_send()
        xs = x_s[:, pl.ds(col_of(p, 1), cols)].astype(F32)
        out_ref[:, pl.ds(col_of(p, 1), cols)] = (xs + (sum_s[p].astype(F32) + other_s[p].astype(F32))).astype(BF16)
        copy3(p, core).start()
        return carry

    for i, (a, n) in enumerate(GROUPS):
        copy2(i).wait_send()
        copy2(i).wait_recv()
        lax.fori_loop(a, a + n, finish, 0)

    def drain(p, carry):
        copy3(p, core).wait_send()
        copy3(p, 1 - core).wait_recv()
        return carry

    lax.fori_loop(0, PIECES, drain, 0)


def exchange(x, lhs, w0, wd, wo):
    rows, width = x.shape
    cols = width // 2 // PIECES
    n_ff = wd.shape[0]
    n_ctx = wo.shape[0]
    dma = pltpu.SemaphoreType.DMA
    return pl.pallas_call(
        exchange_kernel,
        name='exchange',
        in_specs=[HBM, VMEM, VMEM, HBM, HBM],
        out_specs=VMEM,
        out_shape=jax.ShapeDtypeStruct((rows, width), BF16),
        scratch_shapes=[
            pltpu.VMEM((rows, width), BF16),
            pltpu.VMEM((W_SLOTS, n_ff + n_ctx, 2 * cols), BF16),
            pltpu.VMEM((PIECES, rows, cols), BF16),
            pltpu.VMEM((PIECES, rows, cols), BF16),
            pltpu.VMEM((PIECES, rows, cols), F32),
            pltpu.VMEM((PIECES, rows, cols), BF16),
            pltpu.VMEM((PIECES, rows, cols), BF16),
            dma((1,)), dma((W_SLOTS,)),
            dma((PIECES,)), dma((PIECES,)), dma((len(GROUPS),)), dma((len(GROUPS),)), dma((PIECES,)), dma((PIECES,)),
        ],
        compiler_params=pltpu.CompilerParams(vmem_limit_bytes=32 * MIB, collective_id=0, has_side_effects=True),
        cost_estimate=pl.CostEstimate(flops=11 * 10 ** 9, bytes_accessed=48 * 10 ** 6, transcendentals=0),
    )(x, lhs, w0, wd, wo)


def solution(mesh):
    row_spec = P('dp', None)
    vec_spec = P(None)
    cache_spec = P('dp', 'tp', None, None)

    def device_step(x, ln_attn_gamma, ln_attn_beta, ln_mlp_gamma, ln_mlp_beta, w_qkv, w_out, w_up, w_down, k_cache, v_cache, positions):
        width = x.shape[1]
        head = w_qkv.shape[3]
        inv_freq = ROPE_BASE ** (-2.0 * np.arange(head // 2) / head)
        freq = jnp.asarray(np.concatenate([inv_freq, inv_freq])[None, :], F32)
        vecs = [v.reshape(1, width) for v in (ln_attn_gamma, ln_attn_beta, ln_mlp_gamma, ln_mlp_beta)]
        wq = jnp.transpose(w_qkv, (0, 2, 1, 3)).reshape(-1, head)
        wo = w_out.reshape(-1, width)
        in_hbm = [pltpu.with_memory_space_constraint(a, pltpu.HBM) for a in (positions, x, *vecs, freq, wq, w_up, w_down, wo, k_cache.reshape(-1, head), v_cache.reshape(-1, head))]
        x_h, wd_h, wo_h = in_hbm[1], in_hbm[-4], in_hbm[-3]
        ko, vo, lhs, w0 = front(*in_hbm)
        out = exchange(x_h, lhs, w0, wd_h, wo_h)
        return out, ko.reshape(k_cache.shape), vo.reshape(v_cache.shape)

    return jax.shard_map(device_step, mesh=mesh, in_specs=(row_spec, vec_spec, vec_spec, vec_spec, vec_spec, P(None, 'tp', None, None), P('tp', None, None, None), P(None, 'tp'), P('tp', None), cache_spec, cache_spec, P('dp')), out_specs=(row_spec, cache_spec, cache_spec), check_vma=False)
```

```python
import jax
import jax.numpy as jnp
import numpy as np
from jax import lax
from jax.experimental import pallas as pl
from jax.experimental.pallas import tpu as pltpu
from jax.sharding import PartitionSpec as P

LN_EPS = 1e-5
ROPE_BASE = 10000.0
NEG_BIG = -1e30
BF16 = jnp.bfloat16
F32 = jnp.float32
ANY = pl.BlockSpec(memory_space=pl.ANY)
HBM = pl.BlockSpec(memory_space=pltpu.HBM)
VMEM = pl.BlockSpec(memory_space=pltpu.VMEM)
SMEM = pl.BlockSpec(memory_space=pltpu.SMEM)
MIB = 1024 * 1024

QKV_CHUNK = 512
LN_ROWS = 16
ROW_BLOCK = 16
SUB_BLOCKS = 1
KV_SLOTS = 6
KV_AHEAD = 4
UP_SLOTS = 4
W_PARTS = 4


def front_kernel(pos_ref, x_hbm, ga_hbm, ba_hbm, gm_hbm, bm_hbm, freq_hbm, wq_hbm, wu_hbm, wd_hbm, wo_hbm, kc_hbm, vc_hbm,
                 ko_hbm, vo_hbm, lhs_ref, w0_ref,
                 x_s, vec_s, freq_s, cos_s, sin_s, attn_s, wqf_s, acc_s, q_s, kv_s, up_s, ctx_s, kbuf, vbuf,
                 in_sem, wq_sem, up_sem, kin_sem, vin_sem, kout_sem, vout_sem, w0_sem):
    mlp_s = x_s
    rows, width = x_s.shape
    seq = kc_hbm.shape[0] // (2 * rows)
    lines_blk = ROW_BLOCK * 2 * seq
    n_ff = lhs_ref.shape[1] - wo_hbm.shape[0]
    n_chunk = width // QKV_CHUNK
    lines = wq_hbm.shape[0] // width
    up_cols = up_s.shape[2]
    n_up = wu_hbm.shape[1] // up_cols
    n_blk = rows // ROW_BLOCK

    x_parts = [pl.ds(k * (rows // W_PARTS), rows // W_PARTS) for k in range(W_PARTS)]
    small = [pltpu.make_async_copy(x_hbm.at[part, :], x_s.at[part, :], in_sem.at[0]) for part in x_parts]
    for i, v in enumerate((ga_hbm, ba_hbm, gm_hbm, bm_hbm)):
        small.append(pltpu.make_async_copy(v, vec_s.at[pl.ds(i, 1), :], in_sem.at[1 + i]))
    freq_in = pltpu.make_async_copy(freq_hbm, freq_s, in_sem.at[5])
    freq_in.start()
    for c in small:
        c.start()

    wq_lines = QKV_CHUNK * lines
    wq_base = (KV_SLOTS - n_chunk * wq_lines // (2 * lines_blk)) * lines_blk
    wq_order = [c for pair in zip(range(n_chunk // 2), range(n_chunk // 2, n_chunk)) for c in pair]

    def wq_view(c):
        buf = kbuf if c < n_chunk // 2 else vbuf
        return buf.at[pl.ds(wq_base + (c % (n_chunk // 2)) * wq_lines, wq_lines), :]

    def wq_copy(c):
        return pltpu.make_async_copy(wq_hbm.at[pl.ds(c * wq_lines, wq_lines), :], wq_view(c), wq_sem.at[c])

    def up_start(b, slot):
        cols = pl.ds(pl.multiple_of(b * up_cols, up_cols), up_cols)
        for k in range(W_PARTS):
            part = pl.ds(k * (width // W_PARTS), width // W_PARTS)
            pltpu.make_async_copy(wu_hbm.at[part, cols], up_s.at[slot, part, :], up_sem.at[slot]).start()

    def up_wait(slot):
        pltpu.make_async_copy(wu_hbm.at[:, pl.ds(0, up_cols)], up_s.at[slot], up_sem.at[slot]).wait()

    def block(ref, i):
        return ref.at[pl.ds(pl.multiple_of(i * lines_blk, lines_blk), lines_blk), :]

    def start_in(i, slot):
        pltpu.make_async_copy(block(kc_hbm, i), block(kbuf, slot), kin_sem.at[slot]).start(priority=1)
        pltpu.make_async_copy(block(vc_hbm, i), block(vbuf, slot), vin_sem.at[slot]).start(priority=1)

    def wait_in(slot):
        pltpu.make_async_copy(block(kc_hbm, 0), block(kbuf, slot), kin_sem.at[slot]).wait()
        pltpu.make_async_copy(block(vc_hbm, 0), block(vbuf, slot), vin_sem.at[slot]).wait()

    def start_out(i, slot):
        pltpu.make_async_copy(block(kbuf, slot), block(ko_hbm, i), kout_sem.at[slot]).start()
        pltpu.make_async_copy(block(vbuf, slot), block(vo_hbm, i), vout_sem.at[slot]).start()

    def wait_out(slot):
        pltpu.make_async_copy(block(kbuf, slot), block(ko_hbm, 0), kout_sem.at[slot]).wait()
        pltpu.make_async_copy(block(vbuf, slot), block(vo_hbm, 0), vout_sem.at[slot]).wait()

    for c in wq_order[:2]:
        wq_copy(c).start()
    start_in(0, 0)

    freq_in.wait()

    def angle_body(b, carry):
        cos_s[pl.ds(b, 1), :] = pos_ref[b].astype(F32) * freq_s[0:1, :]
        return carry

    lax.fori_loop(0, rows, angle_body, 0, unroll=8)
    ang = cos_s[...]
    low = lax.broadcasted_iota(jnp.int32, ang.shape, 1) < 64
    sin_t = jnp.sin(ang)
    sin_s[...] = jnp.where(low, -sin_t, sin_t)
    cos_s[...] = jnp.cos(ang)

    for c in small:
        c.wait()
    for c in wq_order[2:4]:
        wq_copy(c).start()
    start_in(1, 1)

    def ln_body(i, carry):
        r = pl.ds(pl.multiple_of(i * LN_ROWS, LN_ROWS), LN_ROWS)
        xf = x_s[r, :].astype(F32)
        mean = jnp.mean(xf, axis=-1, keepdims=True)
        cen = xf - mean
        var = jnp.mean(cen * cen, axis=-1, keepdims=True)
        nrm = cen * lax.rsqrt(var + LN_EPS)
        attn_s[r, :] = (nrm * vec_s[0:1, :] + vec_s[1:2, :]).astype(BF16)
        mlp_s[r, :] = (nrm * vec_s[2:3, :] + vec_s[3:4, :]).astype(BF16)
        return carry

    half_ln = rows // LN_ROWS // 2
    lax.fori_loop(0, half_ln, ln_body, 0)
    for c in wq_order[4:]:
        wq_copy(c).start()
    free = wq_base // lines_blk
    for i in range(2, free):
        start_in(i, i)
    lax.fori_loop(half_ln, 2 * half_ln, ln_body, 0)

    for step, c in enumerate(wq_order):
        wq_copy(c).wait()
        if step == n_chunk - 2:
            for i in range(free, KV_AHEAD):
                start_in(i, i)
        if step >= n_chunk - UP_SLOTS:
            up_start(step - n_chunk + UP_SLOTS, step - n_chunk + UP_SLOTS)
        wqf_s[...] = wq_view(c)[...].astype(F32)
        lhs = attn_s[:, c * QKV_CHUNK:(c + 1) * QKV_CHUNK]
        for pair in range(lines // 2):
            w = jnp.concatenate([wqf_s[pl.ds(2 * pair + e, QKV_CHUNK, stride=lines), :].astype(BF16) for e in range(2)], axis=1)
            part = jnp.dot(lhs, w, preferred_element_type=F32)
            if step == 0:
                acc_s[:, pair * 256:(pair + 1) * 256] = part
            else:
                acc_s[:, pair * 256:(pair + 1) * 256] += part

    n_slot = lines // 2
    n_q = n_slot - 2
    for j in range(n_slot):
        for g in range(2):
            col = (2 * j + g) * 128
            u = acc_s[:, col:col + 128].astype(BF16).astype(F32)
            if j < n_q + 1:
                u = (u * cos_s[...] + pltpu.roll(u, 64, 1) * sin_s[...]).astype(BF16).astype(F32)
            if j < n_q:
                q_s[pl.ds((g * n_q + j) * rows, rows), :] = u
            else:
                kv_s[pl.ds(((j - n_q) * 2 + g) * rows, rows), :] = u

    slot_ids = lax.broadcasted_iota(jnp.int32, (8, 256), 1)
    tile_ids = lax.broadcasted_iota(jnp.int32, (16, 128), 0)
    first = lax.broadcasted_iota(jnp.int32, (8, 128), 0) < 4
    scale = 128 ** -0.5

    def pair_of(buf, slot, r):
        at = [pl.ds(pl.multiple_of(slot * lines_blk + (2 * r + g) * seq, seq), seq) for g in range(2)]
        return jnp.concatenate([buf[a, :] for a in at], axis=1)

    def attend_block(i, slot):
        pos = [pos_ref[i * ROW_BLOCK + r] for r in range(ROW_BLOCK)]
        for r in range(ROW_BLOCK):
            base = pl.multiple_of((pos[r] // 16) * 16, 16)
            hit = tile_ids == pos[r] - base
            b = i * ROW_BLOCK + r
            for g in range(2):
                tile = pl.ds(pl.multiple_of(slot * lines_blk + (2 * r + g) * seq + base, 16), 16)
                for buf, which in ((kbuf, 0), (vbuf, 1)):
                    new = kv_s[pl.ds((which * 2 + g) * rows + b, 1), :]
                    buf[tile, :] = jnp.where(hit, new, buf[tile, :].astype(F32)).astype(BF16)
        scores = []
        for r in range(ROW_BLOCK):
            b = i * ROW_BLOCK + r
            q = q_s[pl.ds(b, 8, stride=rows), :]
            zero = jnp.zeros_like(q)
            q2 = jnp.concatenate([jnp.where(first, q, zero), jnp.where(first, zero, q)], axis=1).astype(BF16)
            k2 = pair_of(kbuf, slot, r)
            s = lax.dot_general(q2, k2, (((1,), (1,)), ((), ())), preferred_element_type=F32) * scale
            scores.append(jnp.where(slot_ids <= pos[r], s, NEG_BIG))
        s = jnp.concatenate(scores, axis=0)
        e = jnp.exp(s - jnp.max(s, axis=-1, keepdims=True))
        p = (e / jnp.sum(e, axis=-1, keepdims=True)).astype(BF16)
        for r in range(ROW_BLOCK):
            v2 = pair_of(vbuf, slot, r)
            c = jnp.dot(p[8 * r:8 * r + 8], v2, preferred_element_type=F32)
            ctx_s[pl.ds(i * ROW_BLOCK + r, 8, stride=rows), :] = jnp.where(first, c[:, :128], c[:, 128:])

    core = lax.rem(lax.axis_index('tp'), 2)
    cols = w0_ref.shape[1] // 2
    w0_in = []
    for part in range(2):
        src = pl.ds(pl.multiple_of((core if part else 1 - core) * (wd_hbm.shape[1] // 2), cols), cols)
        dst = pl.ds(part * cols, cols)
        w0_in.append(pltpu.make_async_copy(wd_hbm.at[:, src], w0_ref.at[pl.ds(0, n_ff), dst], w0_sem.at[0]))
        w0_in.append(pltpu.make_async_copy(wo_hbm.at[:, src], w0_ref.at[pl.ds(n_ff, wo_hbm.shape[0]), dst], w0_sem.at[0]))

    def body(i, carry):
        for s in range(SUB_BLOCKS):
            nxt = i * SUB_BLOCKS + s + KV_AHEAD

            @pl.when(nxt < n_blk)
            def _():
                nslot = lax.rem(nxt, KV_SLOTS)

                @pl.when(nxt >= KV_SLOTS)
                def _():
                    wait_out(nslot)
                start_in(nxt, nslot)

        @pl.when((i >= 1) & (i - 1 + UP_SLOTS < n_up))
        def _():
            up_start(i - 1 + UP_SLOTS, lax.rem(i - 1, UP_SLOTS))

        uslot = lax.rem(i, UP_SLOTS)
        up_wait(uslot)
        for s in range(SUB_BLOCKS):
            wait_in(lax.rem(i * SUB_BLOCKS + s, KV_SLOTS))
        deep = width // 2
        pre = (jnp.dot(mlp_s[:, :deep], up_s[uslot, :deep, :], preferred_element_type=F32)
               + jnp.dot(mlp_s[:, deep:], up_s[uslot, deep:, :], preferred_element_type=F32))
        act = 0.5 * pre * (1.0 + lax.erf(pre * (0.5 ** 0.5)))
        lhs_ref[:, pl.ds(pl.multiple_of(i * up_cols, up_cols), up_cols)] = act.astype(BF16)
        for s in range(SUB_BLOCKS):
            blk = i * SUB_BLOCKS + s
            attend_block(blk, lax.rem(blk, KV_SLOTS))
        for s in range(SUB_BLOCKS):
            blk = i * SUB_BLOCKS + s
            start_out(blk, lax.rem(blk, KV_SLOTS))

        @pl.when(i == n_up - 4)
        def _():
            for c in w0_in:
                c.start(priority=1)
        return carry

    lax.fori_loop(0, n_up, body, 0)
    for h in range(ctx_s.shape[0] // rows):
        lhs_ref[:, n_ff + h * 128:n_ff + (h + 1) * 128] = ctx_s[h * rows:(h + 1) * rows, :].astype(BF16)
    for c in w0_in:
        c.wait()
    for i in range(n_blk - KV_SLOTS, n_blk):
        wait_out(i % KV_SLOTS)


def front(pos, x, ga, ba, gm, bm, freq, wq, wu, wd, wo, kc, vc):
    rows, width = x.shape
    hid = wu.shape[1]
    lines = wq.shape[0] // width
    n_head = (lines // 2 - 2) * 2
    up_cols = hid // (rows // (ROW_BLOCK * SUB_BLOCKS))
    lines_blk = kc.shape[0] // rows * ROW_BLOCK
    return pl.pallas_call(
        front_kernel,
        name='front',
        in_specs=[SMEM] + [HBM] * 12,
        out_specs=[HBM, HBM, VMEM, VMEM],
        out_shape=[
            jax.ShapeDtypeStruct(kc.shape, BF16),
            jax.ShapeDtypeStruct(vc.shape, BF16),
            jax.ShapeDtypeStruct((rows, hid + wo.shape[0]), BF16),
            jax.ShapeDtypeStruct((hid + wo.shape[0], 2 * width // PIECES), BF16),
        ],
        scratch_shapes=[
            pltpu.VMEM((rows, width), BF16),
            pltpu.VMEM((4, width), F32),
            pltpu.VMEM((1, 128), F32),
            pltpu.VMEM((rows, 128), F32),
            pltpu.VMEM((rows, 128), F32),
            pltpu.VMEM((rows, width), BF16),
            pltpu.VMEM((QKV_CHUNK * lines, 128), F32),
            pltpu.VMEM((rows, lines * 128), F32),
            pltpu.VMEM((n_head * rows, 128), F32),
            pltpu.VMEM((4 * rows, 128), F32),
            pltpu.VMEM((UP_SLOTS, width, up_cols), BF16),
            pltpu.VMEM((n_head * rows, 128), F32),
            pltpu.VMEM((KV_SLOTS * lines_blk, 128), BF16),
            pltpu.VMEM((KV_SLOTS * lines_blk, 128), BF16),
            pltpu.SemaphoreType.DMA((6,)),
            pltpu.SemaphoreType.DMA((width // QKV_CHUNK,)),
            pltpu.SemaphoreType.DMA((UP_SLOTS,)),
            pltpu.SemaphoreType.DMA((KV_SLOTS,)),
            pltpu.SemaphoreType.DMA((KV_SLOTS,)),
            pltpu.SemaphoreType.DMA((KV_SLOTS,)),
            pltpu.SemaphoreType.DMA((KV_SLOTS,)),
            pltpu.SemaphoreType.DMA((1,)),
        ],
        compiler_params=pltpu.CompilerParams(vmem_limit_bytes=44 * MIB),
        cost_estimate=pl.CostEstimate(flops=22 * 10 ** 9, bytes_accessed=180 * 10 ** 6, transcendentals=0),
    )(pos, x, ga, ba, gm, bm, freq, wq, wu, wd, wo, kc, vc)


PIECES = 16
GROUPS = ((0, 1), (1, 1), (2, 2), (4, 2), (6, 2), (8, 2), (10, 2), (12, 2), (14, 1), (15, 1))
W_SLOTS = 3
MESH = pl.DeviceIdType.MESH


def exchange_kernel(x_hbm, lhs_s, w0_ref, wd_hbm, wo_hbm, out_ref,
                    x_s, w_s, send_s, recv_s, keep_s, sum_s, other_s,
                    in_sem, w_sem, c1_send, c1_recv, c2_send, c2_recv, c3_send, c3_recv):
    rows, width = x_s.shape
    half = width // 2
    cols = half // PIECES
    n_ff, n_ctx = wd_hbm.shape[0], wo_hbm.shape[0]
    me = lax.axis_index('tp')
    core = lax.rem(me, 2)
    mate = me + 1 - 2 * core
    far = lax.rem(me + 2, 4)

    def col_of(p, part):
        side = core if part else 1 - core
        return pl.multiple_of(side * half + p * cols, cols)

    def w_start(q):
        slot = lax.rem(q, W_SLOTS)
        for part in range(2):
            src, dst = pl.ds(col_of(2 * q, part), 2 * cols), pl.ds(2 * part * cols, 2 * cols)
            pltpu.make_async_copy(wo_hbm.at[:, src], w_s.at[slot, pl.ds(n_ff, n_ctx), dst], w_sem.at[slot]).start()
            for k in range(W_PARTS):
                deep = pl.ds(k * (n_ff // W_PARTS), n_ff // W_PARTS)
                pltpu.make_async_copy(wd_hbm.at[deep, src], w_s.at[slot, deep, dst], w_sem.at[slot]).start()

    def w_wait(q):
        slot = lax.rem(q, W_SLOTS)
        for part in range(2):
            src, dst = pl.ds(0, 2 * cols), pl.ds(2 * part * cols, 2 * cols)
            pltpu.make_async_copy(wo_hbm.at[:, src], w_s.at[slot, pl.ds(n_ff, n_ctx), dst], w_sem.at[slot]).wait()
            pltpu.make_async_copy(wd_hbm.at[:, src], w_s.at[slot, pl.ds(0, n_ff), dst], w_sem.at[slot]).wait()

    w_start(1)
    x_in = pltpu.make_async_copy(x_hbm, x_s, in_sem.at[0])

    barrier = pltpu.get_barrier_semaphore()
    for peer in (mate, far):
        pl.semaphore_signal(barrier, inc=1, device_id={'tp': peer}, device_id_type=MESH)
    pl.semaphore_wait(barrier, 2)

    def copy1(p):
        return pltpu.make_async_remote_copy(send_s.at[p], recv_s.at[p], c1_send.at[p], c1_recv.at[p], device_id={'tp': mate}, device_id_type=MESH)

    def copy2(i):
        pieces = pl.ds(*GROUPS[i])
        return pltpu.make_async_remote_copy(sum_s.at[pieces], other_s.at[pieces], c2_send.at[i], c2_recv.at[i], device_id={'tp': far}, device_id_type=MESH)

    def copy3(p, side):
        view = out_ref.at[:, pl.ds(pl.multiple_of(side * half + p * cols, cols), cols)]
        return pltpu.make_async_remote_copy(view, view, c3_send.at[p], c3_recv.at[p], device_id={'tp': mate}, device_id_type=MESH)

    def chip_sum(p):
        copy1(p).wait_recv()
        sum_s[p] = (keep_s[p] + recv_s[p].astype(F32)).astype(BF16)
        for i, (a, n) in enumerate(GROUPS):
            @pl.when(p == a + n - 1)
            def _():
                copy2(i).start()

    def partial(p, w, e):
        deep = (n_ff + n_ctx) // 2
        s = None
        for k in range(2):
            rng = slice(k * deep, (k + 1) * deep)
            rhs = jnp.concatenate([w[rng, (2 * part + e) * cols:(2 * part + e + 1) * cols] for part in range(2)], axis=1)
            d = jnp.dot(lhs_s[:, rng], rhs, preferred_element_type=F32)
            s = d if s is None else s + d
        send_s[p] = s[:, :cols].astype(BF16)
        keep_s[p] = s[:, cols:]
        copy1(p).start()

    partial(0, w0_ref, 0)
    w_start(2)
    partial(1, w0_ref, 1)
    chip_sum(0)
    x_in.start()

    def compute(q, carry):
        w_wait(q)

        @pl.when(q + 2 < PIECES // 2)
        def _():
            w_start(q + 2)
        for e in range(2):
            partial(2 * q + e, w_s.at[lax.rem(q, W_SLOTS)], e)
            chip_sum(2 * q + e - 1)
        return carry

    lax.fori_loop(1, PIECES // 2, compute, 0)
    chip_sum(PIECES - 1)
    x_in.wait()

    def finish(p, carry):
        copy1(p).wait_send()
        xs = x_s[:, pl.ds(col_of(p, 1), cols)].astype(F32)
        out_ref[:, pl.ds(col_of(p, 1), cols)] = (xs + (sum_s[p].astype(F32) + other_s[p].astype(F32))).astype(BF16)
        copy3(p, core).start()
        return carry

    for i, (a, n) in enumerate(GROUPS):
        copy2(i).wait_send()
        copy2(i).wait_recv()
        lax.fori_loop(a, a + n, finish, 0)

    def drain(p, carry):
        copy3(p, core).wait_send()
        copy3(p, 1 - core).wait_recv()
        return carry

    lax.fori_loop(0, PIECES, drain, 0)


def exchange(x, lhs, w0, wd, wo):
    rows, width = x.shape
    cols = width // 2 // PIECES
    n_ff = wd.shape[0]
    n_ctx = wo.shape[0]
    dma = pltpu.SemaphoreType.DMA
    return pl.pallas_call(
        exchange_kernel,
        name='exchange',
        in_specs=[HBM, VMEM, VMEM, HBM, HBM],
        out_specs=VMEM,
        out_shape=jax.ShapeDtypeStruct((rows, width), BF16),
        scratch_shapes=[
            pltpu.VMEM((rows, width), BF16),
            pltpu.VMEM((W_SLOTS, n_ff + n_ctx, 4 * cols), BF16),
            pltpu.VMEM((PIECES, rows, cols), BF16),
            pltpu.VMEM((PIECES, rows, cols), BF16),
            pltpu.VMEM((PIECES, rows, cols), F32),
            pltpu.VMEM((PIECES, rows, cols), BF16),
            pltpu.VMEM((PIECES, rows, cols), BF16),
            dma((1,)), dma((W_SLOTS,)),
            dma((PIECES,)), dma((PIECES,)), dma((len(GROUPS),)), dma((len(GROUPS),)), dma((PIECES,)), dma((PIECES,)),
        ],
        compiler_params=pltpu.CompilerParams(vmem_limit_bytes=32 * MIB, collective_id=0, has_side_effects=True),
        cost_estimate=pl.CostEstimate(flops=11 * 10 ** 9, bytes_accessed=48 * 10 ** 6, transcendentals=0),
    )(x, lhs, w0, wd, wo)


def solution(mesh):
    row_spec = P('dp', None)
    vec_spec = P(None)
    cache_spec = P('dp', 'tp', None, None)

    def device_step(x, ln_attn_gamma, ln_attn_beta, ln_mlp_gamma, ln_mlp_beta, w_qkv, w_out, w_up, w_down, k_cache, v_cache, positions):
        width = x.shape[1]
        head = w_qkv.shape[3]
        inv_freq = ROPE_BASE ** (-2.0 * np.arange(head // 2) / head)
        freq = jnp.asarray(np.concatenate([inv_freq, inv_freq])[None, :], F32)
        vecs = [v.reshape(1, width) for v in (ln_attn_gamma, ln_attn_beta, ln_mlp_gamma, ln_mlp_beta)]
        wq = jnp.transpose(w_qkv, (0, 2, 1, 3)).reshape(-1, head)
        wo = w_out.reshape(-1, width)
        in_hbm = [pltpu.with_memory_space_constraint(a, pltpu.HBM) for a in (positions, x, *vecs, freq, wq, w_up, w_down, wo, k_cache.reshape(-1, head), v_cache.reshape(-1, head))]
        x_h, wd_h, wo_h = in_hbm[1], in_hbm[-4], in_hbm[-3]
        ko, vo, lhs, w0 = front(*in_hbm)
        out = exchange(x_h, lhs, w0, wd_h, wo_h)
        return out, ko.reshape(k_cache.shape), vo.reshape(v_cache.shape)

    return jax.shard_map(device_step, mesh=mesh, in_specs=(row_spec, vec_spec, vec_spec, vec_spec, vec_spec, P(None, 'tp', None, None), P('tp', None, None, None), P(None, 'tp'), P('tp', None), cache_spec, cache_spec, P('dp')), out_specs=(row_spec, cache_spec, cache_spec), check_vma=False)
```

```python
import jax
import jax.numpy as jnp
import numpy as np
from jax import lax
from jax.experimental import pallas as pl
from jax.experimental.pallas import tpu as pltpu
from jax.sharding import PartitionSpec as P

LN_EPS = 1e-5
ROPE_BASE = 10000.0
NEG_BIG = -1e30
BF16 = jnp.bfloat16
F32 = jnp.float32
ANY = pl.BlockSpec(memory_space=pl.ANY)
HBM = pl.BlockSpec(memory_space=pltpu.HBM)
VMEM = pl.BlockSpec(memory_space=pltpu.VMEM)
SMEM = pl.BlockSpec(memory_space=pltpu.SMEM)
MIB = 1024 * 1024

QKV_CHUNK = 512
LN_ROWS = 16
ROW_BLOCK = 16
SUB_BLOCKS = 1
KV_SLOTS = 6
KV_AHEAD = 4
UP_SLOTS = 4
W_PARTS = 4


def front_kernel(pos_ref, x_hbm, ga_hbm, ba_hbm, gm_hbm, bm_hbm, freq_hbm, wq_hbm, wu_hbm, wd_hbm, wo_hbm, kc_hbm, vc_hbm,
                 ko_hbm, vo_hbm, lhs_ref, w0_ref,
                 x_s, vec_s, freq_s, cos_s, sin_s, attn_s, wqf_s, acc_s, q_s, kv_s, up_s, ctx_s, kbuf, vbuf,
                 in_sem, wq_sem, up_sem, kin_sem, vin_sem, kout_sem, vout_sem, w0_sem):
    mlp_s = x_s
    rows, width = x_s.shape
    seq = kc_hbm.shape[0] // (2 * rows)
    lines_blk = ROW_BLOCK * 2 * seq
    n_ff = lhs_ref.shape[1] - wo_hbm.shape[0]
    n_chunk = width // QKV_CHUNK
    lines = wq_hbm.shape[0] // width
    up_cols = up_s.shape[2]
    n_up = wu_hbm.shape[1] // up_cols
    n_blk = rows // ROW_BLOCK

    x_parts = [pl.ds(k * (rows // W_PARTS), rows // W_PARTS) for k in range(W_PARTS)]
    small = [pltpu.make_async_copy(x_hbm.at[part, :], x_s.at[part, :], in_sem.at[0]) for part in x_parts]
    for i, v in enumerate((ga_hbm, ba_hbm, gm_hbm, bm_hbm)):
        small.append(pltpu.make_async_copy(v, vec_s.at[pl.ds(i, 1), :], in_sem.at[1 + i]))
    freq_in = pltpu.make_async_copy(freq_hbm, freq_s, in_sem.at[5])
    freq_in.start()
    for c in small:
        c.start()

    wq_lines = QKV_CHUNK * lines
    wq_base = (KV_SLOTS - n_chunk * wq_lines // (2 * lines_blk)) * lines_blk
    wq_order = [c for pair in zip(range(n_chunk // 2), range(n_chunk // 2, n_chunk)) for c in pair]

    def wq_view(c):
        buf = kbuf if c < n_chunk // 2 else vbuf
        return buf.at[pl.ds(wq_base + (c % (n_chunk // 2)) * wq_lines, wq_lines), :]

    def wq_copy(c):
        return pltpu.make_async_copy(wq_hbm.at[pl.ds(c * wq_lines, wq_lines), :], wq_view(c), wq_sem.at[c])

    def up_start(b, slot):
        cols = pl.ds(pl.multiple_of(b * up_cols, up_cols), up_cols)
        for k in range(W_PARTS):
            part = pl.ds(k * (width // W_PARTS), width // W_PARTS)
            pltpu.make_async_copy(wu_hbm.at[part, cols], up_s.at[slot, part, :], up_sem.at[slot]).start()

    def up_wait(slot):
        pltpu.make_async_copy(wu_hbm.at[:, pl.ds(0, up_cols)], up_s.at[slot], up_sem.at[slot]).wait()

    def block(ref, i):
        return ref.at[pl.ds(pl.multiple_of(i * lines_blk, lines_blk), lines_blk), :]

    def start_in(i, slot):
        pltpu.make_async_copy(block(kc_hbm, i), block(kbuf, slot), kin_sem.at[slot]).start(priority=1)
        pltpu.make_async_copy(block(vc_hbm, i), block(vbuf, slot), vin_sem.at[slot]).start(priority=1)

    def wait_in(slot):
        pltpu.make_async_copy(block(kc_hbm, 0), block(kbuf, slot), kin_sem.at[slot]).wait()
        pltpu.make_async_copy(block(vc_hbm, 0), block(vbuf, slot), vin_sem.at[slot]).wait()

    def start_out(i, slot):
        pltpu.make_async_copy(block(kbuf, slot), block(ko_hbm, i), kout_sem.at[slot]).start()
        pltpu.make_async_copy(block(vbuf, slot), block(vo_hbm, i), vout_sem.at[slot]).start()

    def wait_out(slot):
        pltpu.make_async_copy(block(kbuf, slot), block(ko_hbm, 0), kout_sem.at[slot]).wait()
        pltpu.make_async_copy(block(vbuf, slot), block(vo_hbm, 0), vout_sem.at[slot]).wait()

    for c in wq_order[:2]:
        wq_copy(c).start()
    start_in(0, 0)

    freq_in.wait()

    def angle_body(b, carry):
        cos_s[pl.ds(b, 1), :] = pos_ref[b].astype(F32) * freq_s[0:1, :]
        return carry

    lax.fori_loop(0, rows, angle_body, 0, unroll=8)
    ang = cos_s[...]
    low = lax.broadcasted_iota(jnp.int32, ang.shape, 1) < 64
    sin_t = jnp.sin(ang)
    sin_s[...] = jnp.where(low, -sin_t, sin_t)
    cos_s[...] = jnp.cos(ang)

    for c in small:
        c.wait()
    for c in wq_order[2:4]:
        wq_copy(c).start()
    start_in(1, 1)

    def ln_body(i, carry):
        r = pl.ds(pl.multiple_of(i * LN_ROWS, LN_ROWS), LN_ROWS)
        xf = x_s[r, :].astype(F32)
        mean = jnp.mean(xf, axis=-1, keepdims=True)
        cen = xf - mean
        var = jnp.mean(cen * cen, axis=-1, keepdims=True)
        nrm = cen * lax.rsqrt(var + LN_EPS)
        attn_s[r, :] = (nrm * vec_s[0:1, :] + vec_s[1:2, :]).astype(BF16)
        mlp_s[r, :] = (nrm * vec_s[2:3, :] + vec_s[3:4, :]).astype(BF16)
        return carry

    half_ln = rows // LN_ROWS // 2
    lax.fori_loop(0, half_ln, ln_body, 0)
    for c in wq_order[4:]:
        wq_copy(c).start()
    free = wq_base // lines_blk
    for i in range(2, free):
        start_in(i, i)
    lax.fori_loop(half_ln, 2 * half_ln, ln_body, 0)

    for step, c in enumerate(wq_order):
        wq_copy(c).wait()
        if step == n_chunk - 2:
            for i in range(free, KV_AHEAD):
                start_in(i, i)
        if step >= n_chunk - UP_SLOTS:
            up_start(step - n_chunk + UP_SLOTS, step - n_chunk + UP_SLOTS)
        wqf_s[...] = wq_view(c)[...].astype(F32)
        lhs = attn_s[:, c * QKV_CHUNK:(c + 1) * QKV_CHUNK]
        for pair in range(lines // 2):
            w = jnp.concatenate([wqf_s[pl.ds(2 * pair + e, QKV_CHUNK, stride=lines), :].astype(BF16) for e in range(2)], axis=1)
            part = jnp.dot(lhs, w, preferred_element_type=F32)
            if step == 0:
                acc_s[:, pair * 256:(pair + 1) * 256] = part
            else:
                acc_s[:, pair * 256:(pair + 1) * 256] += part

    n_slot = lines // 2
    n_q = n_slot - 2
    for j in range(n_slot):
        for g in range(2):
            col = (2 * j + g) * 128
            u = acc_s[:, col:col + 128].astype(BF16).astype(F32)
            if j < n_q + 1:
                u = (u * cos_s[...] + pltpu.roll(u, 64, 1) * sin_s[...]).astype(BF16).astype(F32)
            if j < n_q:
                q_s[pl.ds((g * n_q + j) * rows, rows), :] = u
            else:
                kv_s[pl.ds(((j - n_q) * 2 + g) * rows, rows), :] = u

    slot_ids = lax.broadcasted_iota(jnp.int32, (8, 256), 1)
    tile_ids = lax.broadcasted_iota(jnp.int32, (16, 128), 0)
    first = lax.broadcasted_iota(jnp.int32, (8, 128), 0) < 4
    scale = 128 ** -0.5

    def pair_of(buf, slot, r):
        at = [pl.ds(pl.multiple_of(slot * lines_blk + (2 * r + g) * seq, seq), seq) for g in range(2)]
        return jnp.concatenate([buf[a, :] for a in at], axis=1)

    def attend_block(i, slot):
        pos = [pos_ref[i * ROW_BLOCK + r] for r in range(ROW_BLOCK)]
        for r in range(ROW_BLOCK):
            base = pl.multiple_of((pos[r] // 16) * 16, 16)
            hit = tile_ids == pos[r] - base
            b = i * ROW_BLOCK + r
            for g in range(2):
                tile = pl.ds(pl.multiple_of(slot * lines_blk + (2 * r + g) * seq + base, 16), 16)
                for buf, which in ((kbuf, 0), (vbuf, 1)):
                    new = kv_s[pl.ds((which * 2 + g) * rows + b, 1), :]
                    buf[tile, :] = jnp.where(hit, new, buf[tile, :].astype(F32)).astype(BF16)
        scores = []
        for r in range(ROW_BLOCK):
            b = i * ROW_BLOCK + r
            q = q_s[pl.ds(b, 8, stride=rows), :]
            zero = jnp.zeros_like(q)
            q2 = jnp.concatenate([jnp.where(first, q, zero), jnp.where(first, zero, q)], axis=1).astype(BF16)
            k2 = pair_of(kbuf, slot, r)
            s = lax.dot_general(q2, k2, (((1,), (1,)), ((), ())), preferred_element_type=F32) * scale
            scores.append(jnp.where(slot_ids <= pos[r], s, NEG_BIG))
        s = jnp.concatenate(scores, axis=0)
        e = jnp.exp(s - jnp.max(s, axis=-1, keepdims=True))
        p = (e / jnp.sum(e, axis=-1, keepdims=True)).astype(BF16)
        for r in range(ROW_BLOCK):
            v2 = pair_of(vbuf, slot, r)
            c = jnp.dot(p[8 * r:8 * r + 8], v2, preferred_element_type=F32)
            ctx_s[pl.ds(i * ROW_BLOCK + r, 8, stride=rows), :] = jnp.where(first, c[:, :128], c[:, 128:])

    core = lax.rem(lax.axis_index('tp'), 2)
    cols = w0_ref.shape[1] // 2
    w0_in = []
    for part in range(2):
        src = pl.ds(pl.multiple_of((core if part else 1 - core) * (wd_hbm.shape[1] // 2), cols), cols)
        dst = pl.ds(part * cols, cols)
        w0_in.append(pltpu.make_async_copy(wd_hbm.at[:, src], w0_ref.at[pl.ds(0, n_ff), dst], w0_sem.at[0]))
        w0_in.append(pltpu.make_async_copy(wo_hbm.at[:, src], w0_ref.at[pl.ds(n_ff, wo_hbm.shape[0]), dst], w0_sem.at[0]))

    def body(i, carry):
        for s in range(SUB_BLOCKS):
            nxt = i * SUB_BLOCKS + s + KV_AHEAD

            @pl.when(nxt < n_blk)
            def _():
                nslot = lax.rem(nxt, KV_SLOTS)

                @pl.when(nxt >= KV_SLOTS)
                def _():
                    wait_out(nslot)
                start_in(nxt, nslot)

        @pl.when((i >= 1) & (i - 1 + UP_SLOTS < n_up))
        def _():
            up_start(i - 1 + UP_SLOTS, lax.rem(i - 1, UP_SLOTS))

        uslot = lax.rem(i, UP_SLOTS)
        up_wait(uslot)
        for s in range(SUB_BLOCKS):
            wait_in(lax.rem(i * SUB_BLOCKS + s, KV_SLOTS))
        deep = width // 2
        pre = (jnp.dot(mlp_s[:, :deep], up_s[uslot, :deep, :], preferred_element_type=F32)
               + jnp.dot(mlp_s[:, deep:], up_s[uslot, deep:, :], preferred_element_type=F32))
        act = 0.5 * pre * (1.0 + lax.erf(pre * (0.5 ** 0.5)))
        lhs_ref[:, pl.ds(pl.multiple_of(i * up_cols, up_cols), up_cols)] = act.astype(BF16)
        for s in range(SUB_BLOCKS):
            blk = i * SUB_BLOCKS + s
            attend_block(blk, lax.rem(blk, KV_SLOTS))
        for s in range(SUB_BLOCKS):
            blk = i * SUB_BLOCKS + s
            start_out(blk, lax.rem(blk, KV_SLOTS))

        @pl.when(i == n_up - 4)
        def _():
            for c in w0_in:
                c.start(priority=1)
        return carry

    lax.fori_loop(0, n_up, body, 0)
    for h in range(ctx_s.shape[0] // rows):
        lhs_ref[:, n_ff + h * 128:n_ff + (h + 1) * 128] = ctx_s[h * rows:(h + 1) * rows, :].astype(BF16)
    for c in w0_in:
        c.wait()
    for i in range(n_blk - KV_SLOTS, n_blk):
        wait_out(i % KV_SLOTS)


def front(pos, x, ga, ba, gm, bm, freq, wq, wu, wd, wo, kc, vc):
    rows, width = x.shape
    hid = wu.shape[1]
    lines = wq.shape[0] // width
    n_head = (lines // 2 - 2) * 2
    up_cols = hid // (rows // (ROW_BLOCK * SUB_BLOCKS))
    lines_blk = kc.shape[0] // rows * ROW_BLOCK
    return pl.pallas_call(
        front_kernel,
        name='front',
        in_specs=[SMEM] + [HBM] * 12,
        out_specs=[HBM, HBM, VMEM, VMEM],
        out_shape=[
            jax.ShapeDtypeStruct(kc.shape, BF16),
            jax.ShapeDtypeStruct(vc.shape, BF16),
            jax.ShapeDtypeStruct((rows, hid + wo.shape[0]), BF16),
            jax.ShapeDtypeStruct((hid + wo.shape[0], width // PIECES), BF16),
        ],
        scratch_shapes=[
            pltpu.VMEM((rows, width), BF16),
            pltpu.VMEM((4, width), F32),
            pltpu.VMEM((1, 128), F32),
            pltpu.VMEM((rows, 128), F32),
            pltpu.VMEM((rows, 128), F32),
            pltpu.VMEM((rows, width), BF16),
            pltpu.VMEM((QKV_CHUNK * lines, 128), F32),
            pltpu.VMEM((rows, lines * 128), F32),
            pltpu.VMEM((n_head * rows, 128), F32),
            pltpu.VMEM((4 * rows, 128), F32),
            pltpu.VMEM((UP_SLOTS, width, up_cols), BF16),
            pltpu.VMEM((n_head * rows, 128), F32),
            pltpu.VMEM((KV_SLOTS * lines_blk, 128), BF16),
            pltpu.VMEM((KV_SLOTS * lines_blk, 128), BF16),
            pltpu.SemaphoreType.DMA((6,)),
            pltpu.SemaphoreType.DMA((width // QKV_CHUNK,)),
            pltpu.SemaphoreType.DMA((UP_SLOTS,)),
            pltpu.SemaphoreType.DMA((KV_SLOTS,)),
            pltpu.SemaphoreType.DMA((KV_SLOTS,)),
            pltpu.SemaphoreType.DMA((KV_SLOTS,)),
            pltpu.SemaphoreType.DMA((KV_SLOTS,)),
            pltpu.SemaphoreType.DMA((1,)),
        ],
        compiler_params=pltpu.CompilerParams(vmem_limit_bytes=44 * MIB),
        cost_estimate=pl.CostEstimate(flops=22 * 10 ** 9, bytes_accessed=180 * 10 ** 6, transcendentals=0),
    )(pos, x, ga, ba, gm, bm, freq, wq, wu, wd, wo, kc, vc)


PIECES = 16
W_SLOTS = 3
MESH = pl.DeviceIdType.MESH


def exchange_kernel(x_hbm, lhs_s, w0_ref, wd_hbm, wo_hbm, out_ref,
                    x_s, w_s, send_s, recv_s, keep_s, sum_s, other_s,
                    in_sem, w_sem, c1_send, c1_recv, c2_send, c2_recv, c3_send, c3_recv):
    rows, width = x_s.shape
    half = width // 2
    cols = half // PIECES
    n_ff, n_ctx = wd_hbm.shape[0], wo_hbm.shape[0]
    me = lax.axis_index('tp')
    core = lax.rem(me, 2)
    mate = me + 1 - 2 * core
    far = lax.rem(me + 2, 4)

    def col_of(p, part):
        side = core if part else 1 - core
        return pl.multiple_of(side * half + p * cols, cols)

    def w_start(p):
        slot = lax.rem(p, W_SLOTS)
        for part in range(2):
            src, dst = pl.ds(col_of(p, part), cols), pl.ds(part * cols, cols)
            pltpu.make_async_copy(wo_hbm.at[:, src], w_s.at[slot, pl.ds(n_ff, n_ctx), dst], w_sem.at[slot]).start()
            for k in range(2):
                deep = pl.ds(k * (n_ff // 2), n_ff // 2)
                pltpu.make_async_copy(wd_hbm.at[deep, src], w_s.at[slot, deep, dst], w_sem.at[slot]).start()

    def w_wait(p):
        slot = lax.rem(p, W_SLOTS)
        for part in range(2):
            dst = pl.ds(part * cols, cols)
            pltpu.make_async_copy(wo_hbm.at[:, pl.ds(0, cols)], w_s.at[slot, pl.ds(n_ff, n_ctx), dst], w_sem.at[slot]).wait()
            pltpu.make_async_copy(wd_hbm.at[:, pl.ds(0, cols)], w_s.at[slot, pl.ds(0, n_ff), dst], w_sem.at[slot]).wait()

    w_start(1)
    x_in = pltpu.make_async_copy(x_hbm, x_s, in_sem.at[0])

    barrier = pltpu.get_barrier_semaphore()
    for peer in (mate, far):
        pl.semaphore_signal(barrier, inc=1, device_id={'tp': peer}, device_id_type=MESH)
    pl.semaphore_wait(barrier, 2)

    def copy1(p):
        return pltpu.make_async_remote_copy(send_s.at[p], recv_s.at[p], c1_send.at[p], c1_recv.at[p], device_id={'tp': mate}, device_id_type=MESH)

    def copy2(p):
        return pltpu.make_async_remote_copy(sum_s.at[p], other_s.at[p], c2_send.at[p], c2_recv.at[p], device_id={'tp': far}, device_id_type=MESH)

    def copy3(p, side):
        view = out_ref.at[:, pl.ds(pl.multiple_of(side * half + p * cols, cols), cols)]
        return pltpu.make_async_remote_copy(view, view, c3_send.at[p], c3_recv.at[p], device_id={'tp': mate}, device_id_type=MESH)

    def chip_sum(p):
        copy1(p).wait_recv()
        sum_s[p] = (keep_s[p] + recv_s[p].astype(F32)).astype(BF16)
        copy2(p).start()

    def partial(p, w):
        deep = (n_ff + n_ctx) // 2
        s = (jnp.dot(lhs_s[:, :deep], w[:deep, :], preferred_element_type=F32)
             + jnp.dot(lhs_s[:, deep:], w[deep:, :], preferred_element_type=F32))
        send_s[p] = s[:, :cols].astype(BF16)
        keep_s[p] = s[:, cols:]
        copy1(p).start()

    partial(0, w0_ref)
    w_start(2)
    chip_sum(0)
    x_in.start()

    def compute(p, carry):
        w_wait(p)

        @pl.when(p + 2 < PIECES)
        def _():
            w_start(p + 2)
        partial(p, w_s.at[lax.rem(p, W_SLOTS)])

        @pl.when(p == 2)
        def _():
            chip_sum(1)

        @pl.when(p > 3)
        def _():
            chip_sum(p - 2)
        return carry

    lax.fori_loop(1, PIECES, compute, 0)
    chip_sum(PIECES - 2)
    chip_sum(PIECES - 1)
    x_in.wait()

    def finish(p, carry):
        copy1(p).wait_send()
        copy2(p).wait_send()
        copy2(p).wait_recv()
        xs = x_s[:, pl.ds(col_of(p, 1), cols)].astype(F32)
        out_ref[:, pl.ds(col_of(p, 1), cols)] = (xs + (sum_s[p].astype(F32) + other_s[p].astype(F32))).astype(BF16)
        copy3(p, core).start()
        return carry

    lax.fori_loop(0, PIECES, finish, 0)

    def drain(p, carry):
        copy3(p, core).wait_send()
        copy3(p, 1 - core).wait_recv()
        return carry

    lax.fori_loop(0, PIECES, drain, 0)


def exchange(x, lhs, w0, wd, wo):
    rows, width = x.shape
    cols = width // 2 // PIECES
    n_ff = wd.shape[0]
    n_ctx = wo.shape[0]
    dma = pltpu.SemaphoreType.DMA
    return pl.pallas_call(
        exchange_kernel,
        name='exchange',
        in_specs=[HBM, VMEM, VMEM, HBM, HBM],
        out_specs=VMEM,
        out_shape=jax.ShapeDtypeStruct((rows, width), BF16),
        scratch_shapes=[
            pltpu.VMEM((rows, width), BF16),
            pltpu.VMEM((W_SLOTS, n_ff + n_ctx, 2 * cols), BF16),
            pltpu.VMEM((PIECES, rows, cols), BF16),
            pltpu.VMEM((PIECES, rows, cols), BF16),
            pltpu.VMEM((PIECES, rows, cols), F32),
            pltpu.VMEM((PIECES, rows, cols), BF16),
            pltpu.VMEM((PIECES, rows, cols), BF16),
            dma((1,)), dma((W_SLOTS,)),
            dma((PIECES,)), dma((PIECES,)), dma((PIECES,)), dma((PIECES,)), dma((PIECES,)), dma((PIECES,)),
        ],
        compiler_params=pltpu.CompilerParams(vmem_limit_bytes=32 * MIB, collective_id=0, has_side_effects=True),
        cost_estimate=pl.CostEstimate(flops=11 * 10 ** 9, bytes_accessed=48 * 10 ** 6, transcendentals=0),
    )(x, lhs, w0, wd, wo)


def solution(mesh):
    row_spec = P('dp', None)
    vec_spec = P(None)
    cache_spec = P('dp', 'tp', None, None)

    def device_step(x, ln_attn_gamma, ln_attn_beta, ln_mlp_gamma, ln_mlp_beta, w_qkv, w_out, w_up, w_down, k_cache, v_cache, positions):
        width = x.shape[1]
        head = w_qkv.shape[3]
        inv_freq = ROPE_BASE ** (-2.0 * np.arange(head // 2) / head)
        freq = jnp.asarray(np.concatenate([inv_freq, inv_freq])[None, :], F32)
        vecs = [v.reshape(1, width) for v in (ln_attn_gamma, ln_attn_beta, ln_mlp_gamma, ln_mlp_beta)]
        wq = jnp.transpose(w_qkv, (0, 2, 1, 3)).reshape(-1, head)
        wo = w_out.reshape(-1, width)
        in_hbm = [pltpu.with_memory_space_constraint(a, pltpu.HBM) for a in (positions, x, *vecs, freq, wq, w_up, w_down, wo, k_cache.reshape(-1, head), v_cache.reshape(-1, head))]
        x_h, wd_h, wo_h = in_hbm[1], in_hbm[-4], in_hbm[-3]
        ko, vo, lhs, w0 = front(*in_hbm)
        out = exchange(x_h, lhs, w0, wd_h, wo_h)
        return out, ko.reshape(k_cache.shape), vo.reshape(v_cache.shape)

    return jax.shard_map(device_step, mesh=mesh, in_specs=(row_spec, vec_spec, vec_spec, vec_spec, vec_spec, P(None, 'tp', None, None), P('tp', None, None, None), P(None, 'tp'), P('tp', None), cache_spec, cache_spec, P('dp')), out_specs=(row_spec, cache_spec, cache_spec), check_vma=False)
```

```python
import jax
import jax.numpy as jnp
import numpy as np
from jax import lax
from jax.experimental import pallas as pl
from jax.experimental.pallas import tpu as pltpu
from jax.sharding import PartitionSpec as P

LN_EPS = 1e-5
ROPE_BASE = 10000.0
NEG_BIG = -1e30
BF16 = jnp.bfloat16
F32 = jnp.float32
ANY = pl.BlockSpec(memory_space=pl.ANY)
HBM = pl.BlockSpec(memory_space=pltpu.HBM)
VMEM = pl.BlockSpec(memory_space=pltpu.VMEM)
SMEM = pl.BlockSpec(memory_space=pltpu.SMEM)
MIB = 1024 * 1024

QKV_CHUNK = 512
LN_ROWS = 16
ROW_BLOCK = 16
KV_SLOTS = 7
KV_AHEAD = 5
UP_SLOTS = 3
UP_EARLY = 3
W_PARTS = 4


def front_kernel(pos_ref, x_hbm, ga_hbm, ba_hbm, gm_hbm, bm_hbm, freq_hbm, wq_hbm, wu_hbm, wd_hbm, wo_hbm, kc_hbm, vc_hbm,
                 ko_hbm, vo_hbm, lhs_ref, w0_ref,
                 x_s, vec_s, freq_s, cos_s, sin_s, attn_s, wqf_s, acc_s, q_s, kv_s, up_s, ctx_s, kbuf, vbuf,
                 in_sem, wq_sem, up_sem, kin_sem, vin_sem, kout_sem, vout_sem, w0_sem):
    mlp_s = x_s
    rows, width = x_s.shape
    seq = kc_hbm.shape[0] // (2 * rows)
    lines_blk = ROW_BLOCK * 2 * seq
    n_ff = lhs_ref.shape[1] - wo_hbm.shape[0]
    n_chunk = width // QKV_CHUNK
    lines = wq_hbm.shape[0] // width
    up_cols = up_s.shape[2]
    n_up = wu_hbm.shape[1] // up_cols
    n_blk = rows // ROW_BLOCK

    x_parts = [pl.ds(k * (rows // W_PARTS), rows // W_PARTS) for k in range(W_PARTS)]
    small = [pltpu.make_async_copy(x_hbm.at[part, :], x_s.at[part, :], in_sem.at[0]) for part in x_parts]
    for i, v in enumerate((ga_hbm, ba_hbm, gm_hbm, bm_hbm)):
        small.append(pltpu.make_async_copy(v, vec_s.at[pl.ds(i, 1), :], in_sem.at[1 + i]))
    freq_in = pltpu.make_async_copy(freq_hbm, freq_s, in_sem.at[5])
    freq_in.start()
    for c in small:
        c.start()

    wq_lines = QKV_CHUNK * lines
    wq_base = (KV_SLOTS - n_chunk * wq_lines // (2 * lines_blk)) * lines_blk
    wq_order = [c for pair in zip(range(n_chunk // 2), range(n_chunk // 2, n_chunk)) for c in pair]

    def wq_view(c):
        buf = kbuf if c < n_chunk // 2 else vbuf
        return buf.at[pl.ds(wq_base + (c % (n_chunk // 2)) * wq_lines, wq_lines), :]

    def wq_copy(c):
        return pltpu.make_async_copy(wq_hbm.at[pl.ds(c * wq_lines, wq_lines), :], wq_view(c), wq_sem.at[c])

    def up_start(b, slot):
        cols = pl.ds(pl.multiple_of(b * up_cols, up_cols), up_cols)
        for k in range(W_PARTS):
            part = pl.ds(k * (width // W_PARTS), width // W_PARTS)
            pltpu.make_async_copy(wu_hbm.at[part, cols], up_s.at[slot, part, :], up_sem.at[slot]).start()

    def up_wait(slot):
        pltpu.make_async_copy(wu_hbm.at[:, pl.ds(0, up_cols)], up_s.at[slot], up_sem.at[slot]).wait()

    def block(ref, i):
        return ref.at[pl.ds(pl.multiple_of(i * lines_blk, lines_blk), lines_blk), :]

    def start_in(i, slot):
        pltpu.make_async_copy(block(kc_hbm, i), block(kbuf, slot), kin_sem.at[slot]).start(priority=1)
        pltpu.make_async_copy(block(vc_hbm, i), block(vbuf, slot), vin_sem.at[slot]).start(priority=1)

    def wait_in(slot):
        pltpu.make_async_copy(block(kc_hbm, 0), block(kbuf, slot), kin_sem.at[slot]).wait()
        pltpu.make_async_copy(block(vc_hbm, 0), block(vbuf, slot), vin_sem.at[slot]).wait()

    def start_out(i, slot):
        pltpu.make_async_copy(block(kbuf, slot), block(ko_hbm, i), kout_sem.at[slot]).start()
        pltpu.make_async_copy(block(vbuf, slot), block(vo_hbm, i), vout_sem.at[slot]).start()

    def wait_out(slot):
        pltpu.make_async_copy(block(kbuf, slot), block(ko_hbm, 0), kout_sem.at[slot]).wait()
        pltpu.make_async_copy(block(vbuf, slot), block(vo_hbm, 0), vout_sem.at[slot]).wait()

    for c in wq_order[:2]:
        wq_copy(c).start()
    start_in(0, 0)

    freq_in.wait()

    def angle_body(b, carry):
        cos_s[pl.ds(b, 1), :] = pos_ref[b].astype(F32) * freq_s[0:1, :]
        return carry

    lax.fori_loop(0, rows, angle_body, 0, unroll=8)
    ang = cos_s[...]
    low = lax.broadcasted_iota(jnp.int32, ang.shape, 1) < 64
    sin_t = jnp.sin(ang)
    sin_s[...] = jnp.where(low, -sin_t, sin_t)
    cos_s[...] = jnp.cos(ang)

    for c in small:
        c.wait()
    for c in wq_order[2:4]:
        wq_copy(c).start()
    start_in(1, 1)

    def ln_body(i, carry):
        r = pl.ds(pl.multiple_of(i * LN_ROWS, LN_ROWS), LN_ROWS)
        xf = x_s[r, :].astype(F32)
        mean = jnp.mean(xf, axis=-1, keepdims=True)
        cen = xf - mean
        var = jnp.mean(cen * cen, axis=-1, keepdims=True)
        nrm = cen * lax.rsqrt(var + LN_EPS)
        attn_s[r, :] = (nrm * vec_s[0:1, :] + vec_s[1:2, :]).astype(BF16)
        mlp_s[r, :] = (nrm * vec_s[2:3, :] + vec_s[3:4, :]).astype(BF16)
        return carry

    half_ln = rows // LN_ROWS // 2
    lax.fori_loop(0, half_ln, ln_body, 0)
    for c in wq_order[4:]:
        wq_copy(c).start()
    free = wq_base // lines_blk
    for i in range(2, free):
        start_in(i, i)
    lax.fori_loop(half_ln, 2 * half_ln, ln_body, 0)

    for step, c in enumerate(wq_order):
        wq_copy(c).wait()
        if step == n_chunk - 2:
            for i in range(free, KV_AHEAD):
                start_in(i, i)
        if step >= n_chunk - UP_SLOTS:
            up_start(step - n_chunk + UP_SLOTS, step - n_chunk + UP_SLOTS)
        wqf_s[...] = wq_view(c)[...].astype(F32)
        lhs = attn_s[:, c * QKV_CHUNK:(c + 1) * QKV_CHUNK]
        for pair in range(lines // 2):
            w = jnp.concatenate([wqf_s[pl.ds(2 * pair + e, QKV_CHUNK, stride=lines), :].astype(BF16) for e in range(2)], axis=1)
            part = jnp.dot(lhs, w, preferred_element_type=F32)
            if step == 0:
                acc_s[:, pair * 256:(pair + 1) * 256] = part
            else:
                acc_s[:, pair * 256:(pair + 1) * 256] += part

    n_slot = lines // 2
    n_q = n_slot - 2
    for j in range(n_slot):
        for g in range(2):
            col = (2 * j + g) * 128
            u = acc_s[:, col:col + 128].astype(BF16).astype(F32)
            if j < n_q + 1:
                u = (u * cos_s[...] + pltpu.roll(u, 64, 1) * sin_s[...]).astype(BF16).astype(F32)
            if j < n_q:
                q_s[pl.ds((g * n_q + j) * rows, rows), :] = u
            else:
                kv_s[pl.ds(((j - n_q) * 2 + g) * rows, rows), :] = u

    slot_ids = lax.broadcasted_iota(jnp.int32, (8, 256), 1)
    tile_ids = lax.broadcasted_iota(jnp.int32, (16, 128), 0)
    first = lax.broadcasted_iota(jnp.int32, (8, 128), 0) < 4
    scale = 128 ** -0.5

    def pair_of(buf, slot, r):
        at = [pl.ds(pl.multiple_of(slot * lines_blk + (2 * r + g) * seq, seq), seq) for g in range(2)]
        return jnp.concatenate([buf[a, :] for a in at], axis=1)

    def attend_block(i, slot):
        pos = [pos_ref[i * ROW_BLOCK + r] for r in range(ROW_BLOCK)]
        for r in range(ROW_BLOCK):
            base = pl.multiple_of((pos[r] // 16) * 16, 16)
            hit = tile_ids == pos[r] - base
            b = i * ROW_BLOCK + r
            for g in range(2):
                tile = pl.ds(pl.multiple_of(slot * lines_blk + (2 * r + g) * seq + base, 16), 16)
                for buf, which in ((kbuf, 0), (vbuf, 1)):
                    new = kv_s[pl.ds((which * 2 + g) * rows + b, 1), :]
                    buf[tile, :] = jnp.where(hit, new, buf[tile, :].astype(F32)).astype(BF16)
        scores = []
        for r in range(ROW_BLOCK):
            b = i * ROW_BLOCK + r
            q = q_s[pl.ds(b, 8, stride=rows), :]
            zero = jnp.zeros_like(q)
            q2 = jnp.concatenate([jnp.where(first, q, zero), jnp.where(first, zero, q)], axis=1).astype(BF16)
            k2 = pair_of(kbuf, slot, r)
            s = lax.dot_general(q2, k2, (((1,), (1,)), ((), ())), preferred_element_type=F32) * scale
            scores.append(jnp.where(slot_ids <= pos[r], s, NEG_BIG))
        s = jnp.concatenate(scores, axis=0)
        e = jnp.exp(s - jnp.max(s, axis=-1, keepdims=True))
        p = (e / jnp.sum(e, axis=-1, keepdims=True)).astype(BF16)
        for r in range(ROW_BLOCK):
            v2 = pair_of(vbuf, slot, r)
            c = jnp.dot(p[8 * r:8 * r + 8], v2, preferred_element_type=F32)
            ctx_s[pl.ds(i * ROW_BLOCK + r, 8, stride=rows), :] = jnp.where(first, c[:, :128], c[:, 128:])

    core = lax.rem(lax.axis_index('tp'), 2)
    cols = w0_ref.shape[1] // 2
    w0_in = []
    for part in range(2):
        src = pl.ds(pl.multiple_of((core if part else 1 - core) * (wd_hbm.shape[1] // 2), cols), cols)
        dst = pl.ds(part * cols, cols)
        w0_in.append(pltpu.make_async_copy(wd_hbm.at[:, src], w0_ref.at[pl.ds(0, n_ff), dst], w0_sem.at[0]))
        w0_in.append(pltpu.make_async_copy(wo_hbm.at[:, src], w0_ref.at[pl.ds(n_ff, wo_hbm.shape[0]), dst], w0_sem.at[0]))

    def up_block(b):
        uslot = lax.rem(b, UP_SLOTS)
        deep = width // 2
        pre = (jnp.dot(mlp_s[:, :deep], up_s[uslot, :deep, :], preferred_element_type=F32)
               + jnp.dot(mlp_s[:, deep:], up_s[uslot, deep:, :], preferred_element_type=F32))
        act = 0.5 * pre * (1.0 + lax.erf(pre * (0.5 ** 0.5)))
        lhs_ref[:, pl.ds(pl.multiple_of(b * up_cols, up_cols), up_cols)] = act.astype(BF16)

    def body(i, carry, with_up):
        nxt = i + KV_AHEAD

        @pl.when(nxt < n_blk)
        def _():
            nslot = lax.rem(nxt, KV_SLOTS)

            @pl.when(nxt >= KV_SLOTS)
            def _():
                wait_out(nslot)
            start_in(nxt, nslot)

        slot = lax.rem(i, KV_SLOTS)
        if with_up:
            b = i + UP_EARLY

            @pl.when(b - 1 + UP_SLOTS < n_up)
            def _():
                up_start(b - 1 + UP_SLOTS, lax.rem(b - 1, UP_SLOTS))

            up_wait(lax.rem(b, UP_SLOTS))
            wait_in(slot)
            up_block(b)
        else:
            wait_in(slot)
        attend_block(i, slot)
        start_out(i, slot)

        @pl.when(i == n_blk - 5)
        def _():
            for c in w0_in:
                c.start(priority=1)
        return carry

    for b in range(UP_EARLY):
        up_wait(b % UP_SLOTS)
        up_block(b)
        if b:
            up_start(b - 1 + UP_SLOTS, (b - 1) % UP_SLOTS)
    lax.fori_loop(0, n_blk - UP_EARLY, lambda i, c: body(i, c, True), 0)
    lax.fori_loop(n_blk - UP_EARLY, n_blk, lambda i, c: body(i, c, False), 0)
    for h in range(ctx_s.shape[0] // rows):
        lhs_ref[:, n_ff + h * 128:n_ff + (h + 1) * 128] = ctx_s[h * rows:(h + 1) * rows, :].astype(BF16)
    for c in w0_in:
        c.wait()
    for i in range(n_blk - KV_SLOTS, n_blk):
        wait_out(i % KV_SLOTS)


def front(pos, x, ga, ba, gm, bm, freq, wq, wu, wd, wo, kc, vc):
    rows, width = x.shape
    hid = wu.shape[1]
    lines = wq.shape[0] // width
    n_head = (lines // 2 - 2) * 2
    up_cols = hid // (rows // ROW_BLOCK)
    lines_blk = kc.shape[0] // rows * ROW_BLOCK
    return pl.pallas_call(
        front_kernel,
        name='front',
        in_specs=[SMEM] + [HBM] * 12,
        out_specs=[HBM, HBM, VMEM, VMEM],
        out_shape=[
            jax.ShapeDtypeStruct(kc.shape, BF16),
            jax.ShapeDtypeStruct(vc.shape, BF16),
            jax.ShapeDtypeStruct((rows, hid + wo.shape[0]), BF16),
            jax.ShapeDtypeStruct((hid + wo.shape[0], width // PIECES), BF16),
        ],
        scratch_shapes=[
            pltpu.VMEM((rows, width), BF16),
            pltpu.VMEM((4, width), F32),
            pltpu.VMEM((1, 128), F32),
            pltpu.VMEM((rows, 128), F32),
            pltpu.VMEM((rows, 128), F32),
            pltpu.VMEM((rows, width), BF16),
            pltpu.VMEM((QKV_CHUNK * lines, 128), F32),
            pltpu.VMEM((rows, lines * 128), F32),
            pltpu.VMEM((n_head * rows, 128), F32),
            pltpu.VMEM((4 * rows, 128), F32),
            pltpu.VMEM((UP_SLOTS, width, up_cols), BF16),
            pltpu.VMEM((n_head * rows, 128), F32),
            pltpu.VMEM((KV_SLOTS * lines_blk, 128), BF16),
            pltpu.VMEM((KV_SLOTS * lines_blk, 128), BF16),
            pltpu.SemaphoreType.DMA((6,)),
            pltpu.SemaphoreType.DMA((width // QKV_CHUNK,)),
            pltpu.SemaphoreType.DMA((UP_SLOTS,)),
            pltpu.SemaphoreType.DMA((KV_SLOTS,)),
            pltpu.SemaphoreType.DMA((KV_SLOTS,)),
            pltpu.SemaphoreType.DMA((KV_SLOTS,)),
            pltpu.SemaphoreType.DMA((KV_SLOTS,)),
            pltpu.SemaphoreType.DMA((1,)),
        ],
        compiler_params=pltpu.CompilerParams(vmem_limit_bytes=47 * MIB),
        cost_estimate=pl.CostEstimate(flops=22 * 10 ** 9, bytes_accessed=180 * 10 ** 6, transcendentals=0),
    )(pos, x, ga, ba, gm, bm, freq, wq, wu, wd, wo, kc, vc)


PIECES = 16
W_SLOTS = 4
MESH = pl.DeviceIdType.MESH


def exchange_kernel(x_hbm, lhs_s, w0_ref, wd_hbm, wo_hbm, out_ref,
                    x_s, w_s, send_s, recv_s, keep_s, sum_s, other_s,
                    in_sem, w_sem, c1_send, c1_recv, c2_send, c2_recv, c3_send, c3_recv):
    rows, width = x_s.shape
    half = width // 2
    cols = half // PIECES
    n_ff, n_ctx = wd_hbm.shape[0], wo_hbm.shape[0]
    me = lax.axis_index('tp')
    core = lax.rem(me, 2)
    mate = me + 1 - 2 * core
    far = lax.rem(me + 2, 4)

    def col_of(p, part):
        side = core if part else 1 - core
        return pl.multiple_of(side * half + p * cols, cols)

    def w_start(p):
        slot = lax.rem(p, W_SLOTS)
        for part in range(2):
            src, dst = pl.ds(col_of(p, part), cols), pl.ds(part * cols, cols)
            pltpu.make_async_copy(wo_hbm.at[:, src], w_s.at[slot, pl.ds(n_ff, n_ctx), dst], w_sem.at[slot]).start()
            for k in range(2):
                deep = pl.ds(k * (n_ff // 2), n_ff // 2)
                pltpu.make_async_copy(wd_hbm.at[deep, src], w_s.at[slot, deep, dst], w_sem.at[slot]).start()

    def w_wait(p):
        slot = lax.rem(p, W_SLOTS)
        for part in range(2):
            dst = pl.ds(part * cols, cols)
            pltpu.make_async_copy(wo_hbm.at[:, pl.ds(0, cols)], w_s.at[slot, pl.ds(n_ff, n_ctx), dst], w_sem.at[slot]).wait()
            pltpu.make_async_copy(wd_hbm.at[:, pl.ds(0, cols)], w_s.at[slot, pl.ds(0, n_ff), dst], w_sem.at[slot]).wait()

    w_start(1)
    x_in = pltpu.make_async_copy(x_hbm, x_s, in_sem.at[0])

    barrier = pltpu.get_barrier_semaphore()
    for peer in (mate, far):
        pl.semaphore_signal(barrier, inc=1, device_id={'tp': peer}, device_id_type=MESH)
    pl.semaphore_wait(barrier, 2)

    def copy1(p):
        return pltpu.make_async_remote_copy(send_s.at[p], recv_s.at[p], c1_send.at[p], c1_recv.at[p], device_id={'tp': mate}, device_id_type=MESH)

    def copy2(p):
        return pltpu.make_async_remote_copy(sum_s.at[p], other_s.at[p], c2_send.at[p], c2_recv.at[p], device_id={'tp': far}, device_id_type=MESH)

    def copy3(p, side):
        view = out_ref.at[:, pl.ds(pl.multiple_of(side * half + p * cols, cols), cols)]
        return pltpu.make_async_remote_copy(view, view, c3_send.at[p], c3_recv.at[p], device_id={'tp': mate}, device_id_type=MESH)

    def chip_sum(p):
        copy1(p).wait_recv()
        sum_s[p] = (keep_s[p] + recv_s[p].astype(F32)).astype(BF16)
        copy2(p).start()

    def partial(p, w):
        deep = (n_ff + n_ctx) // 2
        s = (jnp.dot(lhs_s[:, :deep], w[:deep, :], preferred_element_type=F32)
             + jnp.dot(lhs_s[:, deep:], w[deep:, :], preferred_element_type=F32))
        send_s[p] = s[:, :cols].astype(BF16)
        keep_s[p] = s[:, cols:]
        copy1(p).start()

    partial(0, w0_ref)
    w_start(2)
    chip_sum(0)
    w_start(3)
    x_in.start()

    def compute(p, carry):
        w_wait(p)

        @pl.when(p + 3 < PIECES)
        def _():
            w_start(p + 3)
        partial(p, w_s.at[lax.rem(p, W_SLOTS)])

        @pl.when(p > 1)
        def _():
            chip_sum(p - 1)
        return carry

    lax.fori_loop(1, PIECES, compute, 0)
    chip_sum(PIECES - 1)
    x_in.wait()

    def finish(p, carry):
        copy1(p).wait_send()
        copy2(p).wait_send()
        copy2(p).wait_recv()
        xs = x_s[:, pl.ds(col_of(p, 1), cols)].astype(F32)
        out_ref[:, pl.ds(col_of(p, 1), cols)] = (xs + (sum_s[p].astype(F32) + other_s[p].astype(F32))).astype(BF16)
        copy3(p, core).start()
        return carry

    lax.fori_loop(0, PIECES, finish, 0)

    def drain(p, carry):
        copy3(p, core).wait_send()
        copy3(p, 1 - core).wait_recv()
        return carry

    lax.fori_loop(0, PIECES, drain, 0)


def exchange(x, lhs, w0, wd, wo):
    rows, width = x.shape
    cols = width // 2 // PIECES
    n_ff = wd.shape[0]
    n_ctx = wo.shape[0]
    dma = pltpu.SemaphoreType.DMA
    return pl.pallas_call(
        exchange_kernel,
        name='exchange',
        in_specs=[HBM, VMEM, VMEM, HBM, HBM],
        out_specs=VMEM,
        out_shape=jax.ShapeDtypeStruct((rows, width), BF16),
        scratch_shapes=[
            pltpu.VMEM((rows, width), BF16),
            pltpu.VMEM((W_SLOTS, n_ff + n_ctx, 2 * cols), BF16),
            pltpu.VMEM((PIECES, rows, cols), BF16),
            pltpu.VMEM((PIECES, rows, cols), BF16),
            pltpu.VMEM((PIECES, rows, cols), F32),
            pltpu.VMEM((PIECES, rows, cols), BF16),
            pltpu.VMEM((PIECES, rows, cols), BF16),
            dma((1,)), dma((W_SLOTS,)),
            dma((PIECES,)), dma((PIECES,)), dma((PIECES,)), dma((PIECES,)), dma((PIECES,)), dma((PIECES,)),
        ],
        compiler_params=pltpu.CompilerParams(vmem_limit_bytes=32 * MIB, collective_id=0, has_side_effects=True),
        cost_estimate=pl.CostEstimate(flops=11 * 10 ** 9, bytes_accessed=48 * 10 ** 6, transcendentals=0),
    )(x, lhs, w0, wd, wo)


def solution(mesh):
    row_spec = P('dp', None)
    vec_spec = P(None)
    cache_spec = P('dp', 'tp', None, None)

    def device_step(x, ln_attn_gamma, ln_attn_beta, ln_mlp_gamma, ln_mlp_beta, w_qkv, w_out, w_up, w_down, k_cache, v_cache, positions):
        width = x.shape[1]
        head = w_qkv.shape[3]
        inv_freq = ROPE_BASE ** (-2.0 * np.arange(head // 2) / head)
        freq = jnp.asarray(np.concatenate([inv_freq, inv_freq])[None, :], F32)
        vecs = [v.reshape(1, width) for v in (ln_attn_gamma, ln_attn_beta, ln_mlp_gamma, ln_mlp_beta)]
        wq = jnp.transpose(w_qkv, (0, 2, 1, 3)).reshape(-1, head)
        wo = w_out.reshape(-1, width)
        in_hbm = [pltpu.with_memory_space_constraint(a, pltpu.HBM) for a in (positions, x, *vecs, freq, wq, w_up, w_down, wo, k_cache.reshape(-1, head), v_cache.reshape(-1, head))]
        x_h, wd_h, wo_h = in_hbm[1], in_hbm[-4], in_hbm[-3]
        ko, vo, lhs, w0 = front(*in_hbm)
        out = exchange(x_h, lhs, w0, wd_h, wo_h)
        return out, ko.reshape(k_cache.shape), vo.reshape(v_cache.shape)

    return jax.shard_map(device_step, mesh=mesh, in_specs=(row_spec, vec_spec, vec_spec, vec_spec, vec_spec, P(None, 'tp', None, None), P('tp', None, None, None), P(None, 'tp'), P('tp', None), cache_spec, cache_spec, P('dp')), out_specs=(row_spec, cache_spec, cache_spec), check_vma=False)
```

```python
import jax
import jax.numpy as jnp
import numpy as np
from jax import lax
from jax.experimental import pallas as pl
from jax.experimental.pallas import tpu as pltpu
from jax.sharding import PartitionSpec as P

LN_EPS = 1e-5
ROPE_BASE = 10000.0
NEG_BIG = -1e30
BF16 = jnp.bfloat16
F32 = jnp.float32
ANY = pl.BlockSpec(memory_space=pl.ANY)
HBM = pl.BlockSpec(memory_space=pltpu.HBM)
VMEM = pl.BlockSpec(memory_space=pltpu.VMEM)
SMEM = pl.BlockSpec(memory_space=pltpu.SMEM)
MIB = 1024 * 1024

QKV_CHUNK = 512
LN_ROWS = 16
ROW_BLOCK = 16
KV_SLOTS = 7
KV_AHEAD = 5
UP_SLOTS = 3
W_PARTS = 4


def front_kernel(pos_ref, x_hbm, ga_hbm, ba_hbm, gm_hbm, bm_hbm, freq_hbm, wq_hbm, wu_hbm, wd_hbm, wo_hbm, kc_hbm, vc_hbm,
                 ko_hbm, vo_hbm, lhs_ref, w0_ref,
                 x_s, vec_s, freq_s, cos_s, sin_s, attn_s, wqf_s, acc_s, q_s, kv_s, up_s, ctx_s, kbuf, vbuf,
                 in_sem, wq_sem, up_sem, kin_sem, vin_sem, kout_sem, vout_sem, w0_sem):
    mlp_s = x_s
    rows, width = x_s.shape
    seq = kc_hbm.shape[0] // (2 * rows)
    lines_blk = ROW_BLOCK * 2 * seq
    n_ff = lhs_ref.shape[1] - wo_hbm.shape[0]
    n_chunk = width // QKV_CHUNK
    lines = wq_hbm.shape[0] // width
    up_cols = up_s.shape[2]
    n_up = wu_hbm.shape[1] // up_cols
    n_blk = rows // ROW_BLOCK

    x_parts = [pl.ds(k * (rows // W_PARTS), rows // W_PARTS) for k in range(W_PARTS)]
    small = [pltpu.make_async_copy(x_hbm.at[part, :], x_s.at[part, :], in_sem.at[0]) for part in x_parts]
    for i, v in enumerate((ga_hbm, ba_hbm, gm_hbm, bm_hbm)):
        small.append(pltpu.make_async_copy(v, vec_s.at[pl.ds(i, 1), :], in_sem.at[1 + i]))
    freq_in = pltpu.make_async_copy(freq_hbm, freq_s, in_sem.at[5])
    freq_in.start()
    for c in small:
        c.start()

    wq_lines = QKV_CHUNK * lines
    wq_base = (KV_SLOTS - n_chunk * wq_lines // (2 * lines_blk)) * lines_blk
    wq_order = [c for pair in zip(range(n_chunk // 2), range(n_chunk // 2, n_chunk)) for c in pair]

    def wq_view(c):
        buf = kbuf if c < n_chunk // 2 else vbuf
        return buf.at[pl.ds(wq_base + (c % (n_chunk // 2)) * wq_lines, wq_lines), :]

    def wq_copy(c):
        return pltpu.make_async_copy(wq_hbm.at[pl.ds(c * wq_lines, wq_lines), :], wq_view(c), wq_sem.at[c])

    def up_start(b, slot):
        cols = pl.ds(pl.multiple_of(b * up_cols, up_cols), up_cols)
        for k in range(W_PARTS):
            part = pl.ds(k * (width // W_PARTS), width // W_PARTS)
            pltpu.make_async_copy(wu_hbm.at[part, cols], up_s.at[slot, part, :], up_sem.at[slot]).start()

    def up_wait(slot):
        pltpu.make_async_copy(wu_hbm.at[:, pl.ds(0, up_cols)], up_s.at[slot], up_sem.at[slot]).wait()

    def block(ref, i):
        return ref.at[pl.ds(pl.multiple_of(i * lines_blk, lines_blk), lines_blk), :]

    def start_in(i, slot):
        pltpu.make_async_copy(block(kc_hbm, i), block(kbuf, slot), kin_sem.at[slot]).start(priority=1)
        pltpu.make_async_copy(block(vc_hbm, i), block(vbuf, slot), vin_sem.at[slot]).start(priority=1)

    def wait_in(slot):
        pltpu.make_async_copy(block(kc_hbm, 0), block(kbuf, slot), kin_sem.at[slot]).wait()
        pltpu.make_async_copy(block(vc_hbm, 0), block(vbuf, slot), vin_sem.at[slot]).wait()

    def start_out(i, slot):
        pltpu.make_async_copy(block(kbuf, slot), block(ko_hbm, i), kout_sem.at[slot]).start()
        pltpu.make_async_copy(block(vbuf, slot), block(vo_hbm, i), vout_sem.at[slot]).start()

    def wait_out(slot):
        pltpu.make_async_copy(block(kbuf, slot), block(ko_hbm, 0), kout_sem.at[slot]).wait()
        pltpu.make_async_copy(block(vbuf, slot), block(vo_hbm, 0), vout_sem.at[slot]).wait()

    for c in wq_order[:2]:
        wq_copy(c).start()
    start_in(0, 0)

    freq_in.wait()

    def angle_body(b, carry):
        cos_s[pl.ds(b, 1), :] = pos_ref[b].astype(F32) * freq_s[0:1, :]
        return carry

    lax.fori_loop(0, rows, angle_body, 0, unroll=8)
    ang = cos_s[...]
    low = lax.broadcasted_iota(jnp.int32, ang.shape, 1) < 64
    sin_t = jnp.sin(ang)
    sin_s[...] = jnp.where(low, -sin_t, sin_t)
    cos_s[...] = jnp.cos(ang)

    for c in small:
        c.wait()
    for c in wq_order[2:4]:
        wq_copy(c).start()
    start_in(1, 1)

    def ln_body(i, carry):
        r = pl.ds(pl.multiple_of(i * LN_ROWS, LN_ROWS), LN_ROWS)
        xf = x_s[r, :].astype(F32)
        mean = jnp.mean(xf, axis=-1, keepdims=True)
        cen = xf - mean
        var = jnp.mean(cen * cen, axis=-1, keepdims=True)
        nrm = cen * lax.rsqrt(var + LN_EPS)
        attn_s[r, :] = (nrm * vec_s[0:1, :] + vec_s[1:2, :]).astype(BF16)
        mlp_s[r, :] = (nrm * vec_s[2:3, :] + vec_s[3:4, :]).astype(BF16)
        return carry

    half_ln = rows // LN_ROWS // 2
    lax.fori_loop(0, half_ln, ln_body, 0)
    for c in wq_order[4:]:
        wq_copy(c).start()
    free = wq_base // lines_blk
    for i in range(2, free):
        start_in(i, i)
    lax.fori_loop(half_ln, 2 * half_ln, ln_body, 0)

    for step, c in enumerate(wq_order):
        wq_copy(c).wait()
        if step == n_chunk - 2:
            for i in range(free, KV_AHEAD):
                start_in(i, i)
        if step >= n_chunk - UP_SLOTS:
            up_start(step - n_chunk + UP_SLOTS, step - n_chunk + UP_SLOTS)
        wqf_s[...] = wq_view(c)[...].astype(F32)
        lhs = attn_s[:, c * QKV_CHUNK:(c + 1) * QKV_CHUNK]
        for pair in range(lines // 2):
            w = jnp.concatenate([wqf_s[pl.ds(2 * pair + e, QKV_CHUNK, stride=lines), :].astype(BF16) for e in range(2)], axis=1)
            part = jnp.dot(lhs, w, preferred_element_type=F32)
            if step == 0:
                acc_s[:, pair * 256:(pair + 1) * 256] = part
            else:
                acc_s[:, pair * 256:(pair + 1) * 256] += part

    n_slot = lines // 2
    n_q = n_slot - 2
    for j in range(n_slot):
        for g in range(2):
            col = (2 * j + g) * 128
            u = acc_s[:, col:col + 128].astype(BF16).astype(F32)
            if j < n_q + 1:
                u = (u * cos_s[...] + pltpu.roll(u, 64, 1) * sin_s[...]).astype(BF16).astype(F32)
            if j < n_q:
                q_s[pl.ds((g * n_q + j) * rows, rows), :] = u
            else:
                kv_s[pl.ds(((j - n_q) * 2 + g) * rows, rows), :] = u

    slot_ids = lax.broadcasted_iota(jnp.int32, (8, 256), 1)
    tile_ids = lax.broadcasted_iota(jnp.int32, (16, 128), 0)
    first = lax.broadcasted_iota(jnp.int32, (8, 128), 0) < 4
    scale = 128 ** -0.5

    def pair_of(buf, slot, r):
        at = [pl.ds(pl.multiple_of(slot * lines_blk + (2 * r + g) * seq, seq), seq) for g in range(2)]
        return jnp.concatenate([buf[a, :] for a in at], axis=1)

    def attend_block(i, slot):
        pos = [pos_ref[i * ROW_BLOCK + r] for r in range(ROW_BLOCK)]
        for r in range(ROW_BLOCK):
            base = pl.multiple_of((pos[r] // 16) * 16, 16)
            hit = tile_ids == pos[r] - base
            b = i * ROW_BLOCK + r
            for g in range(2):
                tile = pl.ds(pl.multiple_of(slot * lines_blk + (2 * r + g) * seq + base, 16), 16)
                for buf, which in ((kbuf, 0), (vbuf, 1)):
                    new = kv_s[pl.ds((which * 2 + g) * rows + b, 1), :]
                    buf[tile, :] = jnp.where(hit, new, buf[tile, :].astype(F32)).astype(BF16)
        scores = []
        for r in range(ROW_BLOCK):
            b = i * ROW_BLOCK + r
            q = q_s[pl.ds(b, 8, stride=rows), :]
            zero = jnp.zeros_like(q)
            q2 = jnp.concatenate([jnp.where(first, q, zero), jnp.where(first, zero, q)], axis=1).astype(BF16)
            k2 = pair_of(kbuf, slot, r)
            s = lax.dot_general(q2, k2, (((1,), (1,)), ((), ())), preferred_element_type=F32) * scale
            scores.append(jnp.where(slot_ids <= pos[r], s, NEG_BIG))
        s = jnp.concatenate(scores, axis=0)
        e = jnp.exp(s - jnp.max(s, axis=-1, keepdims=True))
        p = (e / jnp.sum(e, axis=-1, keepdims=True)).astype(BF16)
        for r in range(ROW_BLOCK):
            v2 = pair_of(vbuf, slot, r)
            c = jnp.dot(p[8 * r:8 * r + 8], v2, preferred_element_type=F32)
            ctx_s[pl.ds(i * ROW_BLOCK + r, 8, stride=rows), :] = jnp.where(first, c[:, :128], c[:, 128:])

    core = lax.rem(lax.axis_index('tp'), 2)
    cols = w0_ref.shape[1] // 2
    w0_in = []
    for part in range(2):
        src = pl.ds(pl.multiple_of((core if part else 1 - core) * (wd_hbm.shape[1] // 2), cols), cols)
        dst = pl.ds(part * cols, cols)
        w0_in.append(pltpu.make_async_copy(wd_hbm.at[:, src], w0_ref.at[pl.ds(0, n_ff), dst], w0_sem.at[0]))
        w0_in.append(pltpu.make_async_copy(wo_hbm.at[:, src], w0_ref.at[pl.ds(n_ff, wo_hbm.shape[0]), dst], w0_sem.at[0]))

    def up_block(b):
        uslot = lax.rem(b, UP_SLOTS)
        deep = width // 2
        pre = (jnp.dot(mlp_s[:, :deep], up_s[uslot, :deep, :], preferred_element_type=F32)
               + jnp.dot(mlp_s[:, deep:], up_s[uslot, deep:, :], preferred_element_type=F32))
        act = 0.5 * pre * (1.0 + lax.erf(pre * (0.5 ** 0.5)))
        lhs_ref[:, pl.ds(pl.multiple_of(b * up_cols, up_cols), up_cols)] = act.astype(BF16)

    def body(i, carry):
        nxt = i + KV_AHEAD

        @pl.when(nxt < n_blk)
        def _():
            nslot = lax.rem(nxt, KV_SLOTS)

            @pl.when(nxt >= KV_SLOTS)
            def _():
                wait_out(nslot)
            start_in(nxt, nslot)

        slot = lax.rem(i, KV_SLOTS)

        @pl.when((i >= 1) & (i - 1 + UP_SLOTS < n_up))
        def _():
            up_start(i - 1 + UP_SLOTS, lax.rem(i - 1, UP_SLOTS))

        up_wait(lax.rem(i, UP_SLOTS))
        wait_in(slot)
        up_block(i)
        attend_block(i, slot)
        start_out(i, slot)

        @pl.when(i == n_blk - 5)
        def _():
            for c in w0_in:
                c.start(priority=1)
        return carry

    lax.fori_loop(0, n_blk, body, 0)
    for h in range(ctx_s.shape[0] // rows):
        lhs_ref[:, n_ff + h * 128:n_ff + (h + 1) * 128] = ctx_s[h * rows:(h + 1) * rows, :].astype(BF16)
    for c in w0_in:
        c.wait()
    for i in range(n_blk - KV_SLOTS, n_blk):
        wait_out(i % KV_SLOTS)


def front(pos, x, ga, ba, gm, bm, freq, wq, wu, wd, wo, kc, vc):
    rows, width = x.shape
    hid = wu.shape[1]
    lines = wq.shape[0] // width
    n_head = (lines // 2 - 2) * 2
    up_cols = hid // (rows // ROW_BLOCK)
    lines_blk = kc.shape[0] // rows * ROW_BLOCK
    return pl.pallas_call(
        front_kernel,
        name='front',
        in_specs=[SMEM] + [HBM] * 12,
        out_specs=[HBM, HBM, VMEM, VMEM],
        out_shape=[
            jax.ShapeDtypeStruct(kc.shape, BF16),
            jax.ShapeDtypeStruct(vc.shape, BF16),
            jax.ShapeDtypeStruct((rows, hid + wo.shape[0]), BF16),
            jax.ShapeDtypeStruct((hid + wo.shape[0], width // PIECES), BF16),
        ],
        scratch_shapes=[
            pltpu.VMEM((rows, width), BF16),
            pltpu.VMEM((4, width), F32),
            pltpu.VMEM((1, 128), F32),
            pltpu.VMEM((rows, 128), F32),
            pltpu.VMEM((rows, 128), F32),
            pltpu.VMEM((rows, width), BF16),
            pltpu.VMEM((QKV_CHUNK * lines, 128), F32),
            pltpu.VMEM((rows, lines * 128), F32),
            pltpu.VMEM((n_head * rows, 128), F32),
            pltpu.VMEM((4 * rows, 128), F32),
            pltpu.VMEM((UP_SLOTS, width, up_cols), BF16),
            pltpu.VMEM((n_head * rows, 128), F32),
            pltpu.VMEM((KV_SLOTS * lines_blk, 128), BF16),
            pltpu.VMEM((KV_SLOTS * lines_blk, 128), BF16),
            pltpu.SemaphoreType.DMA((6,)),
            pltpu.SemaphoreType.DMA((width // QKV_CHUNK,)),
            pltpu.SemaphoreType.DMA((UP_SLOTS,)),
            pltpu.SemaphoreType.DMA((KV_SLOTS,)),
            pltpu.SemaphoreType.DMA((KV_SLOTS,)),
            pltpu.SemaphoreType.DMA((KV_SLOTS,)),
            pltpu.SemaphoreType.DMA((KV_SLOTS,)),
            pltpu.SemaphoreType.DMA((1,)),
        ],
        compiler_params=pltpu.CompilerParams(vmem_limit_bytes=47 * MIB),
        cost_estimate=pl.CostEstimate(flops=22 * 10 ** 9, bytes_accessed=180 * 10 ** 6, transcendentals=0),
    )(pos, x, ga, ba, gm, bm, freq, wq, wu, wd, wo, kc, vc)


PIECES = 16
W_SLOTS = 4
MESH = pl.DeviceIdType.MESH


def exchange_kernel(x_hbm, lhs_s, w0_ref, wd_hbm, wo_hbm, out_ref,
                    x_s, w_s, send_s, recv_s, keep_s, sum_s, other_s,
                    in_sem, w_sem, c1_send, c1_recv, c2_send, c2_recv, c3_send, c3_recv):
    rows, width = x_s.shape
    half = width // 2
    cols = half // PIECES
    n_ff, n_ctx = wd_hbm.shape[0], wo_hbm.shape[0]
    me = lax.axis_index('tp')
    core = lax.rem(me, 2)
    mate = me + 1 - 2 * core
    far = lax.rem(me + 2, 4)

    def col_of(p, part):
        side = core if part else 1 - core
        return pl.multiple_of(side * half + p * cols, cols)

    def w_start(p):
        slot = lax.rem(p, W_SLOTS)
        for part in range(2):
            src, dst = pl.ds(col_of(p, part), cols), pl.ds(part * cols, cols)
            pltpu.make_async_copy(wo_hbm.at[:, src], w_s.at[slot, pl.ds(n_ff, n_ctx), dst], w_sem.at[slot]).start()
            for k in range(2):
                deep = pl.ds(k * (n_ff // 2), n_ff // 2)
                pltpu.make_async_copy(wd_hbm.at[deep, src], w_s.at[slot, deep, dst], w_sem.at[slot]).start()

    def w_wait(p):
        slot = lax.rem(p, W_SLOTS)
        for part in range(2):
            dst = pl.ds(part * cols, cols)
            pltpu.make_async_copy(wo_hbm.at[:, pl.ds(0, cols)], w_s.at[slot, pl.ds(n_ff, n_ctx), dst], w_sem.at[slot]).wait()
            pltpu.make_async_copy(wd_hbm.at[:, pl.ds(0, cols)], w_s.at[slot, pl.ds(0, n_ff), dst], w_sem.at[slot]).wait()

    w_start(1)
    x_in = pltpu.make_async_copy(x_hbm, x_s, in_sem.at[0])

    barrier = pltpu.get_barrier_semaphore()
    for peer in (mate, far):
        pl.semaphore_signal(barrier, inc=1, device_id={'tp': peer}, device_id_type=MESH)
    pl.semaphore_wait(barrier, 2)

    def copy1(p):
        return pltpu.make_async_remote_copy(send_s.at[p], recv_s.at[p], c1_send.at[p], c1_recv.at[p], device_id={'tp': mate}, device_id_type=MESH)

    def copy2(p):
        return pltpu.make_async_remote_copy(sum_s.at[p], other_s.at[p], c2_send.at[p], c2_recv.at[p], device_id={'tp': far}, device_id_type=MESH)

    def copy3(p, side):
        view = out_ref.at[:, pl.ds(pl.multiple_of(side * half + p * cols, cols), cols)]
        return pltpu.make_async_remote_copy(view, view, c3_send.at[p], c3_recv.at[p], device_id={'tp': mate}, device_id_type=MESH)

    def chip_sum(p):
        copy1(p).wait_recv()
        sum_s[p] = (keep_s[p] + recv_s[p].astype(F32)).astype(BF16)
        copy2(p).start()

    def partial(p, w):
        deep = (n_ff + n_ctx) // 2
        s = (jnp.dot(lhs_s[:, :deep], w[:deep, :], preferred_element_type=F32)
             + jnp.dot(lhs_s[:, deep:], w[deep:, :], preferred_element_type=F32))
        send_s[p] = s[:, :cols].astype(BF16)
        keep_s[p] = s[:, cols:]
        copy1(p).start()

    partial(0, w0_ref)
    w_start(2)
    chip_sum(0)
    w_start(3)
    x_in.start()

    def compute(p, carry):
        w_wait(p)

        @pl.when(p + 3 < PIECES)
        def _():
            w_start(p + 3)
        partial(p, w_s.at[lax.rem(p, W_SLOTS)])

        @pl.when(p > 1)
        def _():
            chip_sum(p - 1)
        return carry

    lax.fori_loop(1, PIECES, compute, 0)
    chip_sum(PIECES - 1)
    x_in.wait()

    def finish(p, carry):
        copy1(p).wait_send()
        copy2(p).wait_send()
        copy2(p).wait_recv()
        xs = x_s[:, pl.ds(col_of(p, 1), cols)].astype(F32)
        out_ref[:, pl.ds(col_of(p, 1), cols)] = (xs + (sum_s[p].astype(F32) + other_s[p].astype(F32))).astype(BF16)
        copy3(p, core).start()
        return carry

    lax.fori_loop(0, PIECES, finish, 0)

    def drain(p, carry):
        copy3(p, core).wait_send()
        copy3(p, 1 - core).wait_recv()
        return carry

    lax.fori_loop(0, PIECES, drain, 0)


def exchange(x, lhs, w0, wd, wo):
    rows, width = x.shape
    cols = width // 2 // PIECES
    n_ff = wd.shape[0]
    n_ctx = wo.shape[0]
    dma = pltpu.SemaphoreType.DMA
    return pl.pallas_call(
        exchange_kernel,
        name='exchange',
        in_specs=[HBM, VMEM, VMEM, HBM, HBM],
        out_specs=VMEM,
        out_shape=jax.ShapeDtypeStruct((rows, width), BF16),
        scratch_shapes=[
            pltpu.VMEM((rows, width), BF16),
            pltpu.VMEM((W_SLOTS, n_ff + n_ctx, 2 * cols), BF16),
            pltpu.VMEM((PIECES, rows, cols), BF16),
            pltpu.VMEM((PIECES, rows, cols), BF16),
            pltpu.VMEM((PIECES, rows, cols), F32),
            pltpu.VMEM((PIECES, rows, cols), BF16),
            pltpu.VMEM((PIECES, rows, cols), BF16),
            dma((1,)), dma((W_SLOTS,)),
            dma((PIECES,)), dma((PIECES,)), dma((PIECES,)), dma((PIECES,)), dma((PIECES,)), dma((PIECES,)),
        ],
        compiler_params=pltpu.CompilerParams(vmem_limit_bytes=32 * MIB, collective_id=0, has_side_effects=True),
        cost_estimate=pl.CostEstimate(flops=11 * 10 ** 9, bytes_accessed=48 * 10 ** 6, transcendentals=0),
    )(x, lhs, w0, wd, wo)


def solution(mesh):
    row_spec = P('dp', None)
    vec_spec = P(None)
    cache_spec = P('dp', 'tp', None, None)

    def device_step(x, ln_attn_gamma, ln_attn_beta, ln_mlp_gamma, ln_mlp_beta, w_qkv, w_out, w_up, w_down, k_cache, v_cache, positions):
        width = x.shape[1]
        head = w_qkv.shape[3]
        inv_freq = ROPE_BASE ** (-2.0 * np.arange(head // 2) / head)
        freq = jnp.asarray(np.concatenate([inv_freq, inv_freq])[None, :], F32)
        vecs = [v.reshape(1, width) for v in (ln_attn_gamma, ln_attn_beta, ln_mlp_gamma, ln_mlp_beta)]
        wq = jnp.transpose(w_qkv, (0, 2, 1, 3)).reshape(-1, head)
        wo = w_out.reshape(-1, width)
        in_hbm = [pltpu.with_memory_space_constraint(a, pltpu.HBM) for a in (positions, x, *vecs, freq, wq, w_up, w_down, wo, k_cache.reshape(-1, head), v_cache.reshape(-1, head))]
        x_h, wd_h, wo_h = in_hbm[1], in_hbm[-4], in_hbm[-3]
        ko, vo, lhs, w0 = front(*in_hbm)
        out = exchange(x_h, lhs, w0, wd_h, wo_h)
        return out, ko.reshape(k_cache.shape), vo.reshape(v_cache.shape)

    return jax.shard_map(device_step, mesh=mesh, in_specs=(row_spec, vec_spec, vec_spec, vec_spec, vec_spec, P(None, 'tp', None, None), P('tp', None, None, None), P(None, 'tp'), P('tp', None), cache_spec, cache_spec, P('dp')), out_specs=(row_spec, cache_spec, cache_spec), check_vma=False)
```

```python
import jax
import jax.numpy as jnp
import numpy as np
from jax import lax
from jax.experimental import pallas as pl
from jax.experimental.pallas import tpu as pltpu
from jax.sharding import PartitionSpec as P

LN_EPS = 1e-5
ROPE_BASE = 10000.0
NEG_BIG = -1e30
BF16 = jnp.bfloat16
F32 = jnp.float32
ANY = pl.BlockSpec(memory_space=pl.ANY)
HBM = pl.BlockSpec(memory_space=pltpu.HBM)
VMEM = pl.BlockSpec(memory_space=pltpu.VMEM)
SMEM = pl.BlockSpec(memory_space=pltpu.SMEM)
MIB = 1024 * 1024

QKV_CHUNK = 512
LN_ROWS = 16
ROW_BLOCK = 16
KV_SLOTS = 6
KV_AHEAD = 4
UP_SLOTS = 4
W_PARTS = 4


def front_kernel(pos_ref, x_hbm, ga_hbm, ba_hbm, gm_hbm, bm_hbm, freq_hbm, wq_hbm, wu_hbm, wd_hbm, wo_hbm, kc_hbm, vc_hbm,
                 ko_hbm, vo_hbm, lhs_ref, w0_ref,
                 x_s, vec_s, freq_s, cos_s, sin_s, attn_s, wqf_s, acc_s, q_s, kv_s, up_s, ctx_s, kbuf, vbuf,
                 in_sem, wq_sem, up_sem, kin_sem, vin_sem, kout_sem, vout_sem, w0_sem):
    mlp_s = x_s
    rows, width = x_s.shape
    seq = kc_hbm.shape[0] // (2 * rows)
    lines_blk = ROW_BLOCK * 2 * seq
    n_ff = lhs_ref.shape[1] - wo_hbm.shape[0]
    n_chunk = width // QKV_CHUNK
    lines = wq_hbm.shape[0] // width
    up_cols = up_s.shape[2]
    n_up = wu_hbm.shape[1] // up_cols
    n_blk = rows // ROW_BLOCK

    x_parts = [pl.ds(k * (rows // W_PARTS), rows // W_PARTS) for k in range(W_PARTS)]
    small = [pltpu.make_async_copy(x_hbm.at[part, :], x_s.at[part, :], in_sem.at[0]) for part in x_parts]
    for i, v in enumerate((ga_hbm, ba_hbm, gm_hbm, bm_hbm)):
        small.append(pltpu.make_async_copy(v, vec_s.at[pl.ds(i, 1), :], in_sem.at[1 + i]))
    freq_in = pltpu.make_async_copy(freq_hbm, freq_s, in_sem.at[5])
    freq_in.start()
    for c in small:
        c.start()

    wq_lines = QKV_CHUNK * lines
    wq_base = (KV_SLOTS - n_chunk * wq_lines // (2 * lines_blk)) * lines_blk
    wq_order = [c for pair in zip(range(n_chunk // 2), range(n_chunk // 2, n_chunk)) for c in pair]

    def wq_view(c):
        buf = kbuf if c < n_chunk // 2 else vbuf
        return buf.at[pl.ds(wq_base + (c % (n_chunk // 2)) * wq_lines, wq_lines), :]

    def wq_copy(c):
        return pltpu.make_async_copy(wq_hbm.at[pl.ds(c * wq_lines, wq_lines), :], wq_view(c), wq_sem.at[c])

    def up_start(b, slot):
        cols = pl.ds(pl.multiple_of(b * up_cols, up_cols), up_cols)
        for k in range(W_PARTS):
            part = pl.ds(k * (width // W_PARTS), width // W_PARTS)
            pltpu.make_async_copy(wu_hbm.at[part, cols], up_s.at[slot, part, :], up_sem.at[slot]).start()

    def up_wait(slot):
        pltpu.make_async_copy(wu_hbm.at[:, pl.ds(0, up_cols)], up_s.at[slot], up_sem.at[slot]).wait()

    def block(ref, i):
        return ref.at[pl.ds(pl.multiple_of(i * lines_blk, lines_blk), lines_blk), :]

    def start_in(i, slot):
        pltpu.make_async_copy(block(kc_hbm, i), block(kbuf, slot), kin_sem.at[slot]).start(priority=1)
        pltpu.make_async_copy(block(vc_hbm, i), block(vbuf, slot), vin_sem.at[slot]).start(priority=1)

    def wait_in(slot):
        pltpu.make_async_copy(block(kc_hbm, 0), block(kbuf, slot), kin_sem.at[slot]).wait()
        pltpu.make_async_copy(block(vc_hbm, 0), block(vbuf, slot), vin_sem.at[slot]).wait()

    def start_out(i, slot):
        pltpu.make_async_copy(block(kbuf, slot), block(ko_hbm, i), kout_sem.at[slot]).start()
        pltpu.make_async_copy(block(vbuf, slot), block(vo_hbm, i), vout_sem.at[slot]).start()

    def wait_out(slot):
        pltpu.make_async_copy(block(kbuf, slot), block(ko_hbm, 0), kout_sem.at[slot]).wait()
        pltpu.make_async_copy(block(vbuf, slot), block(vo_hbm, 0), vout_sem.at[slot]).wait()

    for c in wq_order[:2]:
        wq_copy(c).start()
    start_in(0, 0)

    freq_in.wait()

    def angle_body(b, carry):
        cos_s[pl.ds(b, 1), :] = pos_ref[b].astype(F32) * freq_s[0:1, :]
        return carry

    lax.fori_loop(0, rows, angle_body, 0, unroll=8)
    ang = cos_s[...]
    low = lax.broadcasted_iota(jnp.int32, ang.shape, 1) < 64
    sin_t = jnp.sin(ang)
    sin_s[...] = jnp.where(low, -sin_t, sin_t)
    cos_s[...] = jnp.cos(ang)

    for c in small:
        c.wait()
    for c in wq_order[2:4]:
        wq_copy(c).start()
    start_in(1, 1)

    def ln_body(i, carry):
        r = pl.ds(pl.multiple_of(i * LN_ROWS, LN_ROWS), LN_ROWS)
        xf = x_s[r, :].astype(F32)
        mean = jnp.mean(xf, axis=-1, keepdims=True)
        cen = xf - mean
        var = jnp.mean(cen * cen, axis=-1, keepdims=True)
        nrm = cen * lax.rsqrt(var + LN_EPS)
        attn_s[r, :] = (nrm * vec_s[0:1, :] + vec_s[1:2, :]).astype(BF16)
        mlp_s[r, :] = (nrm * vec_s[2:3, :] + vec_s[3:4, :]).astype(BF16)
        return carry

    half_ln = rows // LN_ROWS // 2
    lax.fori_loop(0, half_ln, ln_body, 0)
    for c in wq_order[4:]:
        wq_copy(c).start()
    free = wq_base // lines_blk
    for i in range(2, free):
        start_in(i, i)
    lax.fori_loop(half_ln, 2 * half_ln, ln_body, 0)

    for step, c in enumerate(wq_order):
        wq_copy(c).wait()
        if step == n_chunk - 2:
            for i in range(free, KV_AHEAD):
                start_in(i, i)
        if step >= n_chunk - UP_SLOTS:
            up_start(step - n_chunk + UP_SLOTS, step - n_chunk + UP_SLOTS)
        wqf_s[...] = wq_view(c)[...].astype(F32)
        lhs = attn_s[:, c * QKV_CHUNK:(c + 1) * QKV_CHUNK]
        for pair in range(lines // 2):
            w = jnp.concatenate([wqf_s[pl.ds(2 * pair + e, QKV_CHUNK, stride=lines), :].astype(BF16) for e in range(2)], axis=1)
            part = jnp.dot(lhs, w, preferred_element_type=F32)
            if step == 0:
                acc_s[:, pair * 256:(pair + 1) * 256] = part
            else:
                acc_s[:, pair * 256:(pair + 1) * 256] += part

    n_slot = lines // 2
    n_q = n_slot - 2
    for j in range(n_slot):
        for g in range(2):
            col = (2 * j + g) * 128
            u = acc_s[:, col:col + 128].astype(BF16).astype(F32)
            if j < n_q + 1:
                u = (u * cos_s[...] + pltpu.roll(u, 64, 1) * sin_s[...]).astype(BF16).astype(F32)
            if j < n_q:
                q_s[pl.ds((g * n_q + j) * rows, rows), :] = u
            else:
                kv_s[pl.ds(((j - n_q) * 2 + g) * rows, rows), :] = u

    slot_ids = lax.broadcasted_iota(jnp.int32, (8, 256), 1)
    tile_ids = lax.broadcasted_iota(jnp.int32, (16, 128), 0)
    first = lax.broadcasted_iota(jnp.int32, (8, 128), 0) < 4
    scale = 128 ** -0.5

    def pair_of(buf, slot, r):
        at = [pl.ds(pl.multiple_of(slot * lines_blk + (2 * r + g) * seq, seq), seq) for g in range(2)]
        return jnp.concatenate([buf[a, :] for a in at], axis=1)

    def attend_block(i, slot):
        pos = [pos_ref[i * ROW_BLOCK + r] for r in range(ROW_BLOCK)]
        for r in range(ROW_BLOCK):
            base = pl.multiple_of((pos[r] // 16) * 16, 16)
            hit = tile_ids == pos[r] - base
            b = i * ROW_BLOCK + r
            for g in range(2):
                tile = pl.ds(pl.multiple_of(slot * lines_blk + (2 * r + g) * seq + base, 16), 16)
                for buf, which in ((kbuf, 0), (vbuf, 1)):
                    new = kv_s[pl.ds((which * 2 + g) * rows + b, 1), :]
                    buf[tile, :] = jnp.where(hit, new, buf[tile, :].astype(F32)).astype(BF16)
        scores = []
        for r in range(ROW_BLOCK):
            b = i * ROW_BLOCK + r
            q = q_s[pl.ds(b, 8, stride=rows), :]
            zero = jnp.zeros_like(q)
            q2 = jnp.concatenate([jnp.where(first, q, zero), jnp.where(first, zero, q)], axis=1).astype(BF16)
            k2 = pair_of(kbuf, slot, r)
            s = lax.dot_general(q2, k2, (((1,), (1,)), ((), ())), preferred_element_type=F32) * scale
            scores.append(jnp.where(slot_ids <= pos[r], s, NEG_BIG))
        s = jnp.concatenate(scores, axis=0)
        e = jnp.exp(s - jnp.max(s, axis=-1, keepdims=True))
        p = (e / jnp.sum(e, axis=-1, keepdims=True)).astype(BF16)
        for r in range(ROW_BLOCK):
            v2 = pair_of(vbuf, slot, r)
            c = jnp.dot(p[8 * r:8 * r + 8], v2, preferred_element_type=F32)
            ctx_s[pl.ds(i * ROW_BLOCK + r, 8, stride=rows), :] = jnp.where(first, c[:, :128], c[:, 128:])

    core = lax.rem(lax.axis_index('tp'), 2)
    cols = w0_ref.shape[1] // 2
    w0_in = []
    for part in range(2):
        src = pl.ds(pl.multiple_of((core if part else 1 - core) * (wd_hbm.shape[1] // 2), cols), cols)
        dst = pl.ds(part * cols, cols)
        w0_in.append(pltpu.make_async_copy(wd_hbm.at[:, src], w0_ref.at[pl.ds(0, n_ff), dst], w0_sem.at[0]))
        w0_in.append(pltpu.make_async_copy(wo_hbm.at[:, src], w0_ref.at[pl.ds(n_ff, wo_hbm.shape[0]), dst], w0_sem.at[0]))

    def up_block(b):
        uslot = lax.rem(b, UP_SLOTS)
        deep = width // 2
        pre = (jnp.dot(mlp_s[:, :deep], up_s[uslot, :deep, :], preferred_element_type=F32)
               + jnp.dot(mlp_s[:, deep:], up_s[uslot, deep:, :], preferred_element_type=F32))
        act = 0.5 * pre * (1.0 + lax.erf(pre * (0.5 ** 0.5)))
        lhs_ref[:, pl.ds(pl.multiple_of(b * up_cols, up_cols), up_cols)] = act.astype(BF16)

    def body(i, carry):
        nxt = i + KV_AHEAD

        @pl.when(nxt < n_blk)
        def _():
            nslot = lax.rem(nxt, KV_SLOTS)

            @pl.when(nxt >= KV_SLOTS)
            def _():
                wait_out(nslot)
            start_in(nxt, nslot)

        slot = lax.rem(i, KV_SLOTS)

        @pl.when((i >= 1) & (i - 1 + UP_SLOTS < n_up))
        def _():
            up_start(i - 1 + UP_SLOTS, lax.rem(i - 1, UP_SLOTS))

        up_wait(lax.rem(i, UP_SLOTS))
        wait_in(slot)
        up_block(i)
        attend_block(i, slot)
        start_out(i, slot)

        @pl.when(i == n_blk - 5)
        def _():
            for c in w0_in:
                c.start(priority=1)
        return carry

    lax.fori_loop(0, n_blk, body, 0)
    for h in range(ctx_s.shape[0] // rows):
        lhs_ref[:, n_ff + h * 128:n_ff + (h + 1) * 128] = ctx_s[h * rows:(h + 1) * rows, :].astype(BF16)
    for c in w0_in:
        c.wait()
    for i in range(n_blk - KV_SLOTS, n_blk):
        wait_out(i % KV_SLOTS)


def front(pos, x, ga, ba, gm, bm, freq, wq, wu, wd, wo, kc, vc):
    rows, width = x.shape
    hid = wu.shape[1]
    lines = wq.shape[0] // width
    n_head = (lines // 2 - 2) * 2
    up_cols = hid // (rows // ROW_BLOCK)
    lines_blk = kc.shape[0] // rows * ROW_BLOCK
    return pl.pallas_call(
        front_kernel,
        name='front',
        in_specs=[SMEM] + [HBM] * 12,
        out_specs=[HBM, HBM, VMEM, VMEM],
        out_shape=[
            jax.ShapeDtypeStruct(kc.shape, BF16),
            jax.ShapeDtypeStruct(vc.shape, BF16),
            jax.ShapeDtypeStruct((rows, hid + wo.shape[0]), BF16),
            jax.ShapeDtypeStruct((hid + wo.shape[0], width // PIECES), BF16),
        ],
        scratch_shapes=[
            pltpu.VMEM((rows, width), BF16),
            pltpu.VMEM((4, width), F32),
            pltpu.VMEM((1, 128), F32),
            pltpu.VMEM((rows, 128), F32),
            pltpu.VMEM((rows, 128), F32),
            pltpu.VMEM((rows, width), BF16),
            pltpu.VMEM((QKV_CHUNK * lines, 128), F32),
            pltpu.VMEM((rows, lines * 128), F32),
            pltpu.VMEM((n_head * rows, 128), F32),
            pltpu.VMEM((4 * rows, 128), F32),
            pltpu.VMEM((UP_SLOTS, width, up_cols), BF16),
            pltpu.VMEM((n_head * rows, 128), F32),
            pltpu.VMEM((KV_SLOTS * lines_blk, 128), BF16),
            pltpu.VMEM((KV_SLOTS * lines_blk, 128), BF16),
            pltpu.SemaphoreType.DMA((6,)),
            pltpu.SemaphoreType.DMA((width // QKV_CHUNK,)),
            pltpu.SemaphoreType.DMA((UP_SLOTS,)),
            pltpu.SemaphoreType.DMA((KV_SLOTS,)),
            pltpu.SemaphoreType.DMA((KV_SLOTS,)),
            pltpu.SemaphoreType.DMA((KV_SLOTS,)),
            pltpu.SemaphoreType.DMA((KV_SLOTS,)),
            pltpu.SemaphoreType.DMA((1,)),
        ],
        compiler_params=pltpu.CompilerParams(vmem_limit_bytes=44 * MIB),
        cost_estimate=pl.CostEstimate(flops=22 * 10 ** 9, bytes_accessed=180 * 10 ** 6, transcendentals=0),
    )(pos, x, ga, ba, gm, bm, freq, wq, wu, wd, wo, kc, vc)


PIECES = 16
W_SLOTS = 4
MESH = pl.DeviceIdType.MESH


def exchange_kernel(x_hbm, lhs_s, w0_ref, wd_hbm, wo_hbm, out_ref,
                    x_s, w_s, send_s, recv_s, keep_s, sum_s, other_s,
                    in_sem, w_sem, c1_send, c1_recv, c2_send, c2_recv, c3_send, c3_recv):
    rows, width = x_s.shape
    half = width // 2
    cols = half // PIECES
    n_ff, n_ctx = wd_hbm.shape[0], wo_hbm.shape[0]
    me = lax.axis_index('tp')
    core = lax.rem(me, 2)
    mate = me + 1 - 2 * core
    far = lax.rem(me + 2, 4)

    def col_of(p, part):
        side = core if part else 1 - core
        return pl.multiple_of(side * half + p * cols, cols)

    def w_start(p):
        slot = lax.rem(p, W_SLOTS)
        for part in range(2):
            src, dst = pl.ds(col_of(p, part), cols), pl.ds(part * cols, cols)
            pltpu.make_async_copy(wo_hbm.at[:, src], w_s.at[slot, pl.ds(n_ff, n_ctx), dst], w_sem.at[slot]).start()
            for k in range(2):
                deep = pl.ds(k * (n_ff // 2), n_ff // 2)
                pltpu.make_async_copy(wd_hbm.at[deep, src], w_s.at[slot, deep, dst], w_sem.at[slot]).start()

    def w_wait(p):
        slot = lax.rem(p, W_SLOTS)
        for part in range(2):
            dst = pl.ds(part * cols, cols)
            pltpu.make_async_copy(wo_hbm.at[:, pl.ds(0, cols)], w_s.at[slot, pl.ds(n_ff, n_ctx), dst], w_sem.at[slot]).wait()
            pltpu.make_async_copy(wd_hbm.at[:, pl.ds(0, cols)], w_s.at[slot, pl.ds(0, n_ff), dst], w_sem.at[slot]).wait()

    w_start(1)
    x_in = pltpu.make_async_copy(x_hbm, x_s, in_sem.at[0])

    barrier = pltpu.get_barrier_semaphore()
    for peer in (mate, far):
        pl.semaphore_signal(barrier, inc=1, device_id={'tp': peer}, device_id_type=MESH)
    pl.semaphore_wait(barrier, 2)

    def copy1(p):
        return pltpu.make_async_remote_copy(send_s.at[p], recv_s.at[p], c1_send.at[p], c1_recv.at[p], device_id={'tp': mate}, device_id_type=MESH)

    def copy2(p):
        return pltpu.make_async_remote_copy(sum_s.at[p], other_s.at[p], c2_send.at[p], c2_recv.at[p], device_id={'tp': far}, device_id_type=MESH)

    def copy3(p, side):
        view = out_ref.at[:, pl.ds(pl.multiple_of(side * half + p * cols, cols), cols)]
        return pltpu.make_async_remote_copy(view, view, c3_send.at[p], c3_recv.at[p], device_id={'tp': mate}, device_id_type=MESH)

    def chip_sum(p):
        copy1(p).wait_recv()
        sum_s[p] = (keep_s[p] + recv_s[p].astype(F32)).astype(BF16)
        copy2(p).start()

    def partial(p, w):
        deep = (n_ff + n_ctx) // 2
        s = (jnp.dot(lhs_s[:, :deep], w[:deep, :], preferred_element_type=F32)
             + jnp.dot(lhs_s[:, deep:], w[deep:, :], preferred_element_type=F32))
        send_s[p] = s[:, :cols].astype(BF16)
        keep_s[p] = s[:, cols:]
        copy1(p).start()

    partial(0, w0_ref)
    w_start(2)
    chip_sum(0)
    w_start(3)
    x_in.start()

    def compute(p, carry):
        w_wait(p)

        @pl.when(p + 3 < PIECES)
        def _():
            w_start(p + 3)
        partial(p, w_s.at[lax.rem(p, W_SLOTS)])

        @pl.when(p > 1)
        def _():
            chip_sum(p - 1)
        return carry

    lax.fori_loop(1, PIECES, compute, 0)
    chip_sum(PIECES - 1)
    x_in.wait()

    def finish(p, carry):
        copy1(p).wait_send()
        copy2(p).wait_send()
        copy2(p).wait_recv()
        xs = x_s[:, pl.ds(col_of(p, 1), cols)].astype(F32)
        out_ref[:, pl.ds(col_of(p, 1), cols)] = (xs + (sum_s[p].astype(F32) + other_s[p].astype(F32))).astype(BF16)
        copy3(p, core).start()
        return carry

    lax.fori_loop(0, PIECES, finish, 0)

    def drain(p, carry):
        copy3(p, core).wait_send()
        copy3(p, 1 - core).wait_recv()
        return carry

    lax.fori_loop(0, PIECES, drain, 0)


def exchange(x, lhs, w0, wd, wo):
    rows, width = x.shape
    cols = width // 2 // PIECES
    n_ff = wd.shape[0]
    n_ctx = wo.shape[0]
    dma = pltpu.SemaphoreType.DMA
    return pl.pallas_call(
        exchange_kernel,
        name='exchange',
        in_specs=[HBM, VMEM, VMEM, HBM, HBM],
        out_specs=VMEM,
        out_shape=jax.ShapeDtypeStruct((rows, width), BF16),
        scratch_shapes=[
            pltpu.VMEM((rows, width), BF16),
            pltpu.VMEM((W_SLOTS, n_ff + n_ctx, 2 * cols), BF16),
            pltpu.VMEM((PIECES, rows, cols), BF16),
            pltpu.VMEM((PIECES, rows, cols), BF16),
            pltpu.VMEM((PIECES, rows, cols), F32),
            pltpu.VMEM((PIECES, rows, cols), BF16),
            pltpu.VMEM((PIECES, rows, cols), BF16),
            dma((1,)), dma((W_SLOTS,)),
            dma((PIECES,)), dma((PIECES,)), dma((PIECES,)), dma((PIECES,)), dma((PIECES,)), dma((PIECES,)),
        ],
        compiler_params=pltpu.CompilerParams(vmem_limit_bytes=32 * MIB, collective_id=0, has_side_effects=True),
        cost_estimate=pl.CostEstimate(flops=11 * 10 ** 9, bytes_accessed=48 * 10 ** 6, transcendentals=0),
    )(x, lhs, w0, wd, wo)


def solution(mesh):
    row_spec = P('dp', None)
    vec_spec = P(None)
    cache_spec = P('dp', 'tp', None, None)

    def device_step(x, ln_attn_gamma, ln_attn_beta, ln_mlp_gamma, ln_mlp_beta, w_qkv, w_out, w_up, w_down, k_cache, v_cache, positions):
        width = x.shape[1]
        head = w_qkv.shape[3]
        inv_freq = ROPE_BASE ** (-2.0 * np.arange(head // 2) / head)
        freq = jnp.asarray(np.concatenate([inv_freq, inv_freq])[None, :], F32)
        vecs = [v.reshape(1, width) for v in (ln_attn_gamma, ln_attn_beta, ln_mlp_gamma, ln_mlp_beta)]
        wq = jnp.transpose(w_qkv, (0, 2, 1, 3)).reshape(-1, head)
        wo = w_out.reshape(-1, width)
        in_hbm = [pltpu.with_memory_space_constraint(a, pltpu.HBM) for a in (positions, x, *vecs, freq, wq, w_up, w_down, wo, k_cache.reshape(-1, head), v_cache.reshape(-1, head))]
        x_h, wd_h, wo_h = in_hbm[1], in_hbm[-4], in_hbm[-3]
        ko, vo, lhs, w0 = front(*in_hbm)
        out = exchange(x_h, lhs, w0, wd_h, wo_h)
        return out, ko.reshape(k_cache.shape), vo.reshape(v_cache.shape)

    return jax.shard_map(device_step, mesh=mesh, in_specs=(row_spec, vec_spec, vec_spec, vec_spec, vec_spec, P(None, 'tp', None, None), P('tp', None, None, None), P(None, 'tp'), P('tp', None), cache_spec, cache_spec, P('dp')), out_specs=(row_spec, cache_spec, cache_spec), check_vma=False)
```

```python
import jax
import jax.numpy as jnp
import numpy as np
from jax import lax
from jax.experimental import pallas as pl
from jax.experimental.pallas import tpu as pltpu
from jax.sharding import PartitionSpec as P

LN_EPS = 1e-5
ROPE_BASE = 10000.0
NEG_BIG = -1e30
BF16 = jnp.bfloat16
F32 = jnp.float32
ANY = pl.BlockSpec(memory_space=pl.ANY)
HBM = pl.BlockSpec(memory_space=pltpu.HBM)
VMEM = pl.BlockSpec(memory_space=pltpu.VMEM)
SMEM = pl.BlockSpec(memory_space=pltpu.SMEM)
MIB = 1024 * 1024

QKV_CHUNK = 512
LN_ROWS = 16
ROW_BLOCK = 16
KV_SLOTS = 6
KV_AHEAD = 4
UP_SLOTS = 5
W_PARTS = 4


def front_kernel(pos_ref, x_hbm, ga_hbm, ba_hbm, gm_hbm, bm_hbm, freq_hbm, wq_hbm, wu_hbm, wd_hbm, wo_hbm, kc_hbm, vc_hbm,
                 ko_hbm, vo_hbm, lhs_ref, w0_ref,
                 x_s, vec_s, freq_s, cos_s, sin_s, attn_s, wqf_s, acc_s, q_s, kv_s, up_s, ctx_s, kbuf, vbuf,
                 in_sem, wq_sem, up_sem, kin_sem, vin_sem, kout_sem, vout_sem, w0_sem):
    mlp_s = x_s
    rows, width = x_s.shape
    seq = kc_hbm.shape[0] // (2 * rows)
    lines_blk = ROW_BLOCK * 2 * seq
    n_ff = lhs_ref.shape[1] - wo_hbm.shape[0]
    n_chunk = width // QKV_CHUNK
    lines = wq_hbm.shape[0] // width
    up_cols = up_s.shape[2]
    n_up = wu_hbm.shape[1] // up_cols
    n_blk = rows // ROW_BLOCK

    x_parts = [pl.ds(k * (rows // W_PARTS), rows // W_PARTS) for k in range(W_PARTS)]
    small = [pltpu.make_async_copy(x_hbm.at[part, :], x_s.at[part, :], in_sem.at[0]) for part in x_parts]
    for i, v in enumerate((ga_hbm, ba_hbm, gm_hbm, bm_hbm)):
        small.append(pltpu.make_async_copy(v, vec_s.at[pl.ds(i, 1), :], in_sem.at[1 + i]))
    freq_in = pltpu.make_async_copy(freq_hbm, freq_s, in_sem.at[5])
    freq_in.start()
    for c in small:
        c.start()

    wq_lines = QKV_CHUNK * lines
    wq_base = (KV_SLOTS - n_chunk * wq_lines // (2 * lines_blk)) * lines_blk
    wq_order = [c for pair in zip(range(n_chunk // 2), range(n_chunk // 2, n_chunk)) for c in pair]

    def wq_view(c):
        buf = kbuf if c < n_chunk // 2 else vbuf
        return buf.at[pl.ds(wq_base + (c % (n_chunk // 2)) * wq_lines, wq_lines), :]

    def wq_copy(c):
        return pltpu.make_async_copy(wq_hbm.at[pl.ds(c * wq_lines, wq_lines), :], wq_view(c), wq_sem.at[c])

    def up_start(b, slot):
        cols = pl.ds(pl.multiple_of(b * up_cols, up_cols), up_cols)
        for k in range(W_PARTS):
            part = pl.ds(k * (width // W_PARTS), width // W_PARTS)
            pltpu.make_async_copy(wu_hbm.at[part, cols], up_s.at[slot, part, :], up_sem.at[slot]).start()

    def up_wait(slot):
        pltpu.make_async_copy(wu_hbm.at[:, pl.ds(0, up_cols)], up_s.at[slot], up_sem.at[slot]).wait()

    def block(ref, i):
        return ref.at[pl.ds(pl.multiple_of(i * lines_blk, lines_blk), lines_blk), :]

    def start_in(i, slot):
        pltpu.make_async_copy(block(kc_hbm, i), block(kbuf, slot), kin_sem.at[slot]).start(priority=1)
        pltpu.make_async_copy(block(vc_hbm, i), block(vbuf, slot), vin_sem.at[slot]).start(priority=1)

    def wait_in(slot):
        pltpu.make_async_copy(block(kc_hbm, 0), block(kbuf, slot), kin_sem.at[slot]).wait()
        pltpu.make_async_copy(block(vc_hbm, 0), block(vbuf, slot), vin_sem.at[slot]).wait()

    def start_out(i, slot):
        pltpu.make_async_copy(block(kbuf, slot), block(ko_hbm, i), kout_sem.at[slot]).start()
        pltpu.make_async_copy(block(vbuf, slot), block(vo_hbm, i), vout_sem.at[slot]).start()

    def wait_out(slot):
        pltpu.make_async_copy(block(kbuf, slot), block(ko_hbm, 0), kout_sem.at[slot]).wait()
        pltpu.make_async_copy(block(vbuf, slot), block(vo_hbm, 0), vout_sem.at[slot]).wait()

    for c in wq_order[:2]:
        wq_copy(c).start()
    start_in(0, 0)

    freq_in.wait()

    def angle_body(b, carry):
        cos_s[pl.ds(b, 1), :] = pos_ref[b].astype(F32) * freq_s[0:1, :]
        return carry

    lax.fori_loop(0, rows, angle_body, 0, unroll=8)
    ang = cos_s[...]
    low = lax.broadcasted_iota(jnp.int32, ang.shape, 1) < 64
    sin_t = jnp.sin(ang)
    sin_s[...] = jnp.where(low, -sin_t, sin_t)
    cos_s[...] = jnp.cos(ang)

    for c in small:
        c.wait()
    for c in wq_order[2:4]:
        wq_copy(c).start()
    start_in(1, 1)

    def ln_body(i, carry):
        r = pl.ds(pl.multiple_of(i * LN_ROWS, LN_ROWS), LN_ROWS)
        xf = x_s[r, :].astype(F32)
        mean = jnp.mean(xf, axis=-1, keepdims=True)
        cen = xf - mean
        var = jnp.mean(cen * cen, axis=-1, keepdims=True)
        nrm = cen * lax.rsqrt(var + LN_EPS)
        attn_s[r, :] = (nrm * vec_s[0:1, :] + vec_s[1:2, :]).astype(BF16)
        mlp_s[r, :] = (nrm * vec_s[2:3, :] + vec_s[3:4, :]).astype(BF16)
        return carry

    half_ln = rows // LN_ROWS // 2
    lax.fori_loop(0, half_ln, ln_body, 0)
    for c in wq_order[4:]:
        wq_copy(c).start()
    free = wq_base // lines_blk
    for i in range(2, free):
        start_in(i, i)
    lax.fori_loop(half_ln, 2 * half_ln, ln_body, 0)

    for step, c in enumerate(wq_order):
        wq_copy(c).wait()
        if step == n_chunk - 2:
            for i in range(free, KV_AHEAD):
                start_in(i, i)
        if step >= n_chunk - UP_SLOTS:
            up_start(step - n_chunk + UP_SLOTS, step - n_chunk + UP_SLOTS)
        wqf_s[...] = wq_view(c)[...].astype(F32)
        lhs = attn_s[:, c * QKV_CHUNK:(c + 1) * QKV_CHUNK]
        for pair in range(lines // 2):
            w = jnp.concatenate([wqf_s[pl.ds(2 * pair + e, QKV_CHUNK, stride=lines), :].astype(BF16) for e in range(2)], axis=1)
            part = jnp.dot(lhs, w, preferred_element_type=F32)
            if step == 0:
                acc_s[:, pair * 256:(pair + 1) * 256] = part
            else:
                acc_s[:, pair * 256:(pair + 1) * 256] += part

    n_slot = lines // 2
    n_q = n_slot - 2
    for j in range(n_slot):
        for g in range(2):
            col = (2 * j + g) * 128
            u = acc_s[:, col:col + 128].astype(BF16).astype(F32)
            if j < n_q + 1:
                u = (u * cos_s[...] + pltpu.roll(u, 64, 1) * sin_s[...]).astype(BF16).astype(F32)
            if j < n_q:
                q_s[pl.ds((g * n_q + j) * rows, rows), :] = u
            else:
                kv_s[pl.ds(((j - n_q) * 2 + g) * rows, rows), :] = u

    slot_ids = lax.broadcasted_iota(jnp.int32, (8, 256), 1)
    tile_ids = lax.broadcasted_iota(jnp.int32, (16, 128), 0)
    first = lax.broadcasted_iota(jnp.int32, (8, 128), 0) < 4
    scale = 128 ** -0.5

    def pair_of(buf, slot, r):
        at = [pl.ds(pl.multiple_of(slot * lines_blk + (2 * r + g) * seq, seq), seq) for g in range(2)]
        return jnp.concatenate([buf[a, :] for a in at], axis=1)

    def attend_block(i, slot):
        pos = [pos_ref[i * ROW_BLOCK + r] for r in range(ROW_BLOCK)]
        for r in range(ROW_BLOCK):
            base = pl.multiple_of((pos[r] // 16) * 16, 16)
            hit = tile_ids == pos[r] - base
            b = i * ROW_BLOCK + r
            for g in range(2):
                tile = pl.ds(pl.multiple_of(slot * lines_blk + (2 * r + g) * seq + base, 16), 16)
                for buf, which in ((kbuf, 0), (vbuf, 1)):
                    new = kv_s[pl.ds((which * 2 + g) * rows + b, 1), :]
                    buf[tile, :] = jnp.where(hit, new, buf[tile, :].astype(F32)).astype(BF16)
        scores = []
        for r in range(ROW_BLOCK):
            b = i * ROW_BLOCK + r
            q = q_s[pl.ds(b, 8, stride=rows), :]
            zero = jnp.zeros_like(q)
            q2 = jnp.concatenate([jnp.where(first, q, zero), jnp.where(first, zero, q)], axis=1).astype(BF16)
            k2 = pair_of(kbuf, slot, r)
            s = lax.dot_general(q2, k2, (((1,), (1,)), ((), ())), preferred_element_type=F32) * scale
            scores.append(jnp.where(slot_ids <= pos[r], s, NEG_BIG))
        s = jnp.concatenate(scores, axis=0)
        e = jnp.exp(s - jnp.max(s, axis=-1, keepdims=True))
        p = (e / jnp.sum(e, axis=-1, keepdims=True)).astype(BF16)
        for r in range(ROW_BLOCK):
            v2 = pair_of(vbuf, slot, r)
            c = jnp.dot(p[8 * r:8 * r + 8], v2, preferred_element_type=F32)
            ctx_s[pl.ds(i * ROW_BLOCK + r, 8, stride=rows), :] = jnp.where(first, c[:, :128], c[:, 128:])

    core = lax.rem(lax.axis_index('tp'), 2)
    cols = w0_ref.shape[1] // 2
    w0_in = []
    for part in range(2):
        src = pl.ds(pl.multiple_of((core if part else 1 - core) * (wd_hbm.shape[1] // 2), cols), cols)
        dst = pl.ds(part * cols, cols)
        w0_in.append(pltpu.make_async_copy(wd_hbm.at[:, src], w0_ref.at[pl.ds(0, n_ff), dst], w0_sem.at[0]))
        w0_in.append(pltpu.make_async_copy(wo_hbm.at[:, src], w0_ref.at[pl.ds(n_ff, wo_hbm.shape[0]), dst], w0_sem.at[0]))

    def up_block(b):
        uslot = lax.rem(b, UP_SLOTS)
        deep = width // 2
        pre = (jnp.dot(mlp_s[:, :deep], up_s[uslot, :deep, :], preferred_element_type=F32)
               + jnp.dot(mlp_s[:, deep:], up_s[uslot, deep:, :], preferred_element_type=F32))
        act = 0.5 * pre * (1.0 + lax.erf(pre * (0.5 ** 0.5)))
        lhs_ref[:, pl.ds(pl.multiple_of(b * up_cols, up_cols), up_cols)] = act.astype(BF16)

    def body(i, carry):
        nxt = i + KV_AHEAD

        @pl.when(nxt < n_blk)
        def _():
            nslot = lax.rem(nxt, KV_SLOTS)

            @pl.when(nxt >= KV_SLOTS)
            def _():
                wait_out(nslot)
            start_in(nxt, nslot)

        slot = lax.rem(i, KV_SLOTS)

        @pl.when((i >= 1) & (i - 1 + UP_SLOTS < n_up))
        def _():
            up_start(i - 1 + UP_SLOTS, lax.rem(i - 1, UP_SLOTS))

        up_wait(lax.rem(i, UP_SLOTS))
        wait_in(slot)
        up_block(i)
        attend_block(i, slot)
        start_out(i, slot)

        @pl.when(i == n_blk - 5)
        def _():
            for c in w0_in:
                c.start(priority=1)
        return carry

    lax.fori_loop(0, n_blk, body, 0)
    for h in range(ctx_s.shape[0] // rows):
        lhs_ref[:, n_ff + h * 128:n_ff + (h + 1) * 128] = ctx_s[h * rows:(h + 1) * rows, :].astype(BF16)
    for c in w0_in:
        c.wait()
    for i in range(n_blk - KV_SLOTS, n_blk):
        wait_out(i % KV_SLOTS)


def front(pos, x, ga, ba, gm, bm, freq, wq, wu, wd, wo, kc, vc):
    rows, width = x.shape
    hid = wu.shape[1]
    lines = wq.shape[0] // width
    n_head = (lines // 2 - 2) * 2
    up_cols = hid // (rows // ROW_BLOCK)
    lines_blk = kc.shape[0] // rows * ROW_BLOCK
    return pl.pallas_call(
        front_kernel,
        name='front',
        in_specs=[SMEM] + [HBM] * 12,
        out_specs=[HBM, HBM, VMEM, VMEM],
        out_shape=[
            jax.ShapeDtypeStruct(kc.shape, BF16),
            jax.ShapeDtypeStruct(vc.shape, BF16),
            jax.ShapeDtypeStruct((rows, hid + wo.shape[0]), BF16),
            jax.ShapeDtypeStruct((hid + wo.shape[0], width // PIECES), BF16),
        ],
        scratch_shapes=[
            pltpu.VMEM((rows, width), BF16),
            pltpu.VMEM((4, width), F32),
            pltpu.VMEM((1, 128), F32),
            pltpu.VMEM((rows, 128), F32),
            pltpu.VMEM((rows, 128), F32),
            pltpu.VMEM((rows, width), BF16),
            pltpu.VMEM((QKV_CHUNK * lines, 128), F32),
            pltpu.VMEM((rows, lines * 128), F32),
            pltpu.VMEM((n_head * rows, 128), F32),
            pltpu.VMEM((4 * rows, 128), F32),
            pltpu.VMEM((UP_SLOTS, width, up_cols), BF16),
            pltpu.VMEM((n_head * rows, 128), F32),
            pltpu.VMEM((KV_SLOTS * lines_blk, 128), BF16),
            pltpu.VMEM((KV_SLOTS * lines_blk, 128), BF16),
            pltpu.SemaphoreType.DMA((6,)),
            pltpu.SemaphoreType.DMA((width // QKV_CHUNK,)),
            pltpu.SemaphoreType.DMA((UP_SLOTS,)),
            pltpu.SemaphoreType.DMA((KV_SLOTS,)),
            pltpu.SemaphoreType.DMA((KV_SLOTS,)),
            pltpu.SemaphoreType.DMA((KV_SLOTS,)),
            pltpu.SemaphoreType.DMA((KV_SLOTS,)),
            pltpu.SemaphoreType.DMA((1,)),
        ],
        compiler_params=pltpu.CompilerParams(vmem_limit_bytes=46 * MIB),
        cost_estimate=pl.CostEstimate(flops=22 * 10 ** 9, bytes_accessed=180 * 10 ** 6, transcendentals=0),
    )(pos, x, ga, ba, gm, bm, freq, wq, wu, wd, wo, kc, vc)


PIECES = 16
W_SLOTS = 4
MESH = pl.DeviceIdType.MESH


def exchange_kernel(x_hbm, lhs_s, w0_ref, wd_hbm, wo_hbm, out_ref,
                    x_s, w_s, send_s, recv_s, keep_s, sum_s, other_s,
                    in_sem, w_sem, c1_send, c1_recv, c2_send, c2_recv, c3_send, c3_recv):
    rows, width = x_s.shape
    half = width // 2
    cols = half // PIECES
    n_ff, n_ctx = wd_hbm.shape[0], wo_hbm.shape[0]
    me = lax.axis_index('tp')
    core = lax.rem(me, 2)
    mate = me + 1 - 2 * core
    far = lax.rem(me + 2, 4)

    def col_of(p, part):
        side = core if part else 1 - core
        return pl.multiple_of(side * half + p * cols, cols)

    def w_start(p):
        slot = lax.rem(p, W_SLOTS)
        for part in range(2):
            src, dst = pl.ds(col_of(p, part), cols), pl.ds(part * cols, cols)
            pltpu.make_async_copy(wo_hbm.at[:, src], w_s.at[slot, pl.ds(n_ff, n_ctx), dst], w_sem.at[slot]).start()
            for k in range(2):
                deep = pl.ds(k * (n_ff // 2), n_ff // 2)
                pltpu.make_async_copy(wd_hbm.at[deep, src], w_s.at[slot, deep, dst], w_sem.at[slot]).start()

    def w_wait(p):
        slot = lax.rem(p, W_SLOTS)
        for part in range(2):
            dst = pl.ds(part * cols, cols)
            pltpu.make_async_copy(wo_hbm.at[:, pl.ds(0, cols)], w_s.at[slot, pl.ds(n_ff, n_ctx), dst], w_sem.at[slot]).wait()
            pltpu.make_async_copy(wd_hbm.at[:, pl.ds(0, cols)], w_s.at[slot, pl.ds(0, n_ff), dst], w_sem.at[slot]).wait()

    w_start(1)
    x_in = pltpu.make_async_copy(x_hbm, x_s, in_sem.at[0])

    barrier = pltpu.get_barrier_semaphore()
    for peer in (mate, far):
        pl.semaphore_signal(barrier, inc=1, device_id={'tp': peer}, device_id_type=MESH)
    pl.semaphore_wait(barrier, 2)

    def copy1(p):
        return pltpu.make_async_remote_copy(send_s.at[p], recv_s.at[p], c1_send.at[p], c1_recv.at[p], device_id={'tp': mate}, device_id_type=MESH)

    def copy2(p):
        return pltpu.make_async_remote_copy(sum_s.at[p], other_s.at[p], c2_send.at[p], c2_recv.at[p], device_id={'tp': far}, device_id_type=MESH)

    def copy3(p, side):
        view = out_ref.at[:, pl.ds(pl.multiple_of(side * half + p * cols, cols), cols)]
        return pltpu.make_async_remote_copy(view, view, c3_send.at[p], c3_recv.at[p], device_id={'tp': mate}, device_id_type=MESH)

    def chip_sum(p):
        copy1(p).wait_recv()
        sum_s[p] = (keep_s[p] + recv_s[p].astype(F32)).astype(BF16)
        copy2(p).start()

    def partial(p, w):
        deep = (n_ff + n_ctx) // 2
        s = (jnp.dot(lhs_s[:, :deep], w[:deep, :], preferred_element_type=F32)
             + jnp.dot(lhs_s[:, deep:], w[deep:, :], preferred_element_type=F32))
        send_s[p] = s[:, :cols].astype(BF16)
        keep_s[p] = s[:, cols:]
        copy1(p).start()

    partial(0, w0_ref)
    w_start(2)
    chip_sum(0)
    w_start(3)
    x_in.start()

    def compute(p, carry):
        w_wait(p)

        @pl.when(p + 3 < PIECES)
        def _():
            w_start(p + 3)
        partial(p, w_s.at[lax.rem(p, W_SLOTS)])

        @pl.when(p > 1)
        def _():
            chip_sum(p - 1)
        return carry

    lax.fori_loop(1, PIECES, compute, 0)
    chip_sum(PIECES - 1)
    x_in.wait()

    def finish(p, carry):
        copy1(p).wait_send()
        copy2(p).wait_send()
        copy2(p).wait_recv()
        xs = x_s[:, pl.ds(col_of(p, 1), cols)].astype(F32)
        out_ref[:, pl.ds(col_of(p, 1), cols)] = (xs + (sum_s[p].astype(F32) + other_s[p].astype(F32))).astype(BF16)
        copy3(p, core).start()
        return carry

    lax.fori_loop(0, PIECES, finish, 0)

    def drain(p, carry):
        copy3(p, core).wait_send()
        copy3(p, 1 - core).wait_recv()
        return carry

    lax.fori_loop(0, PIECES, drain, 0)


def exchange(x, lhs, w0, wd, wo):
    rows, width = x.shape
    cols = width // 2 // PIECES
    n_ff = wd.shape[0]
    n_ctx = wo.shape[0]
    dma = pltpu.SemaphoreType.DMA
    return pl.pallas_call(
        exchange_kernel,
        name='exchange',
        in_specs=[HBM, VMEM, VMEM, HBM, HBM],
        out_specs=VMEM,
        out_shape=jax.ShapeDtypeStruct((rows, width), BF16),
        scratch_shapes=[
            pltpu.VMEM((rows, width), BF16),
            pltpu.VMEM((W_SLOTS, n_ff + n_ctx, 2 * cols), BF16),
            pltpu.VMEM((PIECES, rows, cols), BF16),
            pltpu.VMEM((PIECES, rows, cols), BF16),
            pltpu.VMEM((PIECES, rows, cols), F32),
            pltpu.VMEM((PIECES, rows, cols), BF16),
            pltpu.VMEM((PIECES, rows, cols), BF16),
            dma((1,)), dma((W_SLOTS,)),
            dma((PIECES,)), dma((PIECES,)), dma((PIECES,)), dma((PIECES,)), dma((PIECES,)), dma((PIECES,)),
        ],
        compiler_params=pltpu.CompilerParams(vmem_limit_bytes=32 * MIB, collective_id=0, has_side_effects=True),
        cost_estimate=pl.CostEstimate(flops=11 * 10 ** 9, bytes_accessed=48 * 10 ** 6, transcendentals=0),
    )(x, lhs, w0, wd, wo)


def solution(mesh):
    row_spec = P('dp', None)
    vec_spec = P(None)
    cache_spec = P('dp', 'tp', None, None)

    def device_step(x, ln_attn_gamma, ln_attn_beta, ln_mlp_gamma, ln_mlp_beta, w_qkv, w_out, w_up, w_down, k_cache, v_cache, positions):
        width = x.shape[1]
        head = w_qkv.shape[3]
        inv_freq = ROPE_BASE ** (-2.0 * np.arange(head // 2) / head)
        freq = jnp.asarray(np.concatenate([inv_freq, inv_freq])[None, :], F32)
        vecs = [v.reshape(1, width) for v in (ln_attn_gamma, ln_attn_beta, ln_mlp_gamma, ln_mlp_beta)]
        wq = jnp.transpose(w_qkv, (0, 2, 1, 3)).reshape(-1, head)
        wo = w_out.reshape(-1, width)
        in_hbm = [pltpu.with_memory_space_constraint(a, pltpu.HBM) for a in (positions, x, *vecs, freq, wq, w_up, w_down, wo, k_cache.reshape(-1, head), v_cache.reshape(-1, head))]
        x_h, wd_h, wo_h = in_hbm[1], in_hbm[-4], in_hbm[-3]
        ko, vo, lhs, w0 = front(*in_hbm)
        out = exchange(x_h, lhs, w0, wd_h, wo_h)
        return out, ko.reshape(k_cache.shape), vo.reshape(v_cache.shape)

    return jax.shard_map(device_step, mesh=mesh, in_specs=(row_spec, vec_spec, vec_spec, vec_spec, vec_spec, P(None, 'tp', None, None), P('tp', None, None, None), P(None, 'tp'), P('tp', None), cache_spec, cache_spec, P('dp')), out_specs=(row_spec, cache_spec, cache_spec), check_vma=False)
```
